512 devices in a mesh: grp: 8 (over z), tp: 16 (over x_lo, y), src: 4 (over x_hi, core).
Axes of the slice: x: 4 (x_hi: 2, x_lo: 2; x = x_hi * 2 + x_lo), y: 8, z: 8, core: 2. Of those that a mesh axis runs over, the one named last changes fastest.
Arguments:
- hidden_in: bfloat16 [2048, 5120], P(('grp', 'src')), may hold values from -6 to 6
- attn_gain: float32 [5120], replicated, may hold values from 0.5 to 1.5
- w_qkv: int32 [1280, 5120], P(None, 'tp'), may hold values from -2147483648 to 2147483646
- qkv_scale: float32 [5120], P('tp'), may hold values from 0.0001118034 to 0.00041926274
- q_gain: float32 [128], replicated, may hold values from 0.25 to 1.75
- k_gain: float32 [128], replicated, may hold values from 0.1 to 1.9
- key_cache: bfloat16 [32, 64, 128, 512], P(('grp', 'src'), 'tp'), may hold values from -400 to 400
- value_cache: bfloat16 [32, 64, 128, 512], P(('grp', 'src'), 'tp'), may hold values from -9 to 9
- lengths: int32 [32, 64], P(('grp', 'src'), 'tp'), may hold values from 1 to 128, as said below
- w_out: int32 [1024, 5120], P('tp'), may hold values from -2147483648 to 2147483646
- out_scale: float32 [5120], replicated, may hold values from 0.0003125 to 0.00125
- mlp_gain: float32 [5120], replicated, may hold values from 0.5 to 1.5
- w_gate: int32 [1280, 12800], P(('grp', 'src'), 'tp'), may hold values from -2147483648 to 2147483646
- w_up: int32 [1280, 12800], P(('grp', 'src'), 'tp'), may hold values from -2147483648 to 2147483646
- gate_scale: float32 [12800], P('tp'), may hold values from 0.0001118034 to 0.00041926274
- up_scale: float32 [12800], P('tp'), may hold values from 0.0001118034 to 0.00041926274
- w_down: int32 [3200, 5120], P('tp', ('grp', 'src')), may hold values from -2147483648 to 2147483646
- down_scale: float32 [5120], replicated, may hold values from 0.00013258251 to 0.00053033006
Outputs:
- layer_out: bfloat16 [2048, 5120], P(('grp', 'src'), 'tp')
The draws below stay inside these ranges and needn't reach their ends.
Inputs may be any that keep to these rules, and one draw needn't show every extreme that they name: `lengths`: some sequence has exactly 128 cached positions.
All inputs are finite; a program needn't handle non-finite values.
Results may differ from the reference program's by a relative error of at most 0.028.
Values may be sent and summed in bfloat16 or wider, within the bound.
A program may use at most 64 MiB of HBM per device.

```python
import math
import jax
import jax.numpy as jnp
from jax import lax

D = 5120
QUERY_HEADS = 32
KEY_VALUE_HEADS = 4
HEAD_SIZE = 128
FFW = 12800
B_DEV = 64
CACHE_POSITIONS = 128
NGROUPS = 32
B = 2048
QUERY_COLUMNS = 4096
KEY_COLUMNS = 512
QKV = 5120


def draw_key_cache(key, part):
    first_key = jax.random.fold_in(jax.random.fold_in(key, 11), 0)
    normal_part = jax.random.normal(first_key, (NGROUPS, B_DEV, CACHE_POSITIONS, KEY_COLUMNS), jnp.float32)
    return jnp.clip(normal_part, -6.0, 6.0).astype(jnp.bfloat16)


def draw_lengths(key, part):
    first_key, second_key = jax.random.split(jax.random.fold_in(key, 23))
    base_lengths = jax.random.randint(first_key, (NGROUPS * B_DEV,), 1, CACHE_POSITIONS + 1)
    longest_slot = jax.random.randint(second_key, (), 0, NGROUPS * B_DEV)
    flat_lengths = jnp.where(jnp.arange(NGROUPS * B_DEV) == longest_slot, CACHE_POSITIONS, base_lengths)
    return flat_lengths.reshape(NGROUPS, B_DEV).astype(jnp.int32)


def set_ends(array, stream_key, least, largest):
    longest = array.shape.index(max(array.shape))
    spots = []
    for shift in (0, 1):
        where = [jax.random.randint(jax.random.fold_in(stream_key, axis), (), 0, length) for axis, length in enumerate(array.shape)]
        where[longest] = (where[longest] + shift) % array.shape[longest]
        spots.append(tuple(where))
    return array.at[spots[0]].set(least).at[spots[1]].set(largest)


def steps_of(own_key, extent, pieces, least, top_value):
    level, own = 1.0, jax.random.fold_in(own_key, 6)
    for axis_at, blocks in pieces:
        draws = jnp.exp(jax.random.uniform(jax.random.fold_in(own, axis_at), (blocks,), jnp.float32, least / len(pieces), top_value / len(pieces)))
        level = level * jnp.repeat(draws, extent[axis_at] // blocks).reshape([-1 if axis == axis_at else 1 for axis in range(len(extent))])
    return level


def scatter_about(rng, dims, width, bound, cuts=(), kind=jnp.bfloat16):
    loudness = steps_of(rng, dims, cuts, -0.22, 0.18) if cuts else 1.0
    result = jax.random.normal(rng, dims, jnp.float32) * width * loudness
    return jnp.minimum(jnp.maximum(result, -bound), bound).astype(kind)


def setup_inputs(seed: int = 0) -> dict:
    arg_keys = jax.random.split(jax.random.key(seed), 19)
    hidden_in = scatter_about(arg_keys[0], (B, D), 1.0, 6.0, ((0, 32),))
    attn_gain = jnp.clip(1.0 + 0.1 * jax.random.normal(arg_keys[1], (D,), jnp.float32), 0.5, 1.5)
    w_qkv = set_ends(jax.random.randint(arg_keys[2], (D // 4, QKV), -2147483648, 2147483647), jax.random.fold_in(arg_keys[2], 1), -2147483648, 2147483646).astype(jnp.int32)
    qkv_scale = jnp.clip(jnp.exp(math.log(0.00041926274) - 1.32175583 * jax.random.uniform(arg_keys[3], (QKV,), jnp.float32) ** steps_of(arg_keys[3], (QKV,), ((0, 16),), -0.2, 0.2)), 0.0001118034, 0.00041926274)
    q_gain = jnp.clip(1.0 + 0.15 * jax.random.normal(arg_keys[4], (HEAD_SIZE,), jnp.float32), 0.25, 1.75)
    k_gain = jnp.clip(1.0 + 0.18 * jax.random.normal(arg_keys[5], (HEAD_SIZE,), jnp.float32), 0.1, 1.9)
    key_cache = draw_key_cache(jax.random.fold_in(arg_keys[18], 71), 0)
    value_cache = scatter_about(arg_keys[7], (NGROUPS, B_DEV, CACHE_POSITIONS, KEY_COLUMNS), 1.5, 9.0, ((0, 32), (1, 16)))
    lengths = draw_lengths(jax.random.fold_in(arg_keys[18], 71), 0)
    w_out = set_ends(jax.random.randint(arg_keys[9], (QUERY_COLUMNS // 4, D), -2147483648, 2147483647), jax.random.fold_in(arg_keys[9], 1), -2147483648, 2147483646).astype(jnp.int32)
    out_scale = jnp.clip(jnp.exp(jax.random.uniform(arg_keys[10], (D,), jnp.float32, math.log(0.0003125), math.log(0.00125))), 0.0003125, 0.00125)
    mlp_gain = jnp.clip(1.0 + 0.1 * jax.random.normal(arg_keys[11], (D,), jnp.float32), 0.5, 1.5)
    w_gate = set_ends(jax.random.randint(arg_keys[12], (D // 4, FFW), -2147483648, 2147483647), jax.random.fold_in(arg_keys[12], 1), -2147483648, 2147483646).astype(jnp.int32)
    w_up = set_ends(jax.random.randint(arg_keys[13], (D // 4, FFW), -2147483648, 2147483647), jax.random.fold_in(arg_keys[13], 1), -2147483648, 2147483646).astype(jnp.int32)
    gate_scale = jnp.clip(jnp.exp(math.log(0.00041926274) - 1.32175583 * jax.random.uniform(arg_keys[14], (FFW,), jnp.float32) ** steps_of(arg_keys[14], (FFW,), ((0, 16),), -0.2, 0.2)), 0.0001118034, 0.00041926274)
    up_scale = jnp.clip(jnp.exp(math.log(0.00041926274) - 1.32175583 * jax.random.uniform(arg_keys[15], (FFW,), jnp.float32) ** steps_of(arg_keys[15], (FFW,), ((0, 16),), -0.2, 0.2)), 0.0001118034, 0.00041926274)
    w_down = set_ends(jax.random.randint(arg_keys[16], (FFW // 4, D), -2147483648, 2147483647), jax.random.fold_in(arg_keys[16], 1), -2147483648, 2147483646).astype(jnp.int32)
    down_scale = jnp.clip(jnp.exp(jax.random.uniform(arg_keys[17], (D,), jnp.float32, math.log(0.00013258251), math.log(0.00053033006))), 0.00013258251, 0.00053033006)
    return dict(hidden_in=hidden_in, attn_gain=attn_gain, w_qkv=w_qkv, qkv_scale=qkv_scale, q_gain=q_gain, k_gain=k_gain, key_cache=key_cache, value_cache=value_cache, lengths=lengths, w_out=w_out, out_scale=out_scale, mlp_gain=mlp_gain, w_gate=w_gate, w_up=w_up, gate_scale=gate_scale, up_scale=up_scale, w_down=w_down, down_scale=down_scale)


norm_epsilon = 1e-06
rope_base = 1000000.0

def unpack_bytes(packed, byte_index):
    return jnp.right_shift(jnp.left_shift(packed, 24 - 8 * byte_index), 24)

def byte_product(activations, packed):
    products = [jnp.dot(activations[:, byte_index::4], unpack_bytes(packed, byte_index).astype(jnp.bfloat16), preferred_element_type=jnp.float32) for byte_index in range(4)]
    return products[0] + products[1] + products[2] + products[3]

def normalize_rows(values, gain_row):
    return values * lax.rsqrt(lax.optimization_barrier(jnp.mean(values * values, axis=-1, keepdims=True)) + norm_epsilon) * gain_row

def rotary_embed(values, positions):
    half_dim = values.shape[-1] // 2
    freq_index = jnp.arange(half_dim, dtype=jnp.float32)
    inverse = jnp.exp(freq_index * (-math.log(rope_base) / half_dim))
    angles = positions.astype(jnp.float32)[:, None] * inverse[None, :]
    cosine = jnp.cos(angles)[:, None, :]
    sine_part = jnp.sin(angles)[:, None, :]
    lower_half = values[..., :half_dim]
    upper_half = values[..., half_dim:]
    return jnp.concatenate([lower_half * cosine - upper_half * sine_part, upper_half * cosine + lower_half * sine_part], axis=-1)

def attention_rows(query_key_value, q_gain, k_gain, stored_keys, stored_values, seq_lengths):
    count_of_rows = query_key_value.shape[0]
    query_matrix = query_key_value[:, :QUERY_COLUMNS].astype(jnp.float32).reshape(count_of_rows, QUERY_HEADS, HEAD_SIZE)
    incoming_keys = query_key_value[:, QUERY_COLUMNS:QUERY_COLUMNS + KEY_COLUMNS].astype(jnp.float32).reshape(count_of_rows, KEY_VALUE_HEADS, HEAD_SIZE)
    incoming_values = query_key_value[:, QUERY_COLUMNS + KEY_COLUMNS:].reshape(count_of_rows, KEY_VALUE_HEADS, HEAD_SIZE)
    query_matrix = rotary_embed(normalize_rows(query_matrix, q_gain), seq_lengths).astype(jnp.bfloat16)
    incoming_keys = rotary_embed(normalize_rows(incoming_keys, k_gain), seq_lengths).astype(jnp.bfloat16)
    query_groups = query_matrix.astype(jnp.float32).reshape(count_of_rows, KEY_VALUE_HEADS, QUERY_HEADS // KEY_VALUE_HEADS, HEAD_SIZE)
    key_slices = stored_keys.astype(jnp.float32).reshape(count_of_rows, CACHE_POSITIONS, KEY_VALUE_HEADS, HEAD_SIZE)
    value_slices = stored_values.astype(jnp.float32).reshape(count_of_rows, CACHE_POSITIONS, KEY_VALUE_HEADS, HEAD_SIZE)
    logit_scale = 1.0 / math.sqrt(HEAD_SIZE)
    scores = jnp.einsum('bkgd,bpkd->bkgp', query_groups, key_slices) * logit_scale
    live_mask = jnp.arange(CACHE_POSITIONS, dtype=jnp.int32)[None, :] < seq_lengths[:, None]
    scores = jnp.where(live_mask[:, None, None, :], scores, -jnp.inf)
    self_score = jnp.einsum('nufi,nui->nuf', query_groups, incoming_keys.astype(jnp.float32)) * logit_scale
    row_max = jnp.maximum(lax.optimization_barrier(jnp.max(scores, axis=-1)), self_score)
    soft_weights = jnp.exp(scores - row_max[..., None])
    own_weight = jnp.exp(self_score - row_max)
    denominator = lax.optimization_barrier(jnp.sum(soft_weights, axis=-1)) + own_weight
    soft_low = lax.optimization_barrier(soft_weights.astype(jnp.bfloat16)).astype(jnp.float32)
    own_low = lax.optimization_barrier(own_weight.astype(jnp.bfloat16)).astype(jnp.float32)
    numerator = jnp.einsum('bkgp,bpkd->bkgd', soft_low, value_slices) + own_low[..., None] * incoming_values.astype(jnp.float32)[:, :, None, :]
    return (numerator / denominator[..., None]).reshape(count_of_rows, QUERY_COLUMNS).astype(jnp.bfloat16)

def reference(hidden_in, attn_gain, w_qkv, qkv_scale, q_gain, k_gain, key_cache, value_cache, lengths, w_out, out_scale, mlp_gain, w_gate, w_up, gate_scale, up_scale, w_down, down_scale):
    total_rows = hidden_in.shape[0]
    residual = hidden_in.astype(jnp.float32)
    normed = normalize_rows(residual, attn_gain).astype(jnp.bfloat16)
    query_key_value = (byte_product(normed, w_qkv) * qkv_scale).astype(jnp.bfloat16)
    flat_lengths = lengths.reshape(total_rows)
    heads_out = attention_rows(query_key_value, q_gain, k_gain, key_cache.reshape(total_rows, CACHE_POSITIONS, KEY_COLUMNS), value_cache.reshape(total_rows, CACHE_POSITIONS, KEY_COLUMNS), flat_lengths)
    middle = (residual + byte_product(heads_out, w_out) * out_scale).astype(jnp.bfloat16)
    normed_mlp = normalize_rows(middle.astype(jnp.float32), mlp_gain).astype(jnp.bfloat16)
    gate_value = byte_product(normed_mlp, w_gate) * gate_scale
    up_value = byte_product(normed_mlp, w_up) * up_scale
    activated = (jax.nn.silu(gate_value) * up_value).astype(jnp.bfloat16)
    down_value = byte_product(activated, w_down) * down_scale
    return (middle.astype(jnp.float32) + down_value).astype(jnp.bfloat16)
```

```python
import math

import jax
import jax.numpy as jnp
from jax import lax
from jax.experimental import pallas as pl
from jax.experimental.pallas import tpu as pltpu
from jax.sharding import PartitionSpec as P

D = 5120
HALF = 2560
HEADS = 32
KV = 4
HEAD = 128
ROWS = 64
ALL = 256
YS = 8
ZS = 8
HID = 200
PAD = 256
EPS = 1e-06
ROPE = 1000000.0
MESH = pl.DeviceIdType.MESH
F32 = jnp.float32
BF = jnp.bfloat16
NEAR = (0, 1, 7, 2, 6, 3, 5, 4)


def mo(value, k):
    return pl.multiple_of(value, k)


def byte_of(words, k):
    return jnp.right_shift(jnp.left_shift(words, 24 - 8 * k), 24).astype(F32).astype(BF)


def one_hot(n, used, group, stride):
    row = lax.broadcasted_iota(jnp.int32, (n, n), 0)
    col = lax.broadcasted_iota(jnp.int32, (n, n), 1)
    shift = stride.bit_length() - 1
    k, r = jnp.right_shift(col, shift), jnp.bitwise_and(col, stride - 1)
    return jnp.where((row == 4 * r + k) & (r < used), 1.0, 0.0).astype(BF)


def dot(a, b):
    return jnp.dot(a, b, preferred_element_type=F32)


def kernel(
    hid, again, wq, qscale, gains, kc, vc, ctab, stab, ltab, wout, oscale, mgain, gu4, gsc, dn4, dscale,
    out,
    stage, bsend, brecv, qs, vs, hsend, hrecv, wo_r, wo, pm, rs, X, xk, gub, dnp, dnb, wg, wd, pd, sib,
    pre, spre, splain, smerge, rplain, rmerge, u, yr,
    w1s, w1r, wos, wor, zs, zr, bs, br, hs, hr, rss, rsr, fys, fyr, fxs, fxr, fqs, fqr, fss, fsr,
    sbs, sbr, xps, xpr, xms, xmr, yss, ysr,
):
    z = lax.axis_index("grp")
    tp = lax.axis_index("tp")
    src = lax.axis_index("src")
    xl, y = tp // YS, tp % YS
    xh, core = src // 2, src % 2
    x = xh * 2 + xl

    def at_x(xx, cc):
        return {"tp": (xx % 2) * YS + y, "src": (xx // 2) * 2 + cc}

    xp, xm, xo = (x + 1) % 4, (x + 3) % 4, (x + 2) % 4
    PLUS, MINUS = at_x(xp, core), at_x(xm, core)
    SIB = {"src": xh * 2 + 1 - core}
    ZP, ZM = {"grp": (z + 1) % ZS}, {"grp": (z + ZS - 1) % ZS}

    def rcopy(a, b, s, r, to):
        return pltpu.make_async_remote_copy(
            src_ref=a, dst_ref=b, send_sem=s, recv_sem=r, device_id=to, device_id_type=MESH
        )

    barrier = pltpu.get_barrier_semaphore()

    def greet_tp(d, _):
        pl.semaphore_signal(barrier, inc=1, device_id={"tp": (tp + d) % 16}, device_id_type=MESH)
        return 0

    def greet_src(d, _):
        pl.semaphore_signal(barrier, inc=1, device_id={"src": (src + d) % 4}, device_id_type=MESH)
        return 0

    lax.fori_loop(1, 16, greet_tp, 0)
    lax.fori_loop(1, 4, greet_src, 0)
    across = {"tp": (1 - xl) * YS + y, "src": (1 - xh) * 2 + core}
    for to in (across, ZP, ZM):
        pl.semaphore_signal(barrier, inc=1, device_id=to, device_id_type=MESH)
    pl.semaphore_wait(barrier, 21)

    def w1_gu(d):
        s2 = (src + d) % 4
        return rcopy(
            gu4.at[s2], gub.at[0, pl.ds(mo(src * 40, 8), 40), :], w1s.at[0, d], w1r.at[0, src], {"src": s2}
        )

    def w1_dn(d):
        s2 = (src + d) % 4
        return rcopy(dn4.at[s2], dnp.at[src], w1s.at[1, d], w1r.at[1, src], {"src": s2})

    for d in (2, 3, 1):
        w1_gu(d).start()
        w1_dn(d).start()
    wo_side = (x + 1 + 2 * core) % 4
    wo_copy = rcopy(
        wout.at[:, pl.ds(mo((1 - xl) * HALF, 128), HALF)], wo_r, wos, wor, at_x(wo_side, core)
    )
    wo_copy.start()
    gub[0, pl.ds(mo(src * 40, 8), 40), :] = gu4[src]
    dnp[src] = dn4[src]

    total = jnp.zeros((ROWS, 1), F32)
    for g in range(10):
        v = hid[:, g * 512 : (g + 1) * 512].astype(F32)
        total = total + jnp.sum(v * v, axis=1, keepdims=True)
    rms = lax.rsqrt(total * (1.0 / D) + EPS)
    P512 = one_hot(512, 128, 4, 128)
    stage[...] = jnp.broadcast_to(rms, (ROWS, 384))

    def qkv_group(g, acc):
        at = pl.ds(mo(g * 512, 512), 512)
        r = stage[:, 0:1]
        v = (hid[:, at].astype(F32) * r * again[:, at]).astype(BF)
        v = dot(v, P512).astype(BF)
        w = wq[pl.ds(mo(g * 128, 128), 128), :]
        for k in range(4):
            acc = acc + dot(v[:, k * 128 : (k + 1) * 128], byte_of(w, k))
        return acc

    acc = lax.fori_loop(0, 10, qkv_group, jnp.zeros((ROWS, 320), F32))
    qkv = (acc * qscale[...]).astype(BF).astype(F32)
    stage[...] = jnp.zeros((ROWS, 384), F32)
    stage[:, :320] = qkv
    odd_y = (y % 2) == 1
    placed = stage[...]
    placed = jnp.where(odd_y, pltpu.roll(placed, 64, 1), placed)
    for t in range(16):
        bsend[t] = placed[4 * t : 4 * t + 4, :]

    def b_copy(d):
        to = (tp + d) % 16
        return rcopy(bsend.at[to], brecv.at[tp], bs.at[to], br.at[tp], {"tp": to})

    def b_in(d):
        frm = (tp + d) % 16
        return rcopy(bsend.at[frm], brecv.at[frm], bs.at[frm], br.at[frm], {"tp": frm})

    def start_b(d, _):
        b_copy(d).start()
        return 0

    def wait_b(d, _):
        b_in(d).wait_recv()
        return 0

    lax.fori_loop(1, 16, start_b, 0)
    brecv[pl.ds(tp, 1)] = bsend[pl.ds(tp, 1)]

    def w1_in(j, d):
        s2 = (src + d) % 4
        if j == 0:
            return rcopy(gu4.at[s2], gub.at[0, pl.ds(mo(s2 * 40, 8), 40), :], w1s.at[0, d], w1r.at[0, s2], {"src": s2})
        return rcopy(dn4.at[s2], dnp.at[s2], w1s.at[1, d], w1r.at[1, s2], {"src": s2})

    for d in (1, 2, 3):
        w1_in(0, d).wait_recv()
        w1_in(1, d).wait_recv()
    dnb[0] = jnp.concatenate([dnp[0], dnp[1], dnp[2], dnp[3]], axis=1)

    def ring(step, way):
        a = step - 1 if way == 0 else (9 - step) % 8
        b = step if way == 0 else 8 - step
        to = ZP if way == 0 else ZM
        if step == 4:
            g_at, d_at = (slice(0, 80), slice(0, 32)) if way == 0 else (slice(80, 160), slice(32, 56))
        else:
            g_at, d_at = slice(0, 160), slice(0, 56)
        one = rcopy(gub.at[a, g_at, :], gub.at[b, g_at, :], zs.at[way, step - 1, 0], zr.at[way, step - 1, 0], to)
        two = rcopy(dnb.at[a, d_at, :], dnb.at[b, d_at, :], zs.at[way, step - 1, 1], zr.at[way, step - 1, 1], to)
        return one, two

    def ring_start(step):
        for way in (0, 1):
            for c in ring(step, way):
                c.start()

    def ring_wait(step):
        for way in (0, 1):
            for c in ring(step, way):
                c.wait_recv()

    def unpack(slot):
        zz = (z + ZS - slot) % ZS

        def rows(i, _):
            w = gub[slot, pl.ds(mo(i * 32, 32), 32), :]
            for k in range(4):
                wg[k, pl.ds(mo(zz * 160 + i * 32, 32), 32), :] = byte_of(w, k)
            return 0

        lax.fori_loop(0, 5, rows, 0)
        w = dnb[slot]
        for k in range(4):
            wd[k * 64 : k * 64 + 56, pl.ds(mo(zz * 640, 128), 640)] = byte_of(w, k)

    ring_start(1)
    wd[...] = jnp.zeros(wd.shape, BF)
    unpack(0)
    own_words = wout.at[:, pl.ds(mo(xl * HALF, 128), HALF)]

    def unpack_wo(ref, base):
        def cols(i, _):
            at = pl.ds(mo(i * 640, 128), 640)
            for hl in range(2):
                w = ref[hl * 32 : hl * 32 + 32, at]
                for k in range(4):
                    wo[pl.ds(mo(base + hl * 128 + k * 32, 32), 32), at] = byte_of(w, k)
            return 0

        lax.fori_loop(0, 4, cols, 0)

    unpack_wo(own_words, xl * 256)

    lax.fori_loop(1, 16, wait_b, 0)
    lane = lax.broadcasted_iota(jnp.int32, (4, HEAD), 1)
    for p in range(8):
        even, odd = brecv[2 * p], brecv[2 * p + 1]
        pieces = (
            even[:, 0:128],
            even[:, 128:256],
            jnp.where(lane < 64, even[:, 256:384], odd[:, 0:128]),
            odd[:, 128:256],
            odd[:, 256:384],
        )
        for j, piece in enumerate(pieces):
            h = 5 * p + j
            if h < HEADS:
                qs[4 * h : 4 * h + 4, :] = piece
            elif h < HEADS + KV:
                at = 128 + 8 * (h - HEADS)
                qs[at : at + 4, :] = piece
                qs[at + 4 : at + 8, :] = piece
            else:
                at = 8 * (h - HEADS - KV)
                vs[at : at + 4, :] = piece
                vs[at + 4 : at + 8, :] = piece
    v = qs[...]
    v = v * lax.rsqrt(jnp.mean(v * v, axis=1, keepdims=True) + EPS)
    row = lax.broadcasted_iota(jnp.int32, (160, HEAD), 0)
    v = v * jnp.where(row < 128, gains[0:1, :], gains[1:2, :])
    turned = pltpu.roll(v, 64, 1)
    v = v.reshape(20, 8, HEAD) * ctab[...][None] + turned.reshape(20, 8, HEAD) * stab[...][None]
    v = v.reshape(160, HEAD).astype(BF)
    scale = 1.0 / math.sqrt(HEAD)
    seq = jnp.bitwise_and(lax.broadcasted_iota(jnp.int32, (32, HEAD), 0), 3)
    place = lax.broadcasted_iota(jnp.int32, (8, HEAD), 1)
    live = jnp.where(place < ltab[...], 1.0, 0.0)
    live = jnp.broadcast_to(live[None], (4, 8, HEAD)).reshape(32, HEAD) > 0.5
    heads = []
    for g in range(KV):
        q = v[32 * g : 32 * g + 32]
        newk = v[128 + 8 * g : 136 + 8 * g].astype(F32)
        own = jnp.sum((q.astype(F32).reshape(4, 8, HEAD) * newk[None]).reshape(32, HEAD), axis=1, keepdims=True)
        own = own * scale
        s = jnp.zeros((32, HEAD), F32)
        for b in range(4):
            sb = lax.dot_general(
                q, kc[b, :, g * 128 : (g + 1) * 128], (((1,), (1,)), ((), ())), preferred_element_type=F32
            )
            s = jnp.where(seq == b, sb, s)
        s = jnp.where(live, s * scale, -jnp.inf)
        top = jnp.maximum(jnp.max(s, axis=1, keepdims=True), own)
        e = jnp.exp(s - top)
        own_e = jnp.exp(own - top)
        den = jnp.sum(e, axis=1, keepdims=True) + own_e
        newv = vs[8 * g : 8 * g + 8, :]
        low = own_e.astype(BF).astype(F32)
        num = (low.reshape(4, 8, 1) * newv[None]).reshape(32, HEAD)
        for b in range(4):
            eb = jnp.where(seq == b, e, 0.0).astype(BF)
            num = num + dot(eb, vc[b, :, g * 128 : (g + 1) * 128])
        heads.append(num / den)
    for yy in range(YS):
        g, at = yy // 4, 8 * (yy % 4)
        hsend[yy] = jnp.concatenate([heads[g][at : at + 8], heads[g + 2][at : at + 8]], axis=0).astype(BF)

    def h_slot(t):
        return hrecv.at[pl.ds(mo(t * 16, 16), 16), :]

    def h_copy(d):
        to = (tp + d) % 16
        return rcopy(hsend.at[to % YS], h_slot(tp), hs.at[to], hr.at[tp], {"tp": to})

    def start_h(d, _):
        h_copy(d).start()
        return 0

    def wait_h(d, _):
        frm = (tp + d) % 16
        rcopy(hsend.at[frm % YS], h_slot(frm), hs.at[frm], hr.at[frm], {"tp": frm}).wait_recv()
        return 0

    lax.fori_loop(1, 16, start_h, 0)
    hrecv[pl.ds(mo(tp * 16, 16), 16), :] = hsend[y]

    wo_copy.wait_recv()
    unpack_wo(wo_r, (1 - xl) * 256)

    lax.fori_loop(1, 16, wait_h, 0)
    P128 = one_hot(128, 32, 4, 32)
    got = hrecv[...]
    t = lax.broadcasted_iota(jnp.int32, (ROWS, 256), 0)
    c = lax.broadcasted_iota(jnp.int32, (ROWS, 256), 1)
    zcat = []
    for hl in range(4):
        want = jnp.right_shift(t, 2) * 16 + hl * 4 + jnp.bitwise_and(t, 3)
        pick = jnp.where(c == want, 1.0, 0.0).astype(BF)
        zcat.append(dot(dot(pick, got).astype(BF), P128).astype(BF))
    zcat = jnp.concatenate(zcat, axis=1)

    def part(yy):
        return pl.ds(mo(32 * (yy // 4), 32), 32), pl.ds(mo(640 * (yy % 4), 128), 640)

    for cb in range(4):
        pm[:, cb * 640 : cb * 640 + 640] = dot(zcat, wo[:, cb * 640 : cb * 640 + 640]).astype(BF)

    def r_copy(d):
        to = (y + d) % YS
        a, b = part(to)
        return rcopy(pm.at[a, b], rs.at[y], rss.at[to], rsr.at[y], {"tp": xl * YS + to})

    def start_r(d, _):
        r_copy(d).start()
        return 0

    def wait_r(d, _):
        frm = (y + d) % YS
        a, b = part(frm)
        rcopy(pm.at[a, b], rs.at[frm], rss.at[frm], rsr.at[frm], {"tp": xl * YS + frm}).wait_recv()
        return 0

    lax.fori_loop(1, YS, start_r, 0)
    a, b = part(y)
    rs[y] = pm[a, b]

    ring_wait(1)
    ring_start(2)
    unpack(1)
    unpack(7)

    lax.fori_loop(1, YS, wait_r, 0)
    mid = rs[0].astype(F32)
    for i in range(1, YS):
        mid = mid + rs[i].astype(F32)
    col0 = mo(xl * HALF + 640 * (y % 4), 128)
    mid = hid[a, pl.ds(col0, 640)].astype(F32) + mid * oscale[:, pl.ds(col0, 640)]
    X[pl.ds(mo(src * 64 + 32 * (y // 4), 32), 32), pl.ds(col0, 640)] = mid.astype(BF)

    def blk(xx, cc, yy):
        r0 = ((xx // 2) * 2 + cc) * 64 + 32 * (yy // 4)
        c0 = (xx % 2) * HALF + 640 * (yy % 4)
        return X.at[pl.ds(mo(r0, 32), 32), pl.ds(mo(c0, 128), 640)]

    def fy_copy(d):
        to = (y + d) % YS
        return rcopy(blk(x, core, y), blk(x, core, y), fys.at[to], fyr.at[y], {"tp": xl * YS + to})

    for d in NEAR[1:]:
        fy_copy(d).start()

    def fx_copy(way, i):
        b0 = blk(x, core, (y + i) % YS)
        return rcopy(b0, b0, fxs.at[way, i], fxr.at[way, i], PLUS if way == 0 else MINUS)

    def fx_in(way, i):
        b0 = blk(xm if way == 0 else xp, core, (y + i) % YS)
        return rcopy(b0, b0, fxs.at[way, i], fxr.at[way, i], MINUS if way == 0 else PLUS)

    def fq_copy(i):
        way = i % 2
        b0 = blk(xm if way == 0 else xp, core, (y + i) % YS)
        return rcopy(b0, b0, fqs.at[i], fqr.at[i], PLUS if way == 0 else MINUS)

    def fq_in(i):
        b0 = blk(xo, core, (y + i) % YS)
        return rcopy(b0, b0, fqs.at[i], fqr.at[i], MINUS if i % 2 == 0 else PLUS)

    froms = (x, xm, xp, xo)

    def fs_copy(j, i):
        b0 = blk(froms[j], core, (y + i) % YS)
        return rcopy(b0, b0, fss.at[j, i], fsr.at[j, i], SIB)

    def fs_in(j, i):
        b0 = blk(froms[j], 1 - core, (y + i) % YS)
        return rcopy(b0, b0, fss.at[j, i], fsr.at[j, i], SIB)

    for i in NEAR:
        yy = (y + i) % YS
        if i:
            b0 = blk(x, core, yy)
            rcopy(b0, b0, fys.at[yy], fyr.at[yy], {"tp": xl * YS + yy}).wait_recv()
        fx_copy(0, i).start()
        fx_copy(1, i).start()
        fs_copy(0, i).start()
    ring_wait(2)
    ring_start(3)
    for i in NEAR:
        fx_in(0, i).wait_recv()
        fx_in(1, i).wait_recv()
        fq_copy(i).start()
        fs_copy(1, i).start()
        fs_copy(2, i).start()
    unpack(2)
    unpack(6)
    ring_wait(3)
    ring_start(4)
    unpack(3)
    unpack(5)
    for i in NEAR:
        fq_in(i).wait_recv()
        fs_copy(3, i).start()
    for j in range(4):
        for i in NEAR:
            fs_in(j, i).wait_recv()

    P512 = one_hot(512, 128, 4, 128)

    def norm_rows(m, _):
        at = pl.ds(mo(m * 64, 64), 64)
        total = jnp.zeros((64, 1), F32)
        for g in range(10):
            v = X[at, g * 512 : (g + 1) * 512].astype(F32)
            total = total + jnp.sum(v * v, axis=1, keepdims=True)
        rms = lax.rsqrt(total * (1.0 / D) + EPS)
        for g in range(10):
            v = X[at, g * 512 : (g + 1) * 512].astype(F32)
            v = (v * rms * mgain[:, g * 512 : (g + 1) * 512]).astype(BF)
            v = dot(v, P512).astype(BF)
            for k in range(4):
                xk[k, at, g * 128 : (g + 1) * 128] = v[:, k * 128 : (k + 1) * 128]
        return 0

    lax.fori_loop(0, 4, norm_rows, 0)
    ring_wait(4)
    unpack(4)
    both = dot(xk[0], wg[0])
    for k in range(1, 4):
        both = both + dot(xk[k], wg[k])
    both = both * gsc[pl.ds(src, 1), :]
    gate, up = both[:, :PAD], both[:, PAD:]
    act = (gate / (1.0 + jnp.exp(-gate)) * up).astype(BF)
    act = dot(act, one_hot(PAD, HID // 4, 4, 64)).astype(BF)
    xk[0, :, :PAD] = act

    def down(n, _):
        at = pl.ds(mo(n * 640, 128), 640)
        pd[:, at] = dot(xk[0, :, :PAD], wd[:, at]).astype(BF)
        return 0

    lax.fori_loop(0, 8, down, 0)

    def slab_rows(h, cc):
        return pl.ds(mo((h * 2 + cc) * 64, 64), 64)

    def sb_copy(h):
        return rcopy(pd.at[slab_rows(h, 1 - core), :], sib.at[h], sbs.at[h], sbr.at[h], SIB)

    for h in (0, 1):
        sb_copy(h).start()
    for h in (0, 1):
        sb_copy(h).wait_recv()

    def slab(xx, half):
        at = pl.ds(mo((xx % 2) * HALF + half * 1280, 128), 1280)
        return pd[slab_rows(xx // 2, core), at].astype(F32) + sib[xx // 2, :, at].astype(F32)

    sides = (PLUS, MINUS)
    nexts = (xp, xm)
    pre_copies = [rcopy(spre.at[w], pre.at[w], xps.at[w], xpr.at[w], sides[w]) for w in (0, 1)]
    plain = [rcopy(splain.at[w], rplain.at[w], xms.at[w, 0], xmr.at[w, 0], sides[w]) for w in (0, 1)]
    merge = [rcopy(smerge.at[w], rmerge.at[w], xms.at[w, 1], xmr.at[w, 1], sides[w]) for w in (0, 1)]
    for w in (0, 1):
        spre[w] = slab(xo, w).astype(BF)
        pre_copies[w].start()
    for w in (0, 1):
        splain[w] = slab(nexts[w], 1 - w).astype(BF)
        plain[w].start()
    for w in (0, 1):
        pre_copies[w].wait_recv()
        smerge[w] = (slab(nexts[w], w) + pre[w].astype(F32)).astype(BF)
        merge[w].start()
    mine = [slab(x, 0), slab(x, 1)]
    for w in (0, 1):
        plain[w].wait_recv()
        mine[1 - w] = mine[1 - w] + rplain[w].astype(F32)
    for w in (0, 1):
        merge[w].wait_recv()
        mine[w] = mine[w] + rmerge[w].astype(F32)
    u[:, :1280] = mine[0].astype(BF)
    u[:, 1280:] = mine[1].astype(BF)

    def window(yy):
        return pl.ds(mo(320 * yy - 64 * (yy % 2), 128), 384)

    def y_copy(d):
        to = (y + d) % YS
        return rcopy(u.at[:, window(to)], yr.at[y], yss.at[to], ysr.at[y], {"tp": xl * YS + to})

    def y_in(d):
        frm = (y + d) % YS
        return rcopy(u.at[:, window(frm)], yr.at[frm], yss.at[frm], ysr.at[frm], {"tp": xl * YS + frm})

    for d in NEAR[1:]:
        y_copy(d).start()
    yr[y] = u[:, window(y)]
    for d in NEAR[1:]:
        y_in(d).wait_recv()
    last = yr[0].astype(F32)
    for i in range(1, YS):
        last = last + yr[i].astype(F32)
    at = pl.ds(mo(xl * HALF + 320 * y - 64 * (y % 2), 128), 384)
    last = X[pl.ds(mo(src * 64, 64), 64), at].astype(F32) + last * dscale[:, at]
    last = jnp.where(odd_y, pltpu.roll(last, 320, 1), last)
    out[...] = last[:, :320].astype(BF)

    for d in (1, 2, 3):
        w1_gu(d).wait_send()
        w1_dn(d).wait_send()
    wo_copy.wait_send()
    for step in (1, 2, 3, 4):
        for way in (0, 1):
            for c in ring(step, way):
                c.wait_send()

    def sent_tp(d, _):
        b_copy(d).wait_send()
        h_copy(d).wait_send()
        return 0

    def sent_y(d, _):
        r_copy(d).wait_send()
        fy_copy(d).wait_send()
        y_copy(d).wait_send()
        return 0

    lax.fori_loop(1, 16, sent_tp, 0)
    lax.fori_loop(1, YS, sent_y, 0)
    for i in range(YS):
        fx_copy(0, i).wait_send()
        fx_copy(1, i).wait_send()
        fq_copy(i).wait_send()
        for j in range(4):
            fs_copy(j, i).wait_send()
    for w in (0, 1):
        sb_copy(w).wait_send()
        pre_copies[w].wait_send()
        plain[w].wait_send()
        merge[w].wait_send()


def local(
    hidden_in, attn_gain, w_qkv, qkv_scale, q_gain, k_gain, key_cache, value_cache, lengths, w_out, out_scale,
    mlp_gain, w_gate, w_up, gate_scale, up_scale, w_down, down_scale,
):
    def quarters(w):
        return jnp.pad(w.reshape(40, 4, HID), ((0, 0), (0, 0), (0, PAD - HID)))

    gu4 = jnp.concatenate([quarters(w_gate), quarters(w_up)], axis=2).transpose(1, 0, 2)
    dn4 = jnp.pad(w_down.reshape(4, 50, 160), ((0, 0), (0, 6), (0, 0)))

    def padded(v):
        return jnp.pad(v.reshape(4, HID), ((0, 0), (0, PAD - HID)))

    gsc = jnp.concatenate([padded(gate_scale), padded(up_scale)], axis=1)
    freq = jnp.arange(64, dtype=F32)
    inverse = jnp.exp(freq * (-math.log(ROPE) / 64))
    angle = lengths[0].astype(F32)[:, None] * inverse[None, :]
    cos, sin = jnp.cos(angle), jnp.sin(angle)
    ctab = jnp.tile(jnp.concatenate([cos, cos], axis=1), (2, 1))
    stab = jnp.tile(jnp.concatenate([-sin, sin], axis=1), (2, 1))
    ltab = jnp.broadcast_to(jnp.tile(lengths[0], 2)[:, None], (8, HEAD))
    gains = jnp.stack([q_gain, k_gain])
    V, S = pltpu.VMEM, pltpu.SemaphoreType.DMA
    scratch = [
        V((ROWS, 384), F32), V((16, 4, 384), F32), V((16, 4, 384), F32), V((160, HEAD), F32), V((32, HEAD), F32),
        V((YS, 16, HEAD), BF), V((256, HEAD), BF), V((64, HALF), jnp.int32), V((512, HALF), BF), V((ROWS, HALF), BF),
        V((YS, 32, 640), BF), V((ALL, D), BF), V((4, ALL, 1280), BF), V((ZS, 160, 512), jnp.int32),
        V((4, 56, 160), jnp.int32), V((ZS, 56, 640), jnp.int32), V((4, 1280, 512), BF), V((256, D), BF),
        V((ALL, D), BF), V((2, ROWS, D), BF),
        V((2, ROWS, 1280), BF), V((2, ROWS, 1280), BF), V((2, ROWS, 1280), BF), V((2, ROWS, 1280), BF),
        V((2, ROWS, 1280), BF), V((2, ROWS, 1280), BF), V((ROWS, HALF), BF), V((YS, ROWS, 384), BF),
        S((2, 4)), S((2, 4)), S, S, S((2, 4, 2)), S((2, 4, 2)), S((16,)), S((16,)), S((16,)), S((16,)),
        S((8,)), S((8,)), S((8,)), S((8,)), S((2, 8)), S((2, 8)), S((8,)), S((8,)), S((4, 8)), S((4, 8)),
        S((2,)), S((2,)), S((2,)), S((2,)), S((2, 2)), S((2, 2)), S((8,)), S((8,)),
    ]
    return pl.pallas_call(
        kernel,
        out_shape=jax.ShapeDtypeStruct((ROWS, 320), BF),
        in_specs=[pl.BlockSpec(memory_space=pltpu.VMEM)] * 17,
        out_specs=pl.BlockSpec(memory_space=pltpu.VMEM),
        scratch_shapes=scratch,
        compiler_params=pltpu.CompilerParams(
            collective_id=0, has_side_effects=True, vmem_limit_bytes=60 * 1024 * 1024
        ),
        name="layer",
    )(
        hidden_in, attn_gain[None], w_qkv, qkv_scale[None], gains, key_cache[0], value_cache[0], ctab, stab, ltab,
        w_out, out_scale[None], mlp_gain[None], gu4, gsc, dn4, down_scale[None],
    )


def solution(mesh):
    return jax.shard_map(
        local,
        mesh=mesh,
        in_specs=(
            P(("grp", "src"), None),
            P(),
            P(None, "tp"),
            P("tp"),
            P(),
            P(),
            P(("grp", "src"), "tp", None, None),
            P(("grp", "src"), "tp", None, None),
            P(("grp", "src"), "tp"),
            P("tp", None),
            P(),
            P(),
            P(("grp", "src"), "tp"),
            P(("grp", "src"), "tp"),
            P("tp"),
            P("tp"),
            P("tp", ("grp", "src")),
            P(),
        ),
        out_specs=P(("grp", "src"), "tp"),
        check_vma=False,
    )
```

```python
import math

import jax
import jax.numpy as jnp
from jax import lax
from jax.experimental import pallas as pl
from jax.experimental.pallas import tpu as pltpu
from jax.sharding import PartitionSpec as P

D = 5120
HALF = 2560
HEADS = 32
KV = 4
HEAD = 128
ROWS = 64
ALL = 256
YS = 8
ZS = 8
HID = 200
PAD = 256
EPS = 1e-06
ROPE = 1000000.0
MESH = pl.DeviceIdType.MESH
F32 = jnp.float32
BF = jnp.bfloat16
NEAR = (0, 1, 7, 2, 6, 3, 5, 4)


def mo(value, k):
    return pl.multiple_of(value, k)


def byte_of(words, k):
    return jnp.right_shift(jnp.left_shift(words, 24 - 8 * k), 24).astype(F32).astype(BF)


def one_hot(n, used, stride):
    row = lax.broadcasted_iota(jnp.int32, (n, n), 0)
    col = lax.broadcasted_iota(jnp.int32, (n, n), 1)
    shift = stride.bit_length() - 1
    k, r = jnp.right_shift(col, shift), jnp.bitwise_and(col, stride - 1)
    return jnp.where((row == 4 * r + k) & (r < used), 1.0, 0.0).astype(BF)


def dot(a, b):
    return jnp.dot(a, b, preferred_element_type=F32)


def kernel(
    hid, again, wq_hbm, qscale, qgain, kgain, kc_hbm, vc_hbm, lens, wout, oscale, mgain, wgate, wup, gscale, uscale,
    wdown, dscale,
    out,
    wq, kc, vc, woh, p512, vec, gsc, stage, gu4, dn4, bsend, brecv, qs, vs, hsend, hrecv, wo_r, wo, pm, rs, X, xk, ssq,
    gub, dnp, dnb, dns, wg, wd, actr, pd, pre, smerge, rplain, rmerge, u, yr,
    ld, w1s, w1r, wos, wor, zs, zr, ns, nr, bs, br, hs, hr, rss, rsr, fys, fyr, fxs, fxr, fqs, fqr, fss, fsr,
    acs, acr, xps, xpr, xas, xar, xms, xmr, yss, ysr,
):
    z = lax.axis_index("grp")
    tp = lax.axis_index("tp")
    src = lax.axis_index("src")
    xl, y = tp // YS, tp % YS
    xh, core = src // 2, src % 2
    x = xh * 2 + xl

    def at_x(xx, cc):
        return {"tp": (xx % 2) * YS + y, "src": (xx // 2) * 2 + cc}

    xp, xm, xo = (x + 1) % 4, (x + 3) % 4, (x + 2) % 4
    PLUS, MINUS = at_x(xp, core), at_x(xm, core)
    SIB = {"src": xh * 2 + 1 - core}
    ZP, ZM = {"grp": (z + 1) % ZS}, {"grp": (z + ZS - 1) % ZS}

    def rcopy(a, b, s, r, to):
        return pltpu.make_async_remote_copy(
            src_ref=a, dst_ref=b, send_sem=s, recv_sem=r, device_id=to, device_id_type=MESH
        )

    load_wq = [
        pltpu.make_async_copy(wq_hbm.at[pl.ds(i * 640, 640), :], wq.at[pl.ds(i * 640, 640), :], ld.at[i]) for i in (0, 1)
    ]
    load_kc = pltpu.make_async_copy(kc_hbm.at[0], kc, ld.at[2])
    load_vc = pltpu.make_async_copy(vc_hbm.at[0], vc, ld.at[3])
    load_wo = pltpu.make_async_copy(wout.at[:, pl.ds(mo(xl * HALF, 128), HALF)], woh, ld.at[4])
    for c in load_wq:
        c.start()
    load_kc.start()
    load_vc.start()
    load_wo.start()

    barrier = pltpu.get_barrier_semaphore()

    def greet_tp(d, _):
        pl.semaphore_signal(barrier, inc=1, device_id={"tp": (tp + d) % 16}, device_id_type=MESH)
        return 0

    def greet_src(d, _):
        pl.semaphore_signal(barrier, inc=1, device_id={"src": (src + d) % 4}, device_id_type=MESH)
        return 0

    lax.fori_loop(1, 16, greet_tp, 0)
    lax.fori_loop(1, 4, greet_src, 0)
    across = {"tp": (1 - xl) * YS + y, "src": (1 - xh) * 2 + core}
    for to in (across, ZP, ZM):
        pl.semaphore_signal(barrier, inc=1, device_id=to, device_id_type=MESH)

    for s in range(4):
        piece = jnp.concatenate([wgate[:, HID * s : HID * s + HID], wup[:, HID * s : HID * s + HID]], axis=1)
        gu4[s] = piece[:, :384]
        dn4[s] = jnp.zeros((56, 256), jnp.int32)
        dn4[s, 0:50, 0:160] = wdown[50 * s : 50 * s + 50, :]
        dn4[s, 0:40, 160:176] = piece[:, 384:400]
    gub[0, pl.ds(mo(src * 40, 8), 40), :] = gu4[src]
    dnp[src] = dn4[src]
    p512[...] = one_hot(512, 128, 128)
    vec[0:1, :] = again[...][None, :]
    vec[1:2, :] = mgain[...][None, :]
    vec[2:3, :] = oscale[...][None, :]
    vec[3:4, :] = dscale[...][None, :]

    total = jnp.zeros((ROWS, 1), F32)
    for g in range(10):
        v = hid[:, g * 512 : (g + 1) * 512].astype(F32)
        total = total + jnp.sum(v * v, axis=1, keepdims=True)
    rms = lax.rsqrt(total * (1.0 / D) + EPS)
    stage[...] = jnp.broadcast_to(rms, (ROWS, 384))

    def qkv_group(g, acc):
        at = pl.ds(mo(g * 512, 512), 512)
        v = (hid[:, at].astype(F32) * stage[:, 0:1] * vec[0:1, at]).astype(BF)
        v = dot(v, p512[...]).astype(BF)
        w = wq[pl.ds(mo(g * 128, 128), 128), :]
        for k in range(4):
            acc = acc + dot(v[:, k * 128 : (k + 1) * 128], byte_of(w, k))
        return acc

    load_wq[0].wait()
    acc = lax.fori_loop(0, 5, qkv_group, jnp.zeros((ROWS, 320), F32))
    pl.semaphore_wait(barrier, 21)

    def w1_gu(d):
        s2 = (src + d) % 4
        return rcopy(
            gu4.at[s2], gub.at[0, pl.ds(mo(src * 40, 8), 40), :], w1s.at[0, d], w1r.at[0, src], {"src": s2}
        )

    def w1_dn(d):
        s2 = (src + d) % 4
        return rcopy(dn4.at[s2], dnp.at[src], w1s.at[1, d], w1r.at[1, src], {"src": s2})

    for d in (1, 2, 3):
        w1_gu(d).start()
        w1_dn(d).start()

    load_wq[1].wait()
    acc = lax.fori_loop(5, 10, qkv_group, acc)
    qkv = (acc * qscale[...][None, :]).astype(BF).astype(F32)
    stage[...] = jnp.zeros((ROWS, 384), F32)
    stage[:, :320] = qkv
    odd_y = (y % 2) == 1
    placed = stage[...]
    placed = jnp.where(odd_y, pltpu.roll(placed, 64, 1), placed)
    for t in range(16):
        bsend[t] = placed[4 * t : 4 * t + 4, :]

    def b_copy(d):
        to = (tp + d) % 16
        return rcopy(bsend.at[to], brecv.at[tp], bs.at[to], br.at[tp], {"tp": to})

    def start_b(d, _):
        b_copy(d).start()
        return 0

    def wait_b(d, _):
        frm = (tp + d) % 16
        rcopy(bsend.at[frm], brecv.at[frm], bs.at[frm], br.at[frm], {"tp": frm}).wait_recv()
        return 0

    lax.fori_loop(1, 16, start_b, 0)
    wo_side = (x + 1 + 2 * core) % 4
    wo_copy = rcopy(
        wout.at[:, pl.ds(mo((1 - xl) * HALF, 128), HALF)], wo_r, wos, wor, at_x(wo_side, core)
    )
    wo_copy.start()
    brecv[pl.ds(tp, 1)] = bsend[pl.ds(tp, 1)]

    def w1_in(d):
        s2 = (src + d) % 4
        rcopy(gu4.at[s2], gub.at[0, pl.ds(mo(s2 * 40, 8), 40), :], w1s.at[0, d], w1r.at[0, s2], {"src": s2}).wait_recv()
        rcopy(dn4.at[s2], dnp.at[s2], w1s.at[1, d], w1r.at[1, s2], {"src": s2}).wait_recv()

    def assemble(h):
        one, two = dnp[2 * h], dnp[2 * h + 1]
        dnb[0, h] = jnp.concatenate(
            [one[:, :160], two[:, :160], one[:, 160:192], two[:, 160:192]], axis=1
        )

    def ring(h, step, way):
        a = step - 1 if way == 0 else (9 - step) % 8
        b = step if way == 0 else 8 - step
        to = ZP if way == 0 else ZM
        if step == 4:
            n, off, d_at = (40, 0, slice(0, 32)) if way == 0 else (40, 40, slice(32, 56))
        else:
            n, off, d_at = 80, 0, slice(0, 56)
        at = pl.ds(mo(h * 80 + off, 8), n)
        one = rcopy(gub.at[a, at, :], gub.at[b, at, :], zs.at[h, way, step - 1, 0], zr.at[h, way, step - 1, 0], to)
        two = rcopy(
            dnb.at[a, h, d_at, :], dnb.at[b, h, d_at, :], zs.at[h, way, step - 1, 1], zr.at[h, way, step - 1, 1], to
        )
        return one, two

    def ring_start(h, step):
        for way in (0, 1):
            for c in ring(h, step, way):
                c.start()

    def ring_wait(h, step):
        for way in (0, 1):
            for c in ring(h, step, way):
                c.wait_recv()

    def to_sib(slot):
        return rcopy(dnb.at[slot], dns.at[slot], ns.at[slot], nr.at[slot], SIB)

    def hop(step):
        for h in (xh, 1 - xh):
            ring_wait(h, step)
            if step < 4:
                ring_start(h, step + 1)
        if step < 4:
            to_sib(step).start()
            to_sib(8 - step).start()
        else:
            to_sib(4).start()

    def unpack_down(ref, slot, which):
        zz = (z + ZS - slot) % ZS
        w = jnp.concatenate([ref[slot, 0, :, :320], ref[slot, 1, :, :320]], axis=1)
        for k in range(4):
            wd[which, k * 64 : k * 64 + 56, pl.ds(mo(zz * 640, 128), 640)] = byte_of(w, k)

    lane40 = lax.broadcasted_iota(jnp.int32, (40, 128), 1)

    def unpack(slot):
        zz = (z + ZS - slot) % ZS

        def rows(i, _):
            w = gub[slot, pl.ds(mo(i * 32, 32), 32), :]
            for k in range(4):
                wg[k, pl.ds(mo(zz * 160 + i * 32, 32), 32), 0:384] = byte_of(w, k)
            return 0

        lax.fori_loop(0, 5, rows, 0)
        tails = []
        for s in range(4):
            t = dnb[slot, s // 2, 0:40, 256:384]
            t = pltpu.roll(t, 64 - 32 * (s % 2), 1)
            tails.append(jnp.where(lane40 < 16, t, 0))
        tails = jnp.concatenate(tails, axis=0)
        for k in range(4):
            wg[k, pl.ds(mo(zz * 160, 32), 160), 384:512] = byte_of(tails, k)
        unpack_down(dnb, slot, 0)

    def unpack_sib(slot):
        to_sib(slot).wait_recv()
        unpack_down(dns, slot, 1)

    rcopy(
        gu4.at[0], gub.at[0, pl.ds(mo((src + 1 - 2 * core) * 40, 8), 40), :], w1s.at[0, 1],
        w1r.at[0, src + 1 - 2 * core], SIB,
    ).wait_recv()
    rcopy(dn4.at[0], dnp.at[src + 1 - 2 * core], w1s.at[1, 1], w1r.at[1, src + 1 - 2 * core], SIB).wait_recv()
    assemble(xh)
    ring_start(xh, 1)
    wd[...] = jnp.zeros(wd.shape, BF)

    def unpack_wo(ref, base):
        def cols(i, _):
            at = pl.ds(mo(i * 640, 128), 640)
            for hl in range(2):
                w = ref[hl * 32 : hl * 32 + 32, at]
                for k in range(4):
                    wo[pl.ds(mo(base + hl * 128 + k * 32, 32), 32), at] = byte_of(w, k)
            return 0

        lax.fori_loop(0, 4, cols, 0)

    load_wo.wait()
    unpack_wo(woh, xl * 256)
    far = (1 - xh) * 2
    for s2 in (far, far + 1):
        rcopy(gu4.at[0], gub.at[0, pl.ds(mo(s2 * 40, 8), 40), :], w1s.at[0, 2], w1r.at[0, s2], {"src": s2}).wait_recv()
        rcopy(dn4.at[0], dnp.at[s2], w1s.at[1, 2], w1r.at[1, s2], {"src": s2}).wait_recv()
    assemble(1 - xh)
    ring_start(1 - xh, 1)
    to_sib(0).start()
    unpack(0)
    load_kc.wait()
    load_vc.wait()
    half = lax.broadcasted_iota(jnp.int32, (8, HEAD), 1)
    pair = jnp.bitwise_and(lax.broadcasted_iota(jnp.int32, (8, HEAD), 0), 3)
    length = jnp.full((8, HEAD), lens[0, 0], jnp.int32)
    for b in range(1, 4):
        length = jnp.where(pair == b, lens[0, b], length)
    freq = jnp.exp(jnp.bitwise_and(half, 63).astype(F32) * (-math.log(ROPE) / 64))
    angle = length.astype(F32) * freq
    ctab = jnp.cos(angle)
    stab = jnp.sin(angle)
    stab = jnp.where(half < 64, -stab, stab)

    lax.fori_loop(1, 16, wait_b, 0)
    lane = lax.broadcasted_iota(jnp.int32, (4, HEAD), 1)
    for p in range(8):
        even, odd = brecv[2 * p], brecv[2 * p + 1]
        pieces = (
            even[:, 0:128],
            even[:, 128:256],
            jnp.where(lane < 64, even[:, 256:384], odd[:, 0:128]),
            odd[:, 128:256],
            odd[:, 256:384],
        )
        for j, piece in enumerate(pieces):
            h = 5 * p + j
            if h < HEADS:
                qs[4 * h : 4 * h + 4, :] = piece
            elif h < HEADS + KV:
                at = 128 + 8 * (h - HEADS)
                qs[at : at + 4, :] = piece
                qs[at + 4 : at + 8, :] = piece
            else:
                at = 8 * (h - HEADS - KV)
                vs[at : at + 4, :] = piece
                vs[at + 4 : at + 8, :] = piece
    v = qs[...]
    v = v * lax.rsqrt(jnp.mean(v * v, axis=1, keepdims=True) + EPS)
    row = lax.broadcasted_iota(jnp.int32, (160, HEAD), 0)
    v = v * jnp.where(row < 128, qgain[...][None, :], kgain[...][None, :])
    turned = pltpu.roll(v, 64, 1)
    v = v.reshape(20, 8, HEAD) * ctab[None] + turned.reshape(20, 8, HEAD) * stab[None]
    v = v.reshape(160, HEAD).astype(BF)
    scale = 1.0 / math.sqrt(HEAD)
    seq = jnp.bitwise_and(lax.broadcasted_iota(jnp.int32, (32, HEAD), 0), 3)
    live = jnp.where(half < length, 1.0, 0.0)
    live = jnp.broadcast_to(live[None], (4, 8, HEAD)).reshape(32, HEAD) > 0.5
    heads = []
    for g in range(KV):
        q = v[32 * g : 32 * g + 32]
        newk = v[128 + 8 * g : 136 + 8 * g].astype(F32)
        own = jnp.sum((q.astype(F32).reshape(4, 8, HEAD) * newk[None]).reshape(32, HEAD), axis=1, keepdims=True)
        own = own * scale
        s = jnp.zeros((32, HEAD), F32)
        for b in range(4):
            sb = lax.dot_general(
                q, kc[b, :, g * 128 : (g + 1) * 128], (((1,), (1,)), ((), ())), preferred_element_type=F32
            )
            s = jnp.where(seq == b, sb, s)
        s = jnp.where(live, s * scale, -jnp.inf)
        top = jnp.maximum(jnp.max(s, axis=1, keepdims=True), own)
        e = jnp.exp(s - top)
        own_e = jnp.exp(own - top)
        den = jnp.sum(e, axis=1, keepdims=True) + own_e
        newv = vs[8 * g : 8 * g + 8, :]
        low = own_e.astype(BF).astype(F32)
        num = (low.reshape(4, 8, 1) * newv[None]).reshape(32, HEAD)
        for b in range(4):
            eb = jnp.where(seq == b, e, 0.0).astype(BF)
            num = num + dot(eb, vc[b, :, g * 128 : (g + 1) * 128])
        heads.append(num / den)
    for yy in range(YS):
        g, at = yy // 4, 8 * (yy % 4)
        hsend[yy] = jnp.concatenate([heads[g][at : at + 8], heads[g + 2][at : at + 8]], axis=0).astype(BF)

    def h_slot(t):
        return hrecv.at[pl.ds(mo(t * 16, 16), 16), :]

    def h_copy(d):
        to = (tp + d) % 16
        return rcopy(hsend.at[to % YS], h_slot(tp), hs.at[to], hr.at[tp], {"tp": to})

    def start_h(d, _):
        h_copy(d).start()
        return 0

    def wait_h(d, _):
        frm = (tp + d) % 16
        rcopy(hsend.at[frm % YS], h_slot(frm), hs.at[frm], hr.at[frm], {"tp": frm}).wait_recv()
        return 0

    lax.fori_loop(1, 16, start_h, 0)
    hrecv[pl.ds(mo(tp * 16, 16), 16), :] = hsend[y]

    wo_copy.wait_recv()
    unpack_wo(wo_r, (1 - xl) * 256)
    hop(1)

    lax.fori_loop(1, 16, wait_h, 0)
    P128 = one_hot(128, 32, 32)
    got = hrecv[...]
    t = lax.broadcasted_iota(jnp.int32, (ROWS, 256), 0)
    c = lax.broadcasted_iota(jnp.int32, (ROWS, 256), 1)
    zcat = []
    for hl in range(4):
        want = jnp.right_shift(t, 2) * 16 + hl * 4 + jnp.bitwise_and(t, 3)
        pick = jnp.where(c == want, 1.0, 0.0).astype(BF)
        zcat.append(dot(dot(pick, got).astype(BF), P128).astype(BF))
    zcat = jnp.concatenate(zcat, axis=1)

    def part(yy):
        return pl.ds(mo(32 * (yy // 4), 32), 32), pl.ds(mo(640 * (yy % 4), 128), 640)

    for cb in range(4):
        pm[:, cb * 640 : cb * 640 + 640] = dot(zcat, wo[:, cb * 640 : cb * 640 + 640]).astype(BF)

    def r_copy(d):
        to = (y + d) % YS
        a, b = part(to)
        return rcopy(pm.at[a, b], rs.at[y], rss.at[to], rsr.at[y], {"tp": xl * YS + to})

    def wait_r(d, _):
        frm = (y + d) % YS
        a, b = part(frm)
        rcopy(pm.at[a, b], rs.at[frm], rss.at[frm], rsr.at[frm], {"tp": xl * YS + frm}).wait_recv()
        return 0

    for d in NEAR[:0:-1]:
        r_copy(d).start()
    a, b = part(y)
    rs[y] = pm[a, b]
    unpack(1)
    unpack(7)
    unpack_sib(0)
    hop(2)

    lax.fori_loop(1, YS, wait_r, 0)
    mid = rs[0].astype(F32)
    for i in range(1, YS):
        mid = mid + rs[i].astype(F32)
    cols = pl.ds(mo(xl * HALF + 640 * (y % 4), 128), 640)
    mid = hid[a, cols].astype(F32) + mid * vec[2:3, cols]
    X[pl.ds(mo(src * 64 + 32 * (y // 4), 32), 32), cols] = mid.astype(BF)

    def blk(xx, cc, yy):
        r0 = ((xx // 2) * 2 + cc) * 64 + 32 * (yy // 4)
        c0 = (xx % 2) * HALF + 640 * (yy % 4)
        return X.at[pl.ds(mo(r0, 32), 32), pl.ds(mo(c0, 128), 640)]

    def fy_copy(d):
        to = (y + d) % YS
        return rcopy(blk(x, core, y), blk(x, core, y), fys.at[to], fyr.at[y], {"tp": xl * YS + to})

    for d in NEAR[1:]:
        fy_copy(d).start()

    def fx_copy(way, i):
        b0 = blk(x, core, (y + i) % YS)
        return rcopy(b0, b0, fxs.at[way, i], fxr.at[way, i], PLUS if way == 0 else MINUS)

    def fx_in(way, i):
        b0 = blk(xm if way == 0 else xp, core, (y + i) % YS)
        return rcopy(b0, b0, fxs.at[way, i], fxr.at[way, i], MINUS if way == 0 else PLUS)

    def fq_copy(i):
        way = i % 2
        b0 = blk(xm if way == 0 else xp, core, (y + i) % YS)
        return rcopy(b0, b0, fqs.at[i], fqr.at[i], PLUS if way == 0 else MINUS)

    def fq_in(i):
        b0 = blk(xo, core, (y + i) % YS)
        return rcopy(b0, b0, fqs.at[i], fqr.at[i], MINUS if i % 2 == 0 else PLUS)

    froms = (x, xm, xp, xo)

    def fs_copy(j, i):
        b0 = blk(froms[j], core, (y + i) % YS)
        return rcopy(b0, b0, fss.at[j, i], fsr.at[j, i], SIB)

    def fs_in(j, i):
        b0 = blk(froms[j], 1 - core, (y + i) % YS)
        return rcopy(b0, b0, fss.at[j, i], fsr.at[j, i], SIB)

    def gained(xx, cc):
        at = pl.ds(mo(((xx // 2) * 2 + cc) * 64, 64), 64)
        total = jnp.zeros((64, 1), F32)
        for g in range(5):
            c0 = (xx % 2) * HALF + g * 512
            cs = pl.ds(mo(c0, 128), 512)
            v = X[at, cs].astype(F32)
            total = total + jnp.sum(v * v, axis=1, keepdims=True)
            v = dot((v * vec[1:2, cs]).astype(BF), p512[...]).astype(BF)
            to = pl.ds(mo((xx % 2) * 640 + g * 128, 128), 128)
            for k in range(4):
                xk[k, at, to] = v[:, k * 128 : (k + 1) * 128]
        ssq[xx % 2, at, :] = jnp.broadcast_to(total, (64, HEAD))

    for n, i in enumerate(NEAR):
        yy = (y + i) % YS
        if i:
            b0 = blk(x, core, yy)
            rcopy(b0, b0, fys.at[yy], fyr.at[yy], {"tp": xl * YS + yy}).wait_recv()
        fx_copy(0, i).start()
        fx_copy(1, i).start()
        fs_copy(0, i).start()
        if n == 3:
            unpack(2)
            unpack(6)
            unpack_sib(1)
            unpack_sib(7)
            hop(3)
    gained(x, core)
    for i in NEAR:
        fx_in(0, i).wait_recv()
        fx_in(1, i).wait_recv()
        fq_copy(i).start()
        fs_copy(1, i).start()
        fs_copy(2, i).start()
    gained(xm, core)
    gained(xp, core)
    unpack(3)
    unpack(5)
    unpack_sib(2)
    unpack_sib(6)
    for i in NEAR:
        fs_in(0, i).wait_recv()
    gained(x, 1 - core)
    hop(4)
    unpack(4)
    unpack_sib(3)
    unpack_sib(5)
    for i in NEAR:
        fq_in(i).wait_recv()
        fs_copy(3, i).start()
    gained(xo, core)
    for j in (1, 2, 3):
        for i in NEAR:
            fs_in(j, i).wait_recv()
        gained(froms[j], 1 - core)
    gsc[...] = jnp.zeros((8, 1024), F32)
    gsc[0:1, :800] = gscale[...][None, :]
    gsc[1:2, :800] = uscale[...][None, :]
    shifted = gsc[...]
    mine = shifted
    for s in range(1, 4):
        mine = jnp.where(src == s, pltpu.roll(shifted, 1024 - HID * s, 1), mine)
    both = dot(xk[0], wg[0])
    for k in range(1, 4):
        both = both + dot(xk[k], wg[k])
    rms = lax.rsqrt((ssq[0, :, 0:1] + ssq[1, :, 0:1]) * (1.0 / D) + EPS)
    gate = both[:, :PAD] * rms * mine[0:1, :PAD]
    up = pltpu.roll(both, 512 - HID, 1)[:, :PAD] * rms * mine[1:2, :PAD]
    used = lax.broadcasted_iota(jnp.int32, (1, PAD), 1) < HID
    act = jnp.where(used, gate / (1.0 + jnp.exp(-gate)) * up, 0.0).astype(BF)
    act = dot(act, one_hot(PAD, HID // 4, 64)).astype(BF)
    xk[0, :, :PAD] = act

    def act_rows(h, cc):
        return pl.ds(mo((h * 2 + cc) * 64, 64), 64)

    def ac_copy(h):
        return rcopy(xk.at[0, act_rows(h, 1 - core), 0:PAD], actr.at[h], acs.at[h], acr.at[h], SIB)

    for h in (0, 1):
        ac_copy(h).start()
    unpack_sib(4)
    for h in (0, 1):
        ac_copy(h).wait_recv()
    lhs = [
        jnp.concatenate([xk[0, act_rows(0, core), 0:PAD], xk[0, act_rows(1, core), 0:PAD]], axis=0),
        jnp.concatenate([actr[0], actr[1]], axis=0),
    ]

    def down(c0):
        def some(n, _):
            at = pl.ds(mo(c0 + n * 640, 128), 640)
            r = dot(lhs[0], wd[0, :, at]) + dot(lhs[1], wd[1, :, at])
            pd[:, at] = r.astype(BF)
            return 0

        lax.fori_loop(0, 2, some, 0)

    sides = (PLUS, MINUS)
    nexts = (xp, xm)

    def slab(xx, q, w):
        rows = pl.ds(mo((xx // 2) * 64, 64), 64)
        return rows, pl.ds(mo((xx % 2) * HALF + q * 1280 + w * 640, 128), 640)

    def pre_copy(q, w):
        a, b = slab(xo, q, w)
        return rcopy(pd.at[a, b], pre.at[q, w], xps.at[q, w], xpr.at[q, w], sides[w])

    def plain_copy(q, w):
        a, b = slab(nexts[w], q, 1 - w)
        return rcopy(pd.at[a, b], rplain.at[q, w], xas.at[q, w], xar.at[q, w], sides[w])

    def merge_copy(q, w):
        return rcopy(smerge.at[q, w], rmerge.at[q, w], xms.at[q, w], xmr.at[q, w], sides[w])

    def merge(q):
        for w in (0, 1):
            pre_copy(q, w).wait_recv()
            a, b = slab(nexts[w], q, w)
            smerge[q, w] = (pd[a, b].astype(F32) + pre[q, w].astype(F32)).astype(BF)
            merge_copy(q, w).start()

    def window(yy):
        return pl.ds(mo(320 * yy - 64 * (yy % 2), 128), 384)

    def finish(q):
        for w in (0, 1):
            plain_copy(q, w).wait_recv()
        for w in (0, 1):
            merge_copy(q, w).wait_recv()
            a, b = slab(x, q, w)
            v = pd[a, b].astype(F32) + rplain[q, 1 - w].astype(F32) + rmerge[q, w].astype(F32)
            u[:, q * 1280 + w * 640 : q * 1280 + w * 640 + 640] = v.astype(BF)

    def y_copy(to):
        return rcopy(u.at[:, window(to)], yr.at[y], yss.at[to], ysr.at[y], {"tp": xl * YS + to})

    def y_sends(q):
        for i in range(4):
            to = 4 * q + i

            @pl.when(to != y)
            def _():
                y_copy(to).start()

            @pl.when(to == y)
            def _():
                yr[y] = u[:, window(to)]

    down(xl * HALF)
    for w in (0, 1):
        pre_copy(0, w).start()
    down((1 - xl) * HALF)
    for w in (0, 1):
        plain_copy(0, w).start()
    down(xl * HALF + 1280)
    for w in (0, 1):
        pre_copy(1, w).start()
    down((1 - xl) * HALF + 1280)
    for w in (0, 1):
        plain_copy(1, w).start()
    merge(0)
    merge(1)
    finish(0)
    y_sends(0)
    finish(1)
    y_sends(1)
    for d in NEAR[1:]:
        frm = (y + d) % YS
        rcopy(u.at[:, window(frm)], yr.at[frm], yss.at[frm], ysr.at[frm], {"tp": xl * YS + frm}).wait_recv()
    last = yr[0].astype(F32)
    for i in range(1, YS):
        last = last + yr[i].astype(F32)
    at = pl.ds(mo(xl * HALF + 320 * y - 64 * (y % 2), 128), 384)
    last = X[pl.ds(mo(src * 64, 64), 64), at].astype(F32) + last * vec[3:4, at]
    last = jnp.where(odd_y, pltpu.roll(last, 320, 1), last)
    out[...] = last[:, :320].astype(BF)

    for d in (1, 2, 3):
        w1_gu(d).wait_send()
        w1_dn(d).wait_send()
    wo_copy.wait_send()
    for h in (0, 1):
        for step in (1, 2, 3, 4):
            for way in (0, 1):
                for c in ring(h, step, way):
                    c.wait_send()
    for slot in range(ZS):
        to_sib(slot).wait_send()

    def sent_tp(d, _):
        b_copy(d).wait_send()
        h_copy(d).wait_send()
        return 0

    def sent_y(d, _):
        r_copy(d).wait_send()
        fy_copy(d).wait_send()
        y_copy((y + d) % YS).wait_send()
        return 0

    lax.fori_loop(1, 16, sent_tp, 0)
    lax.fori_loop(1, YS, sent_y, 0)
    for i in range(YS):
        fx_copy(0, i).wait_send()
        fx_copy(1, i).wait_send()
        fq_copy(i).wait_send()
        for j in range(4):
            fs_copy(j, i).wait_send()
    for w in (0, 1):
        ac_copy(w).wait_send()
        for q in (0, 1):
            pre_copy(q, w).wait_send()
            plain_copy(q, w).wait_send()
            merge_copy(q, w).wait_send()


def local(
    hidden_in, attn_gain, w_qkv, qkv_scale, q_gain, k_gain, key_cache, value_cache, lengths, w_out, out_scale,
    mlp_gain, w_gate, w_up, gate_scale, up_scale, w_down, down_scale,
):
    V, S = pltpu.VMEM, pltpu.SemaphoreType.DMA
    I32 = jnp.int32
    scratch = [
        V((1280, 320), I32), V((4, 128, 512), BF), V((4, 128, 512), BF), V((64, HALF), I32), V((512, 512), BF),
        V((8, D), F32), V((8, 1024), F32),
        V((ROWS, 384), F32), V((4, 40, 384), I32), V((4, 56, 256), I32),
        V((16, 4, 384), F32), V((16, 4, 384), F32), V((160, HEAD), F32), V((32, HEAD), F32),
        V((YS, 16, HEAD), BF), V((256, HEAD), BF), V((64, HALF), I32), V((512, HALF), BF), V((ROWS, HALF), BF),
        V((YS, 32, 640), BF), V((ALL, D), BF), V((4, ALL, 1280), BF), V((2, ALL, HEAD), F32),
        V((ZS, 160, 384), I32), V((4, 56, 256), I32), V((ZS, 2, 56, 384), I32), V((ZS, 2, 56, 384), I32),
        V((4, 1280, 512), BF), V((2, 256, D), BF), V((2, ROWS, PAD), BF), V((2 * ROWS, D), BF),
        V((2, 2, ROWS, 640), BF), V((2, 2, ROWS, 640), BF), V((2, 2, ROWS, 640), BF), V((2, 2, ROWS, 640), BF),
        V((ROWS, HALF), BF), V((YS, ROWS, 384), BF),
        S((5,)), S((2, 4)), S((2, 4)), S, S, S((2, 2, 4, 2)), S((2, 2, 4, 2)), S((8,)), S((8,)),
        S((16,)), S((16,)), S((16,)), S((16,)),
        S((8,)), S((8,)), S((8,)), S((8,)), S((2, 8)), S((2, 8)), S((8,)), S((8,)), S((4, 8)), S((4, 8)),
        S((2,)), S((2,)), S((2, 2)), S((2, 2)), S((2, 2)), S((2, 2)), S((2, 2)), S((2, 2)), S((8,)), S((8,)),
    ]
    vmem = pl.BlockSpec(memory_space=pltpu.VMEM)
    far = pl.BlockSpec(memory_space=pl.ANY)
    specs = [vmem] * 18
    for i in (2, 6, 7, 9):
        specs[i] = far
    specs[8] = pl.BlockSpec(memory_space=pltpu.SMEM)
    return pl.pallas_call(
        kernel,
        out_shape=jax.ShapeDtypeStruct((ROWS, 320), BF),
        in_specs=specs,
        out_specs=vmem,
        scratch_shapes=scratch,
        compiler_params=pltpu.CompilerParams(
            collective_id=0, has_side_effects=True, vmem_limit_bytes=60 * 1024 * 1024
        ),
        name="layer",
    )(
        hidden_in, attn_gain, w_qkv, qkv_scale, q_gain, k_gain, key_cache, value_cache, lengths, w_out, out_scale,
        mlp_gain, w_gate, w_up, gate_scale, up_scale, w_down, down_scale,
    )


def solution(mesh):
    return jax.shard_map(
        local,
        mesh=mesh,
        in_specs=(
            P(("grp", "src"), None),
            P(),
            P(None, "tp"),
            P("tp"),
            P(),
            P(),
            P(("grp", "src"), "tp", None, None),
            P(("grp", "src"), "tp", None, None),
            P(("grp", "src"), "tp"),
            P("tp", None),
            P(),
            P(),
            P(("grp", "src"), "tp"),
            P(("grp", "src"), "tp"),
            P("tp"),
            P("tp"),
            P("tp", ("grp", "src")),
            P(),
        ),
        out_specs=P(("grp", "src"), "tp"),
        check_vma=False,
    )
```

```python
import math

import jax
import jax.numpy as jnp
from jax import lax
from jax.experimental import pallas as pl
from jax.experimental.pallas import tpu as pltpu
from jax.sharding import PartitionSpec as P

D = 5120
HALF = 2560
HEADS = 32
KV = 4
HEAD = 128
ROWS = 64
ALL = 256
YS = 8
ZS = 8
HID = 200
PAD = 256
EPS = 1e-06
ROPE = 1000000.0
MESH = pl.DeviceIdType.MESH
F32 = jnp.float32
BF = jnp.bfloat16
NEAR = (0, 1, 7, 2, 6, 3, 5, 4)


def mo(value, k):
    return pl.multiple_of(value, k)


def byte_of(words, k):
    return jnp.right_shift(jnp.left_shift(words, 24 - 8 * k), 24).astype(F32).astype(BF)


def one_hot(n, used, stride):
    row = lax.broadcasted_iota(jnp.int32, (n, n), 0)
    col = lax.broadcasted_iota(jnp.int32, (n, n), 1)
    shift = stride.bit_length() - 1
    k, r = jnp.right_shift(col, shift), jnp.bitwise_and(col, stride - 1)
    return jnp.where((row == 4 * r + k) & (r < used), 1.0, 0.0).astype(BF)


def dot(a, b):
    return jnp.dot(a, b, preferred_element_type=F32)


def kernel(
    hid_hbm, again_hbm, wq_hbm, qscale_hbm, qgain_hbm, kgain_hbm, kc_hbm, vc_hbm, lens, wout, oscale_hbm, mgain_hbm,
    wgate_hbm, wup_hbm, gscale_hbm, uscale_hbm, wdown_hbm, dscale_hbm,
    out,
    hid, again, qscale, qgain, kgain, oscale, mgain, wgate, wup, gscale, uscale, wdown, dscale,
    wq, kc, vc, woh, p512, vec, gsc, stage, gu4, dn4, bsend, brecv, qs, vs, hsend, hrecv, wo_r, wo, pm, rs, X, xk, ssq,
    gub, dnp, dnb, dns, wg, wd, actr, pd, pre, smerge, rplain, rmerge, u, yr,
    ld, w1s, w1r, wos, wor, zs, zr, ns, nr, bs, br, hs, hr, rss, rsr, fys, fyr, fxs, fxr, fqs, fqr, fss, fsr,
    acs, acr, xps, xpr, xas, xar, xms, xmr, yss, ysr,
):
    z = lax.axis_index("grp")
    tp = lax.axis_index("tp")
    src = lax.axis_index("src")
    xl, y = tp // YS, tp % YS
    xh, core = src // 2, src % 2
    x = xh * 2 + xl

    def at_x(xx, cc):
        return {"tp": (xx % 2) * YS + y, "src": (xx // 2) * 2 + cc}

    xp, xm, xo = (x + 1) % 4, (x + 3) % 4, (x + 2) % 4
    PLUS, MINUS = at_x(xp, core), at_x(xm, core)
    SIB = {"src": xh * 2 + 1 - core}
    ZP, ZM = {"grp": (z + 1) % ZS}, {"grp": (z + ZS - 1) % ZS}

    def rcopy(a, b, s, r, to):
        return pltpu.make_async_remote_copy(
            src_ref=a, dst_ref=b, send_sem=s, recv_sem=r, device_id=to, device_id_type=MESH
        )

    load_wq = [
        pltpu.make_async_copy(wq_hbm.at[:, pl.ds(i * 640, 640)], wq.at[:, pl.ds(i * 640, 640)], ld.at[i]) for i in (0, 1)
    ]
    load_kc = pltpu.make_async_copy(kc_hbm.at[0], kc, ld.at[2])
    load_vc = pltpu.make_async_copy(vc_hbm.at[0], vc, ld.at[3])
    load_wo = pltpu.make_async_copy(wout.at[:, pl.ds(mo(xl * HALF, 128), HALF)], woh, ld.at[4])
    pairs = (
        (hid_hbm, hid), (again_hbm, again), (wgate_hbm, wgate), (wup_hbm, wup), (wdown_hbm, wdown), (mgain_hbm, mgain),
        (oscale_hbm, oscale), (dscale_hbm, dscale), (qscale_hbm, qscale), (qgain_hbm, qgain), (kgain_hbm, kgain),
        (gscale_hbm, gscale), (uscale_hbm, uscale),
    )
    loads = [pltpu.make_async_copy(a, b, ld.at[5 + i]) for i, (a, b) in enumerate(pairs)]
    for c in loads[2:5] + loads[:2] + loads[5:] + load_wq:
        c.start()
    load_kc.start()
    load_vc.start()
    load_wo.start()

    barrier = pltpu.get_barrier_semaphore()

    def greet_tp(d, _):
        pl.semaphore_signal(barrier, inc=1, device_id={"tp": (tp + d) % 16}, device_id_type=MESH)
        return 0

    def greet_src(d, _):
        pl.semaphore_signal(barrier, inc=1, device_id={"src": (src + d) % 4}, device_id_type=MESH)
        return 0

    lax.fori_loop(1, 16, greet_tp, 0)
    lax.fori_loop(1, 4, greet_src, 0)
    across = {"tp": (1 - xl) * YS + y, "src": (1 - xh) * 2 + core}
    for to in (across, ZP, ZM):
        pl.semaphore_signal(barrier, inc=1, device_id=to, device_id_type=MESH)

    for c in loads:
        c.wait()
    turned = jnp.transpose(wdown[...])
    for s in range(4):
        piece = jnp.concatenate([wgate[:, HID * s : HID * s + HID], wup[:, HID * s : HID * s + HID]], axis=1)
        gu4[s] = piece[:, :384]
        dn4[s] = jnp.zeros((56, 256), jnp.int32)
        dn4[s, 0:50, 0:160] = turned[50 * s : 50 * s + 50, :]
        dn4[s, 0:40, 160:176] = piece[:, 384:400]
    gub[0, pl.ds(mo(src * 40, 8), 40), :] = gu4[src]
    dnp[src] = dn4[src]
    p512[...] = one_hot(512, 128, 128)
    vec[0:1, :] = again[...][None, :]
    vec[1:2, :] = mgain[...][None, :]
    vec[2:3, :] = oscale[...][None, :]
    vec[3:4, :] = dscale[...][None, :]

    total = jnp.zeros((ROWS, 1), F32)
    for g in range(10):
        v = hid[:, g * 512 : (g + 1) * 512].astype(F32)
        total = total + jnp.sum(v * v, axis=1, keepdims=True)
    rms = lax.rsqrt(total * (1.0 / D) + EPS)
    stage[...] = jnp.broadcast_to(rms, (ROWS, 384))

    def qkv_group(g, acc):
        at = pl.ds(mo(g * 512, 512), 512)
        v = (hid[:, at].astype(F32) * stage[:, 0:1] * vec[0:1, at]).astype(BF)
        v = dot(v, p512[...]).astype(BF)
        w = wq[:, pl.ds(mo(g * 128, 128), 128)]
        for k in range(4):
            acc = acc + lax.dot_general(
                v[:, k * 128 : (k + 1) * 128], byte_of(w, k), (((1,), (1,)), ((), ())), preferred_element_type=F32
            )
        return acc

    load_wq[0].wait()
    acc = lax.fori_loop(0, 5, qkv_group, jnp.zeros((ROWS, 320), F32))
    pl.semaphore_wait(barrier, 21)

    def w1_gu(d):
        s2 = (src + d) % 4
        return rcopy(
            gu4.at[s2], gub.at[0, pl.ds(mo(src * 40, 8), 40), :], w1s.at[0, d], w1r.at[0, src], {"src": s2}
        )

    def w1_dn(d):
        s2 = (src + d) % 4
        return rcopy(dn4.at[s2], dnp.at[src], w1s.at[1, d], w1r.at[1, src], {"src": s2})

    for d in (1, 2, 3):
        w1_gu(d).start()
        w1_dn(d).start()

    load_wq[1].wait()
    acc = lax.fori_loop(5, 10, qkv_group, acc)
    qkv = (acc * qscale[...][None, :]).astype(BF).astype(F32)
    stage[...] = jnp.zeros((ROWS, 384), F32)
    stage[:, :320] = qkv
    odd_y = (y % 2) == 1
    placed = stage[...]
    placed = jnp.where(odd_y, pltpu.roll(placed, 64, 1), placed)
    for t in range(16):
        bsend[t] = placed[4 * t : 4 * t + 4, :]

    def b_copy(d):
        to = (tp + d) % 16
        return rcopy(bsend.at[to], brecv.at[tp], bs.at[to], br.at[tp], {"tp": to})

    def start_b(d, _):
        b_copy(d).start()
        return 0

    def wait_b(d, _):
        frm = (tp + d) % 16
        rcopy(bsend.at[frm], brecv.at[frm], bs.at[frm], br.at[frm], {"tp": frm}).wait_recv()
        return 0

    lax.fori_loop(1, 16, start_b, 0)
    wo_side = (x + 1 + 2 * core) % 4
    wo_rows = pl.ds(mo(core * 32, 32), 32)
    wo_copy = rcopy(
        wout.at[wo_rows, pl.ds(mo((1 - xl) * HALF, 128), HALF)], wo_r.at[wo_rows, :], wos.at[0], wor.at[0],
        at_x(wo_side, core),
    )
    wo_share = rcopy(wo_r.at[wo_rows, :], wo_r.at[wo_rows, :], wos.at[1], wor.at[1], SIB)
    wo_copy.start()
    brecv[pl.ds(tp, 1)] = bsend[pl.ds(tp, 1)]

    def w1_in(d):
        s2 = (src + d) % 4
        rcopy(gu4.at[s2], gub.at[0, pl.ds(mo(s2 * 40, 8), 40), :], w1s.at[0, d], w1r.at[0, s2], {"src": s2}).wait_recv()
        rcopy(dn4.at[s2], dnp.at[s2], w1s.at[1, d], w1r.at[1, s2], {"src": s2}).wait_recv()

    def assemble(h):
        one, two = dnp[2 * h], dnp[2 * h + 1]
        dnb[0, h] = jnp.concatenate(
            [one[:, :160], two[:, :160], one[:, 160:192], two[:, 160:192]], axis=1
        )

    def ring(h, step, way):
        a = step - 1 if way == 0 else (9 - step) % 8
        b = step if way == 0 else 8 - step
        to = ZP if way == 0 else ZM
        if step == 4:
            n, off, d_at = (40, 0, slice(0, 32)) if way == 0 else (40, 40, slice(32, 56))
        else:
            n, off, d_at = 80, 0, slice(0, 56)
        at = pl.ds(mo(h * 80 + off, 8), n)
        one = rcopy(gub.at[a, at, :], gub.at[b, at, :], zs.at[h, way, step - 1, 0], zr.at[h, way, step - 1, 0], to)
        two = rcopy(
            dnb.at[a, h, d_at, :], dnb.at[b, h, d_at, :], zs.at[h, way, step - 1, 1], zr.at[h, way, step - 1, 1], to
        )
        return one, two

    def ring_start(h, step):
        for way in (0, 1):
            for c in ring(h, step, way):
                c.start()

    def ring_wait(h, step):
        for way in (0, 1):
            for c in ring(h, step, way):
                c.wait_recv()

    def to_sib(slot):
        return rcopy(dnb.at[slot], dns.at[slot], ns.at[slot], nr.at[slot], SIB)

    def hop(stream, step):
        h = xh if stream == 0 else 1 - xh
        ring_wait(h, step)
        if step < 4:
            ring_start(h, step + 1)
        if stream == 1:
            to_sib(step).start()
            if step < 4:
                to_sib(8 - step).start()

    def unpack_down(ref, slot, which):
        zz = (z + ZS - slot) % ZS
        w = jnp.concatenate([ref[slot, 0, :, :320], ref[slot, 1, :, :320]], axis=1)
        for k in range(4):
            wd[which, k * 64 : k * 64 + 56, pl.ds(mo(zz * 640, 128), 640)] = byte_of(w, k)

    lane40 = lax.broadcasted_iota(jnp.int32, (40, 128), 1)

    def unpack(slot):
        zz = (z + ZS - slot) % ZS

        def rows(i, _):
            w = gub[slot, pl.ds(mo(i * 32, 32), 32), :]
            for k in range(4):
                wg[k, pl.ds(mo(zz * 160 + i * 32, 32), 32), 0:384] = byte_of(w, k)
            return 0

        lax.fori_loop(0, 5, rows, 0)
        tails = []
        for s in range(4):
            t = dnb[slot, s // 2, 0:40, 256:384]
            t = pltpu.roll(t, 64 - 32 * (s % 2), 1)
            tails.append(jnp.where(lane40 < 16, t, 0))
        tails = jnp.concatenate(tails, axis=0)
        for k in range(4):
            wg[k, pl.ds(mo(zz * 160, 32), 160), 384:512] = byte_of(tails, k)
        unpack_down(dnb, slot, 0)

    def unpack_sib(slot):
        to_sib(slot).wait_recv()
        unpack_down(dns, slot, 1)

    rcopy(
        gu4.at[0], gub.at[0, pl.ds(mo((src + 1 - 2 * core) * 40, 8), 40), :], w1s.at[0, 1],
        w1r.at[0, src + 1 - 2 * core], SIB,
    ).wait_recv()
    rcopy(dn4.at[0], dnp.at[src + 1 - 2 * core], w1s.at[1, 1], w1r.at[1, src + 1 - 2 * core], SIB).wait_recv()
    assemble(xh)
    ring_start(xh, 1)
    wd[...] = jnp.zeros(wd.shape, BF)

    def unpack_wo(ref, base):
        def cols(i, _):
            at = pl.ds(mo(i * 640, 128), 640)
            for hl in range(2):
                w = ref[hl * 32 : hl * 32 + 32, at]
                for k in range(4):
                    wo[pl.ds(mo(base + hl * 128 + k * 32, 32), 32), at] = byte_of(w, k)
            return 0

        lax.fori_loop(0, 4, cols, 0)

    load_wo.wait()
    unpack_wo(woh, xl * 256)
    far = (1 - xh) * 2
    for s2 in (far, far + 1):
        rcopy(gu4.at[0], gub.at[0, pl.ds(mo(s2 * 40, 8), 40), :], w1s.at[0, 2], w1r.at[0, s2], {"src": s2}).wait_recv()
        rcopy(dn4.at[0], dnp.at[s2], w1s.at[1, 2], w1r.at[1, s2], {"src": s2}).wait_recv()
    assemble(1 - xh)
    ring_start(1 - xh, 1)
    to_sib(0).start()
    load_kc.wait()
    load_vc.wait()
    half = lax.broadcasted_iota(jnp.int32, (8, HEAD), 1)
    pair = jnp.bitwise_and(lax.broadcasted_iota(jnp.int32, (8, HEAD), 0), 3)
    length = jnp.full((8, HEAD), lens[0, 0], jnp.int32)
    for b in range(1, 4):
        length = jnp.where(pair == b, lens[0, b], length)
    freq = jnp.exp(jnp.bitwise_and(half, 63).astype(F32) * (-math.log(ROPE) / 64))
    angle = length.astype(F32) * freq
    ctab = jnp.cos(angle)
    stab = jnp.sin(angle)
    stab = jnp.where(half < 64, -stab, stab)

    lax.fori_loop(1, 16, wait_b, 0)
    wo_copy.wait_recv()
    wo_share.start()
    lane = lax.broadcasted_iota(jnp.int32, (4, HEAD), 1)
    for p in range(8):
        even, odd = brecv[2 * p], brecv[2 * p + 1]
        pieces = (
            even[:, 0:128],
            even[:, 128:256],
            jnp.where(lane < 64, even[:, 256:384], odd[:, 0:128]),
            odd[:, 128:256],
            odd[:, 256:384],
        )
        for j, piece in enumerate(pieces):
            h = 5 * p + j
            if h < HEADS:
                qs[4 * h : 4 * h + 4, :] = piece
            elif h < HEADS + KV:
                at = 128 + 8 * (h - HEADS)
                qs[at : at + 4, :] = piece
                qs[at + 4 : at + 8, :] = piece
            else:
                at = 8 * (h - HEADS - KV)
                vs[at : at + 4, :] = piece
                vs[at + 4 : at + 8, :] = piece
    v = qs[...]
    v = v * lax.rsqrt(jnp.mean(v * v, axis=1, keepdims=True) + EPS)
    row = lax.broadcasted_iota(jnp.int32, (160, HEAD), 0)
    v = v * jnp.where(row < 128, qgain[...][None, :], kgain[...][None, :])
    turned = pltpu.roll(v, 64, 1)
    v = v.reshape(20, 8, HEAD) * ctab[None] + turned.reshape(20, 8, HEAD) * stab[None]
    v = v.reshape(160, HEAD).astype(BF)
    scale = 1.0 / math.sqrt(HEAD)
    seq = jnp.bitwise_and(lax.broadcasted_iota(jnp.int32, (32, HEAD), 0), 3)
    live = jnp.where(half < length, 1.0, 0.0)
    live = jnp.broadcast_to(live[None], (4, 8, HEAD)).reshape(32, HEAD) > 0.5
    heads = []
    for g in range(KV):
        q = v[32 * g : 32 * g + 32]
        newk = v[128 + 8 * g : 136 + 8 * g].astype(F32)
        own = jnp.sum((q.astype(F32).reshape(4, 8, HEAD) * newk[None]).reshape(32, HEAD), axis=1, keepdims=True)
        own = own * scale
        s = jnp.zeros((32, HEAD), F32)
        for b in range(4):
            sb = lax.dot_general(
                q, kc[b, :, g * 128 : (g + 1) * 128], (((1,), (1,)), ((), ())), preferred_element_type=F32
            )
            s = jnp.where(seq == b, sb, s)
        s = jnp.where(live, s * scale, -jnp.inf)
        top = jnp.maximum(jnp.max(s, axis=1, keepdims=True), own)
        e = jnp.exp(s - top)
        own_e = jnp.exp(own - top)
        den = jnp.sum(e, axis=1, keepdims=True) + own_e
        newv = vs[8 * g : 8 * g + 8, :]
        low = own_e.astype(BF).astype(F32)
        num = (low.reshape(4, 8, 1) * newv[None]).reshape(32, HEAD)
        for b in range(4):
            eb = jnp.where(seq == b, e, 0.0).astype(BF)
            num = num + dot(eb, vc[b, :, g * 128 : (g + 1) * 128])
        heads.append(num / den)
    for yy in range(YS):
        g, at = yy // 4, 8 * (yy % 4)
        hsend[yy] = jnp.concatenate([heads[g][at : at + 8], heads[g + 2][at : at + 8]], axis=0).astype(BF)

    def h_slot(t):
        return hrecv.at[pl.ds(mo(t * 16, 16), 16), :]

    def h_copy(d):
        to = (tp + d) % 16
        return rcopy(hsend.at[to % YS], h_slot(tp), hs.at[to], hr.at[tp], {"tp": to})

    def start_h(d, _):
        h_copy(d).start()
        return 0

    def wait_h(d, _):
        frm = (tp + d) % 16
        rcopy(hsend.at[frm % YS], h_slot(frm), hs.at[frm], hr.at[frm], {"tp": frm}).wait_recv()
        return 0

    lax.fori_loop(1, 16, start_h, 0)
    hrecv[pl.ds(mo(tp * 16, 16), 16), :] = hsend[y]

    hop(0, 1)
    unpack(0)
    wo_share.wait_recv()
    unpack_wo(wo_r, (1 - xl) * 256)
    hop(1, 1)

    lax.fori_loop(1, 16, wait_h, 0)
    P128 = one_hot(128, 32, 32)
    got = hrecv[...]
    t = lax.broadcasted_iota(jnp.int32, (ROWS, 256), 0)
    c = lax.broadcasted_iota(jnp.int32, (ROWS, 256), 1)
    zcat = []
    for hl in range(4):
        want = jnp.right_shift(t, 2) * 16 + hl * 4 + jnp.bitwise_and(t, 3)
        pick = jnp.where(c == want, 1.0, 0.0).astype(BF)
        zcat.append(dot(dot(pick, got).astype(BF), P128).astype(BF))
    zcat = jnp.concatenate(zcat, axis=1)

    def part(yy, s):
        return pl.ds(mo(32 * (yy // 4) + 16 * s, 16), 16), pl.ds(mo(640 * (yy % 4), 128), 640)

    for cb in range(4):
        pm[:, cb * 640 : cb * 640 + 640] = dot(zcat, wo[:, cb * 640 : cb * 640 + 640]).astype(BF)

    def r_copy(d, s):
        to = (y + d) % YS
        a, b = part(to, s)
        return rcopy(pm.at[a, b], rs.at[s, y], rss.at[s, to], rsr.at[s, y], {"tp": xl * YS + to})

    def wait_r(d, s):
        frm = (y + d) % YS
        a, b = part(frm, s)
        rcopy(pm.at[a, b], rs.at[s, frm], rss.at[s, frm], rsr.at[s, frm], {"tp": xl * YS + frm}).wait_recv()

    for s in (0, 1):
        for d in NEAR[:0:-1]:
            r_copy(d, s).start()
        a, b = part(y, s)
        rs[s, y] = pm[a, b]
    unpack(1)
    unpack(7)
    unpack_sib(0)
    hop(0, 2)

    def blk(xx, cc, yy, s):
        r0 = ((xx // 2) * 2 + cc) * 64 + 32 * (yy // 4) + 16 * s
        c0 = (xx % 2) * HALF + 640 * (yy % 4)
        return X.at[pl.ds(mo(r0, 16), 16), pl.ds(mo(c0, 128), 640)]

    def fy_copy(d, s):
        to = (y + d) % YS
        b0 = blk(x, core, y, s)
        return rcopy(b0, b0, fys.at[s, to], fyr.at[s, y], {"tp": xl * YS + to})

    def fx_copy(way, i, s):
        b0 = blk(x, core, (y + i) % YS, s)
        return rcopy(b0, b0, fxs.at[s, way, i], fxr.at[s, way, i], PLUS if way == 0 else MINUS)

    def fx_in(way, i, s):
        b0 = blk(xm if way == 0 else xp, core, (y + i) % YS, s)
        return rcopy(b0, b0, fxs.at[s, way, i], fxr.at[s, way, i], MINUS if way == 0 else PLUS)

    def fq_copy(i, s):
        way = i % 2
        b0 = blk(xm if way == 0 else xp, core, (y + i) % YS, s)
        return rcopy(b0, b0, fqs.at[s, i], fqr.at[s, i], PLUS if way == 0 else MINUS)

    def fq_in(i, s):
        b0 = blk(xo, core, (y + i) % YS, s)
        return rcopy(b0, b0, fqs.at[s, i], fqr.at[s, i], MINUS if i % 2 == 0 else PLUS)

    froms = (x, xm, xp, xo)

    def fs_copy(j, i, s):
        b0 = blk(froms[j], core, (y + i) % YS, s)
        return rcopy(b0, b0, fss.at[s, j, i], fsr.at[s, j, i], SIB)

    def fs_in(j, i, s):
        b0 = blk(froms[j], 1 - core, (y + i) % YS, s)
        return rcopy(b0, b0, fss.at[s, j, i], fsr.at[s, j, i], SIB)

    def gained(xx, cc):
        at = pl.ds(mo(((xx // 2) * 2 + cc) * 64, 64), 64)
        total = jnp.zeros((64, 1), F32)
        for g in range(5):
            c0 = (xx % 2) * HALF + g * 512
            cs = pl.ds(mo(c0, 128), 512)
            v = X[at, cs].astype(F32)
            total = total + jnp.sum(v * v, axis=1, keepdims=True)
            v = dot((v * vec[1:2, cs]).astype(BF), p512[...]).astype(BF)
            to = pl.ds(mo((xx % 2) * 640 + g * 128, 128), 128)
            for k in range(4):
                xk[k, at, to] = v[:, k * 128 : (k + 1) * 128]
        ssq[xx % 2, at, :] = jnp.broadcast_to(total, (64, HEAD))

    def onward(i, s):
        fx_copy(0, i, s).start()
        fx_copy(1, i, s).start()
        fs_copy(0, i, s).start()

    def mid(s):
        for d in NEAR[1:]:
            wait_r(d, s)
        m = rs[s, 0].astype(F32)
        for i in range(1, YS):
            m = m + rs[s, i].astype(F32)
        cols = pl.ds(mo(xl * HALF + 640 * (y % 4), 128), 640)
        m = hid[pl.ds(mo(32 * (y // 4) + 16 * s, 16), 16), cols].astype(F32) + m * vec[2:3, cols]
        X[pl.ds(mo(src * 64 + 32 * (y // 4) + 16 * s, 16), 16), cols] = m.astype(BF)
        for d in NEAR[1:]:
            fy_copy(d, s).start()
        onward(0, s)

    def from_y(i, s):
        yy = (y + i) % YS
        b0 = blk(x, core, yy, s)
        rcopy(b0, b0, fys.at[s, yy], fyr.at[s, yy], {"tp": xl * YS + yy}).wait_recv()
        onward(i, s)

    def from_x(i, s):
        fx_in(0, i, s).wait_recv()
        fx_in(1, i, s).wait_recv()
        fq_copy(i, s).start()
        fs_copy(1, i, s).start()
        fs_copy(2, i, s).start()

    def from_sib(j):
        for s in (0, 1):
            for i in NEAR:
                fs_in(j, i, s).wait_recv()
        gained(froms[j], 1 - core)

    mid(0)
    hop(1, 2)
    mid(1)
    for i in NEAR[1:]:
        from_y(i, 0)
    hop(0, 3)
    from_x(0, 0)
    unpack(2)
    unpack(6)
    for i in NEAR[1:]:
        from_y(i, 1)
        from_x(i, 0)
    hop(1, 3)
    unpack_sib(1)
    unpack_sib(7)
    gained(x, core)
    for i in NEAR:
        from_x(i, 1)
    gained(xm, core)
    gained(xp, core)
    hop(0, 4)
    hop(1, 4)
    unpack(3)
    unpack(5)
    unpack_sib(2)
    unpack_sib(6)
    for j in (0, 1, 2):
        from_sib(j)
    unpack(4)
    unpack_sib(3)
    unpack_sib(5)
    for s in (0, 1):
        for i in NEAR:
            fq_in(i, s).wait_recv()
            fs_copy(3, i, s).start()
    gained(xo, core)
    from_sib(3)
    gsc[...] = jnp.zeros((8, 1024), F32)
    gsc[0:1, :800] = gscale[...][None, :]
    gsc[1:2, :800] = uscale[...][None, :]
    shifted = gsc[...]
    mine = shifted
    for s in range(1, 4):
        mine = jnp.where(src == s, pltpu.roll(shifted, 1024 - HID * s, 1), mine)
    both = dot(xk[0], wg[0])
    for k in range(1, 4):
        both = both + dot(xk[k], wg[k])
    rms = lax.rsqrt((ssq[0, :, 0:1] + ssq[1, :, 0:1]) * (1.0 / D) + EPS)
    gate = both[:, :PAD] * rms * mine[0:1, :PAD]
    up = pltpu.roll(both, 512 - HID, 1)[:, :PAD] * rms * mine[1:2, :PAD]
    used = lax.broadcasted_iota(jnp.int32, (1, PAD), 1) < HID
    act = jnp.where(used, gate / (1.0 + jnp.exp(-gate)) * up, 0.0).astype(BF)
    act = dot(act, one_hot(PAD, HID // 4, 64)).astype(BF)
    xk[0, :, :PAD] = act

    def act_rows(h, cc):
        return pl.ds(mo((h * 2 + cc) * 64, 64), 64)

    def ac_copy(h):
        return rcopy(xk.at[0, act_rows(h, 1 - core), 0:PAD], actr.at[h], acs.at[h], acr.at[h], SIB)

    for h in (0, 1):
        ac_copy(h).start()
    unpack_sib(4)
    for h in (0, 1):
        ac_copy(h).wait_recv()
    lhs = [
        jnp.concatenate([xk[0, act_rows(0, core), 0:PAD], xk[0, act_rows(1, core), 0:PAD]], axis=0),
        jnp.concatenate([actr[0], actr[1]], axis=0),
    ]

    def down(c0):
        def some(n, _):
            at = pl.ds(mo(c0 + n * 640, 128), 640)
            r = dot(lhs[0], wd[0, :, at]) + dot(lhs[1], wd[1, :, at])
            pd[:, at] = r.astype(BF)
            return 0

        lax.fori_loop(0, 4, some, 0)

    sides = (PLUS, MINUS)
    nexts = (xp, xm)

    def slab(xx, q, w):
        rows = pl.ds(mo((xx // 2) * 64 + q * 16, 16), 16)
        return rows, pl.ds(mo((xx % 2) * HALF + w * 1280, 128), 1280)

    def pre_copy(q, w):
        a, b = slab(xo, q, w)
        return rcopy(pd.at[a, b], pre.at[q, w], xps.at[q, w], xpr.at[q, w], sides[w])

    def plain_copy(q, w):
        a, b = slab(nexts[w], q, 1 - w)
        return rcopy(pd.at[a, b], rplain.at[q, w], xas.at[q, w], xar.at[q, w], sides[w])

    def merge_copy(q, w):
        return rcopy(smerge.at[q, w], rmerge.at[q, w], xms.at[q, w], xmr.at[q, w], sides[w])

    def pre_start(q):
        for w in (0, 1):
            pre_copy(q, w).start()

    def plain_start(q):
        for w in (0, 1):
            plain_copy(q, w).start()

    def merge(q):
        for w in (0, 1):
            pre_copy(q, w).wait_recv()
            a, b = slab(nexts[w], q, w)
            smerge[q, w] = (pd[a, b].astype(F32) + pre[q, w].astype(F32)).astype(BF)
            merge_copy(q, w).start()

    def window(yy):
        return pl.ds(mo(320 * yy - 64 * (yy % 2), 128), 384)

    def y_copy(d, q):
        to = (y + d) % YS
        at = pl.ds(q * 16, 16)
        return rcopy(u.at[at, window(to)], yr.at[y, at, :], yss.at[q, to], ysr.at[q, y], {"tp": xl * YS + to})

    def y_in(d, q):
        frm = (y + d) % YS
        at = pl.ds(q * 16, 16)
        return rcopy(u.at[at, window(frm)], yr.at[frm, at, :], yss.at[q, frm], ysr.at[q, frm], {"tp": xl * YS + frm})

    def finish(q):
        at = slice(q * 16, q * 16 + 16)
        for w in (0, 1):
            plain_copy(q, w).wait_recv()
        for w in (0, 1):
            merge_copy(q, w).wait_recv()
            a, b = slab(x, q, w)
            v = pd[a, b].astype(F32) + rplain[q, 1 - w].astype(F32) + rmerge[q, w].astype(F32)
            u[at, w * 1280 : w * 1280 + 1280] = v.astype(BF)
        for d in NEAR[:0:-1]:
            y_copy(d, q).start()
        yr[y, at, :] = u[at, window(y)]

    down(xl * HALF)
    pre_start(0)
    pre_start(1)
    down((1 - xl) * HALF)
    plain_start(0)
    merge(0)
    pre_start(2)
    plain_start(1)
    merge(1)
    pre_start(3)
    plain_start(2)
    finish(0)
    merge(2)
    plain_start(3)
    finish(1)
    merge(3)
    finish(2)
    finish(3)
    for q in range(4):
        for d in NEAR[1:]:
            y_in(d, q).wait_recv()
    last = yr[0].astype(F32)
    for i in range(1, YS):
        last = last + yr[i].astype(F32)
    at = pl.ds(mo(xl * HALF + 320 * y - 64 * (y % 2), 128), 384)
    last = X[pl.ds(mo(src * 64, 64), 64), at].astype(F32) + last * vec[3:4, at]
    last = jnp.where(odd_y, pltpu.roll(last, 320, 1), last)
    out[...] = last[:, :320].astype(BF)

    for d in (1, 2, 3):
        w1_gu(d).wait_send()
        w1_dn(d).wait_send()
    wo_copy.wait_send()
    wo_share.wait_send()
    for h in (0, 1):
        for step in (1, 2, 3, 4):
            for way in (0, 1):
                for c in ring(h, step, way):
                    c.wait_send()
    for slot in range(ZS):
        to_sib(slot).wait_send()

    def sent_tp(d, _):
        b_copy(d).wait_send()
        h_copy(d).wait_send()
        return 0

    lax.fori_loop(1, 16, sent_tp, 0)
    for d in NEAR[1:]:
        for s in (0, 1):
            r_copy(d, s).wait_send()
            fy_copy(d, s).wait_send()
        for q in range(4):
            y_copy(d, q).wait_send()
    for s in (0, 1):
        for i in range(YS):
            fx_copy(0, i, s).wait_send()
            fx_copy(1, i, s).wait_send()
            fq_copy(i, s).wait_send()
            for j in range(4):
                fs_copy(j, i, s).wait_send()
    for w in (0, 1):
        ac_copy(w).wait_send()
        for q in range(4):
            pre_copy(q, w).wait_send()
            plain_copy(q, w).wait_send()
            merge_copy(q, w).wait_send()


def local(
    hidden_in, attn_gain, w_qkv, qkv_scale, q_gain, k_gain, key_cache, value_cache, lengths, w_out, out_scale,
    mlp_gain, w_gate, w_up, gate_scale, up_scale, w_down, down_scale,
):
    V, S = pltpu.VMEM, pltpu.SemaphoreType.DMA
    I32 = jnp.int32
    scratch = [
        V((ROWS, D), BF), V((D,), F32), V((320,), F32), V((HEAD,), F32), V((HEAD,), F32), V((D,), F32), V((D,), F32),
        V((40, 800), I32), V((40, 800), I32), V((800,), F32), V((800,), F32), V((160, HID), I32), V((D,), F32),
        V((320, 1280), I32), V((4, 128, 512), BF), V((4, 128, 512), BF), V((64, HALF), I32), V((512, 512), BF),
        V((8, D), F32), V((8, 1024), F32),
        V((ROWS, 384), F32), V((4, 40, 384), I32), V((4, 56, 256), I32),
        V((16, 4, 384), F32), V((16, 4, 384), F32), V((160, HEAD), F32), V((32, HEAD), F32),
        V((YS, 16, HEAD), BF), V((256, HEAD), BF), V((64, HALF), I32), V((512, HALF), BF), V((ROWS, HALF), BF),
        V((2, YS, 16, 640), BF), V((ALL, D), BF), V((4, ALL, 1280), BF), V((2, ALL, HEAD), F32),
        V((ZS, 160, 384), I32), V((4, 56, 256), I32), V((ZS, 2, 56, 384), I32), V((ZS, 2, 56, 384), I32),
        V((4, 1280, 512), BF), V((2, 256, D), BF), V((2, ROWS, PAD), BF), V((2 * ROWS, D), BF),
        V((4, 2, 16, 1280), BF), V((4, 2, 16, 1280), BF), V((4, 2, 16, 1280), BF), V((4, 2, 16, 1280), BF),
        V((ROWS, HALF), BF), V((YS, ROWS, 384), BF),
        S((18,)), S((2, 4)), S((2, 4)), S((2,)), S((2,)), S((2, 2, 4, 2)), S((2, 2, 4, 2)), S((8,)), S((8,)),
        S((16,)), S((16,)), S((16,)), S((16,)),
        S((2, 8)), S((2, 8)), S((2, 8)), S((2, 8)), S((2, 2, 8)), S((2, 2, 8)), S((2, 8)), S((2, 8)), S((2, 4, 8)), S((2, 4, 8)),
        S((2,)), S((2,)), S((4, 2)), S((4, 2)), S((4, 2)), S((4, 2)), S((4, 2)), S((4, 2)), S((4, 8)), S((4, 8)),
    ]
    vmem = pl.BlockSpec(memory_space=pltpu.VMEM)
    far = pl.BlockSpec(memory_space=pl.ANY)
    specs = [far] * 18
    specs[8] = pl.BlockSpec(memory_space=pltpu.SMEM)
    return pl.pallas_call(
        kernel,
        out_shape=jax.ShapeDtypeStruct((ROWS, 320), BF),
        in_specs=specs,
        out_specs=vmem,
        scratch_shapes=scratch,
        compiler_params=pltpu.CompilerParams(
            collective_id=0, has_side_effects=True, vmem_limit_bytes=60 * 1024 * 1024
        ),
        name="layer",
    )(
        hidden_in, attn_gain, w_qkv.T, qkv_scale, q_gain, k_gain, key_cache, value_cache, lengths, w_out, out_scale,
        mlp_gain, w_gate, w_up, gate_scale, up_scale, w_down.T, down_scale,
    )


def solution(mesh):
    return jax.shard_map(
        local,
        mesh=mesh,
        in_specs=(
            P(("grp", "src"), None),
            P(),
            P(None, "tp"),
            P("tp"),
            P(),
            P(),
            P(("grp", "src"), "tp", None, None),
            P(("grp", "src"), "tp", None, None),
            P(("grp", "src"), "tp"),
            P("tp", None),
            P(),
            P(),
            P(("grp", "src"), "tp"),
            P(("grp", "src"), "tp"),
            P("tp"),
            P("tp"),
            P("tp", ("grp", "src")),
            P(),
        ),
        out_specs=P(("grp", "src"), "tp"),
        check_vma=False,
    )
```

```python
import math

import jax
import jax.numpy as jnp
from jax import lax
from jax.experimental import pallas as pl
from jax.experimental.pallas import tpu as pltpu
from jax.sharding import PartitionSpec as P

D = 5120
HALF = 2560
HEADS = 32
KV = 4
HEAD = 128
ROWS = 64
ALL = 256
YS = 8
ZS = 8
HID = 200
PAD = 256
EPS = 1e-06
ROPE = 1000000.0
MESH = pl.DeviceIdType.MESH
F32 = jnp.float32
BF = jnp.bfloat16
NEAR = (0, 1, 7, 2, 6, 3, 5, 4)


def mo(value, k):
    return pl.multiple_of(value, k)


def byte_of(words, k):
    return jnp.right_shift(jnp.left_shift(words, 24 - 8 * k), 24).astype(F32).astype(BF)


def one_hot(n, used, stride):
    row = lax.broadcasted_iota(jnp.int32, (n, n), 0)
    col = lax.broadcasted_iota(jnp.int32, (n, n), 1)
    shift = stride.bit_length() - 1
    k, r = jnp.right_shift(col, shift), jnp.bitwise_and(col, stride - 1)
    return jnp.where((row == 4 * r + k) & (r < used), 1.0, 0.0).astype(BF)


def dot(a, b):
    return jnp.dot(a, b, preferred_element_type=F32)


def kernel(
    hid_hbm, again_hbm, wq_hbm, qscale_hbm, qgain_hbm, kgain_hbm, kc_hbm, vc_hbm, lens, wout, oscale_hbm, mgain_hbm,
    wgate_hbm, wup_hbm, gscale_hbm, uscale_hbm, wdown_hbm, dscale_hbm,
    out,
    hid, again, qscale, qgain, kgain, oscale, mgain, wgate, wup, gscale, uscale, wdown, dscale,
    wq, kc, vc, woh, p512, p128, p256, picks, half_down, vec, gsc, stage, gu4, dn4, bsend, brecv, qs, vs, hsend, hrecv, wo_r, wo, pm, rs, X, xk, ssq,
    gub, dnp, dnb, dns, wg, wd, actr, pd, pre, smerge, rplain, rmerge, u, yr,
    ld, w1s, w1r, wos, wor, zs, zr, ns, nr, bs, br, hs, hr, rss, rsr, fys, fyr, fxs, fxr, fqs, fqr, fss, fsr,
    acs, acr, xps, xpr, xas, xar, xms, xmr, yss, ysr,
):
    z = lax.axis_index("grp")
    tp = lax.axis_index("tp")
    src = lax.axis_index("src")
    xl, y = tp // YS, tp % YS
    xh, core = src // 2, src % 2
    x = xh * 2 + xl

    def at_x(xx, cc):
        return {"tp": (xx % 2) * YS + y, "src": (xx // 2) * 2 + cc}

    xp, xm, xo = (x + 1) % 4, (x + 3) % 4, (x + 2) % 4
    PLUS, MINUS = at_x(xp, core), at_x(xm, core)
    SIB = {"src": xh * 2 + 1 - core}
    ZP, ZM = {"grp": (z + 1) % ZS}, {"grp": (z + ZS - 1) % ZS}

    def rcopy(a, b, s, r, to):
        return pltpu.make_async_remote_copy(
            src_ref=a, dst_ref=b, send_sem=s, recv_sem=r, device_id=to, device_id_type=MESH
        )

    load_wq = [
        pltpu.make_async_copy(wq_hbm.at[:, pl.ds(i * 640, 640)], wq.at[:, pl.ds(i * 640, 640)], ld.at[i]) for i in (0, 1)
    ]
    load_kc = pltpu.make_async_copy(kc_hbm.at[0], kc, ld.at[2])
    load_vc = pltpu.make_async_copy(vc_hbm.at[0], vc, ld.at[3])
    load_wo = pltpu.make_async_copy(wout.at[:, pl.ds(mo(xl * HALF, 128), HALF)], woh, ld.at[4])
    pairs = (
        (hid_hbm, hid), (again_hbm, again), (wgate_hbm, wgate), (wup_hbm, wup), (wdown_hbm, wdown), (mgain_hbm, mgain),
        (oscale_hbm, oscale), (dscale_hbm, dscale), (qscale_hbm, qscale), (qgain_hbm, qgain), (kgain_hbm, kgain),
        (gscale_hbm, gscale), (uscale_hbm, uscale),
    )
    loads = [pltpu.make_async_copy(a, b, ld.at[5 + i]) for i, (a, b) in enumerate(pairs)]
    for c in loads[2:5] + loads[:2] + loads[5:] + load_wq:
        c.start()
    load_kc.start()
    load_vc.start()
    load_wo.start()

    barrier = pltpu.get_barrier_semaphore()

    def greet_tp(d, _):
        pl.semaphore_signal(barrier, inc=1, device_id={"tp": (tp + d) % 16}, device_id_type=MESH)
        return 0

    def greet_src(d, _):
        pl.semaphore_signal(barrier, inc=1, device_id={"src": (src + d) % 4}, device_id_type=MESH)
        return 0

    lax.fori_loop(1, 16, greet_tp, 0)
    lax.fori_loop(1, 4, greet_src, 0)
    across = {"tp": (1 - xl) * YS + y, "src": (1 - xh) * 2 + core}
    for to in (across, ZP, ZM):
        pl.semaphore_signal(barrier, inc=1, device_id=to, device_id_type=MESH)

    for c in loads:
        c.wait()
    turned = jnp.transpose(wdown[...])
    for s in range(4):
        piece = jnp.concatenate([wgate[:, HID * s : HID * s + HID], wup[:, HID * s : HID * s + HID]], axis=1)
        gu4[s] = piece[:, :384]
        dn4[s] = jnp.zeros((56, 256), jnp.int32)
        dn4[s, 0:50, 0:160] = turned[50 * s : 50 * s + 50, :]
        dn4[s, 0:40, 160:176] = piece[:, 384:400]
    gub[0, pl.ds(mo(src * 40, 8), 40), :] = gu4[src]
    dnp[src] = dn4[src]
    p512[...] = one_hot(512, 128, 128)
    vec[0:1, :] = again[...][None, :]
    vec[1:2, :] = mgain[...][None, :]
    vec[2:3, :] = oscale[...][None, :]
    vec[3:4, :] = dscale[...][None, :]

    total = jnp.zeros((ROWS, 1), F32)
    for g in range(10):
        v = hid[:, g * 512 : (g + 1) * 512].astype(F32)
        total = total + jnp.sum(v * v, axis=1, keepdims=True)
    rms = lax.rsqrt(total * (1.0 / D) + EPS)

    for g in range(10):
        at = slice(g * 512, g * 512 + 512)
        v = (hid[:, at].astype(F32) * rms * vec[0:1, at]).astype(BF)
        xk[:ROWS, at] = dot(v, p512[...]).astype(BF)
    pl.semaphore_wait(barrier, 21)

    def w1_gu(d):
        s2 = (src + d) % 4
        return rcopy(
            gu4.at[s2], gub.at[0, pl.ds(mo(src * 40, 8), 40), :], w1s.at[0, d], w1r.at[0, src], {"src": s2}
        )

    def w1_dn(d):
        s2 = (src + d) % 4
        return rcopy(dn4.at[s2], dnp.at[src], w1s.at[1, d], w1r.at[1, src], {"src": s2})

    for d in (1, 2, 3):
        w1_gu(d).start()
        w1_dn(d).start()

    acc = jnp.zeros((ROWS, 320), F32)
    for c in load_wq:
        c.wait()
    for g in range(10):
        w = wq[:, g * 128 : g * 128 + 128]
        for k in (0, 2):
            acc = acc + lax.dot_general(
                xk[:ROWS, g * 512 + k * 128 : g * 512 + k * 128 + 256],
                jnp.concatenate([byte_of(w, k), byte_of(w, k + 1)], axis=1),
                (((1,), (1,)), ((), ())),
                preferred_element_type=F32,
            )
    qkv = (acc * qscale[...][None, :]).astype(BF).astype(F32)
    stage[...] = jnp.zeros((ROWS, 384), F32)
    stage[:, :320] = qkv
    odd_y = (y % 2) == 1
    placed = stage[...]
    placed = jnp.where(odd_y, pltpu.roll(placed, 64, 1), placed)
    for t in range(16):
        bsend[t] = placed[4 * t : 4 * t + 4, :]

    def b_copy(d):
        to = (tp + d) % 16
        return rcopy(bsend.at[to], brecv.at[tp], bs.at[to], br.at[tp], {"tp": to})

    def start_b(d, _):
        b_copy(d).start()
        return 0

    def wait_b(d, _):
        frm = (tp + d) % 16
        rcopy(bsend.at[frm], brecv.at[frm], bs.at[frm], br.at[frm], {"tp": frm}).wait_recv()
        return 0

    lax.fori_loop(1, 16, start_b, 0)
    wo_side = (x + 1 + 2 * core) % 4
    wo_rows = pl.ds(mo(core * 32, 32), 32)
    wo_copy = rcopy(
        wout.at[wo_rows, pl.ds(mo((1 - xl) * HALF, 128), HALF)], wo_r.at[wo_rows, :], wos.at[0], wor.at[0],
        at_x(wo_side, core),
    )
    wo_share = rcopy(wo_r.at[wo_rows, :], wo_r.at[wo_rows, :], wos.at[1], wor.at[1], SIB)
    wo_copy.start()
    brecv[pl.ds(tp, 1)] = bsend[pl.ds(tp, 1)]

    def w1_in(d):
        s2 = (src + d) % 4
        rcopy(gu4.at[s2], gub.at[0, pl.ds(mo(s2 * 40, 8), 40), :], w1s.at[0, d], w1r.at[0, s2], {"src": s2}).wait_recv()
        rcopy(dn4.at[s2], dnp.at[s2], w1s.at[1, d], w1r.at[1, s2], {"src": s2}).wait_recv()

    def assemble(h):
        one, two = dnp[2 * h], dnp[2 * h + 1]
        dnb[0, h] = jnp.concatenate(
            [one[:, :160], two[:, :160], one[:, 160:192], two[:, 160:192]], axis=1
        )

    def ring(h, step, way):
        a = step - 1 if way == 0 else (9 - step) % 8
        b = step if way == 0 else 8 - step
        to = ZP if way == 0 else ZM
        if step == 4:
            n, off, d_at = (40, 0, slice(0, 32)) if way == 0 else (40, 40, slice(32, 56))
        else:
            n, off, d_at = 80, 0, slice(0, 56)
        at = pl.ds(mo(h * 80 + off, 8), n)
        one = rcopy(gub.at[a, at, :], gub.at[b, at, :], zs.at[h, way, step - 1, 0], zr.at[h, way, step - 1, 0], to)
        two = rcopy(
            dnb.at[a, h, d_at, :], dnb.at[b, h, d_at, :], zs.at[h, way, step - 1, 1], zr.at[h, way, step - 1, 1], to
        )
        return one, two

    def ring_start(h, step):
        for way in (0, 1):
            for c in ring(h, step, way):
                c.start()

    def ring_wait(h, step):
        for way in (0, 1):
            for c in ring(h, step, way):
                c.wait_recv()

    def to_sib(slot):
        return rcopy(dnb.at[slot], dns.at[slot], ns.at[slot], nr.at[slot], SIB)

    def hop(stream, step):
        h = xh if stream == 0 else 1 - xh
        ring_wait(h, step)
        if step < 4:
            ring_start(h, step + 1)
        if stream == 1:
            to_sib(step).start()
            if step < 4:
                to_sib(8 - step).start()

    def unpack_down(ref, slot, which):
        zz = (z + ZS - slot) % ZS
        w = jnp.concatenate([ref[slot, 0, :, :320], ref[slot, 1, :, :320]], axis=1)
        for k in range(4):
            wd[which, k * 64 : k * 64 + 56, pl.ds(mo(zz * 640, 128), 640)] = byte_of(w, k)

    lane40 = lax.broadcasted_iota(jnp.int32, (40, 128), 1)

    def unpack(slot):
        zz = (z + ZS - slot) % ZS

        def rows(i, _):
            w = gub[slot, pl.ds(mo(i * 32, 32), 32), :]
            for k in range(4):
                wg[pl.ds(mo(k * 1280 + zz * 160 + i * 32, 32), 32), 0:384] = byte_of(w, k)
            return 0

        lax.fori_loop(0, 5, rows, 0)
        tails = []
        for s in range(4):
            t = dnb[slot, s // 2, 0:40, 256:384]
            t = pltpu.roll(t, 64 - 32 * (s % 2), 1)
            tails.append(jnp.where(lane40 < 16, t, 0))
        tails = jnp.concatenate(tails, axis=0)
        for k in range(4):
            wg[pl.ds(mo(k * 1280 + zz * 160, 32), 160), 384:512] = byte_of(tails, k)
        unpack_down(dnb, slot, 0)

    def unpack_sib(slot):
        to_sib(slot).wait_recv()
        unpack_down(dns, slot, 1)

    rcopy(
        gu4.at[0], gub.at[0, pl.ds(mo((src + 1 - 2 * core) * 40, 8), 40), :], w1s.at[0, 1],
        w1r.at[0, src + 1 - 2 * core], SIB,
    ).wait_recv()
    rcopy(dn4.at[0], dnp.at[src + 1 - 2 * core], w1s.at[1, 1], w1r.at[1, src + 1 - 2 * core], SIB).wait_recv()
    assemble(xh)
    ring_start(xh, 1)
    wd[...] = jnp.zeros(wd.shape, BF)

    def unpack_wo(ref, base):
        def cols(i, _):
            at = pl.ds(mo(i * 640, 128), 640)
            for hl in range(2):
                w = ref[hl * 32 : hl * 32 + 32, at]
                for k in range(4):
                    wo[pl.ds(mo(base + hl * 128 + k * 32, 32), 32), at] = byte_of(w, k)
            return 0

        lax.fori_loop(0, 4, cols, 0)

    load_wo.wait()
    unpack_wo(woh, xl * 256)
    far = (1 - xh) * 2
    for s2 in (far, far + 1):
        rcopy(gu4.at[0], gub.at[0, pl.ds(mo(s2 * 40, 8), 40), :], w1s.at[0, 2], w1r.at[0, s2], {"src": s2}).wait_recv()
        rcopy(dn4.at[0], dnp.at[s2], w1s.at[1, 2], w1r.at[1, s2], {"src": s2}).wait_recv()
    assemble(1 - xh)
    ring_start(1 - xh, 1)
    to_sib(0).start()
    load_kc.wait()
    load_vc.wait()
    half = lax.broadcasted_iota(jnp.int32, (8, HEAD), 1)
    pair = jnp.bitwise_and(lax.broadcasted_iota(jnp.int32, (8, HEAD), 0), 3)
    length = jnp.full((8, HEAD), lens[0, 0], jnp.int32)
    for b in range(1, 4):
        length = jnp.where(pair == b, lens[0, b], length)
    freq = jnp.exp(jnp.bitwise_and(half, 63).astype(F32) * (-math.log(ROPE) / 64))
    angle = length.astype(F32) * freq
    ctab = jnp.cos(angle)
    stab = jnp.sin(angle)
    stab = jnp.where(half < 64, -stab, stab)

    p128[...] = one_hot(128, 32, 32)
    p256[...] = one_hot(PAD, HID // 4, 64)
    t = lax.broadcasted_iota(jnp.int32, (ROWS, 256), 0)
    c = lax.broadcasted_iota(jnp.int32, (ROWS, 256), 1)
    for hl in range(4):
        want = jnp.right_shift(t, 2) * 16 + hl * 4 + jnp.bitwise_and(t, 3)
        picks[hl] = jnp.where(c == want, 1.0, 0.0).astype(BF)
    lax.fori_loop(1, 16, wait_b, 0)
    wo_copy.wait_recv()
    wo_share.start()
    lane = lax.broadcasted_iota(jnp.int32, (4, HEAD), 1)
    for p in range(8):
        even, odd = brecv[2 * p], brecv[2 * p + 1]
        pieces = (
            even[:, 0:128],
            even[:, 128:256],
            jnp.where(lane < 64, even[:, 256:384], odd[:, 0:128]),
            odd[:, 128:256],
            odd[:, 256:384],
        )
        for j, piece in enumerate(pieces):
            h = 5 * p + j
            if h < HEADS:
                qs[4 * h : 4 * h + 4, :] = piece
            elif h < HEADS + KV:
                at = 128 + 8 * (h - HEADS)
                qs[at : at + 4, :] = piece
                qs[at + 4 : at + 8, :] = piece
            else:
                at = 8 * (h - HEADS - KV)
                vs[at : at + 4, :] = piece
                vs[at + 4 : at + 8, :] = piece
    v = qs[...]
    v = v * lax.rsqrt(jnp.mean(v * v, axis=1, keepdims=True) + EPS)
    row = lax.broadcasted_iota(jnp.int32, (160, HEAD), 0)
    v = v * jnp.where(row < 128, qgain[...][None, :], kgain[...][None, :])
    turned = pltpu.roll(v, 64, 1)
    v = v.reshape(20, 8, HEAD) * ctab[None] + turned.reshape(20, 8, HEAD) * stab[None]
    v = v.reshape(160, HEAD).astype(BF)
    scale = 1.0 / math.sqrt(HEAD)
    seq = jnp.bitwise_and(lax.broadcasted_iota(jnp.int32, (32, HEAD), 0), 3)
    live = jnp.where(half < length, 1.0, 0.0)
    live = jnp.broadcast_to(live[None], (4, 8, HEAD)).reshape(32, HEAD) > 0.5
    heads = []
    for g in range(KV):
        q = v[32 * g : 32 * g + 32]
        newk = v[128 + 8 * g : 136 + 8 * g].astype(F32)
        own = jnp.sum((q.astype(F32).reshape(4, 8, HEAD) * newk[None]).reshape(32, HEAD), axis=1, keepdims=True)
        own = own * scale
        s = jnp.zeros((32, HEAD), F32)
        for b in range(4):
            sb = lax.dot_general(
                q, kc[b, :, g * 128 : (g + 1) * 128], (((1,), (1,)), ((), ())), preferred_element_type=F32
            )
            s = jnp.where(seq == b, sb, s)
        s = jnp.where(live, s * scale, -jnp.inf)
        top = jnp.maximum(jnp.max(s, axis=1, keepdims=True), own)
        e = jnp.exp(s - top)
        own_e = jnp.exp(own - top)
        den = jnp.sum(e, axis=1, keepdims=True) + own_e
        newv = vs[8 * g : 8 * g + 8, :]
        low = own_e.astype(BF).astype(F32)
        num = (low.reshape(4, 8, 1) * newv[None]).reshape(32, HEAD)
        for b in range(4):
            eb = jnp.where(seq == b, e, 0.0).astype(BF)
            num = num + dot(eb, vc[b, :, g * 128 : (g + 1) * 128])
        heads.append(num / den)
    for yy in range(YS):
        g, at = yy // 4, 8 * (yy % 4)
        hsend[yy] = jnp.concatenate([heads[g][at : at + 8], heads[g + 2][at : at + 8]], axis=0).astype(BF)

    def h_slot(t):
        return hrecv.at[pl.ds(mo(t * 16, 16), 16), :]

    def h_copy(d):
        to = (tp + d) % 16
        return rcopy(hsend.at[to % YS], h_slot(tp), hs.at[to], hr.at[tp], {"tp": to})

    def start_h(d, _):
        h_copy(d).start()
        return 0

    def wait_h(d, _):
        frm = (tp + d) % 16
        rcopy(hsend.at[frm % YS], h_slot(frm), hs.at[frm], hr.at[frm], {"tp": frm}).wait_recv()
        return 0

    lax.fori_loop(1, 16, start_h, 0)
    hrecv[pl.ds(mo(tp * 16, 16), 16), :] = hsend[y]

    hop(0, 1)
    unpack(0)
    wo_share.wait_recv()
    unpack_wo(wo_r, (1 - xl) * 256)
    hop(1, 1)

    lax.fori_loop(1, 16, wait_h, 0)
    got = hrecv[...]
    zcat = [dot(dot(picks[hl], got).astype(BF), p128[...]).astype(BF) for hl in range(4)]
    zcat = jnp.concatenate(zcat, axis=1)

    def part(yy, s):
        return pl.ds(mo(32 * (yy // 4) + 16 * s, 16), 16), pl.ds(mo(640 * (yy % 4), 128), 640)

    for cb in range(4):
        pm[:, cb * 640 : cb * 640 + 640] = dot(zcat, wo[:, cb * 640 : cb * 640 + 640]).astype(BF)

    def r_copy(d, s):
        to = (y + d) % YS
        a, b = part(to, s)
        return rcopy(pm.at[a, b], rs.at[s, y], rss.at[s, to], rsr.at[s, y], {"tp": xl * YS + to})

    def wait_r(d, s):
        frm = (y + d) % YS
        a, b = part(frm, s)
        rcopy(pm.at[a, b], rs.at[s, frm], rss.at[s, frm], rsr.at[s, frm], {"tp": xl * YS + frm}).wait_recv()

    for s in (0, 1):
        for d in NEAR[:0:-1]:
            r_copy(d, s).start()
        a, b = part(y, s)
        rs[s, y] = pm[a, b]
    unpack(1)
    unpack(7)
    unpack_sib(0)
    hop(0, 2)

    def blk(xx, cc, yy, s):
        r0 = ((xx // 2) * 2 + cc) * 64 + 32 * (yy // 4) + 16 * s
        c0 = (xx % 2) * HALF + 640 * (yy % 4)
        return X.at[pl.ds(mo(r0, 16), 16), pl.ds(mo(c0, 128), 640)]

    def fy_copy(n, s):
        i, hop_by = ((0, 1), (0, 7), (0, 2), (0, 6), (6, 1), (2, 7), (6, 2) if s == 0 else (2, 6))[n]
        yy, to = (y + i) % YS, (y + hop_by) % YS
        b0 = blk(x, core, yy, s)
        return rcopy(b0, b0, fys.at[s, n], fyr.at[s, yy], {"tp": xl * YS + to})

    def fx_copy(way, i, s):
        b0 = blk(x, core, (y + i) % YS, s)
        return rcopy(b0, b0, fxs.at[s, way, i], fxr.at[s, way, i], PLUS if way == 0 else MINUS)

    def fx_in(way, i, s):
        b0 = blk(xm if way == 0 else xp, core, (y + i) % YS, s)
        return rcopy(b0, b0, fxs.at[s, way, i], fxr.at[s, way, i], MINUS if way == 0 else PLUS)

    def fq_copy(i, s):
        way = i % 2
        b0 = blk(xm if way == 0 else xp, core, (y + i) % YS, s)
        return rcopy(b0, b0, fqs.at[s, i], fqr.at[s, i], PLUS if way == 0 else MINUS)

    def fq_in(i, s):
        b0 = blk(xo, core, (y + i) % YS, s)
        return rcopy(b0, b0, fqs.at[s, i], fqr.at[s, i], MINUS if i % 2 == 0 else PLUS)

    froms = (x, xm, xp, xo)

    def fs_copy(j, i, s):
        b0 = blk(froms[j], core, (y + i) % YS, s)
        return rcopy(b0, b0, fss.at[s, j, i], fsr.at[s, j, i], SIB)

    def fs_in(j, i, s):
        b0 = blk(froms[j], 1 - core, (y + i) % YS, s)
        return rcopy(b0, b0, fss.at[s, j, i], fsr.at[s, j, i], SIB)

    def gained(xx, cc):
        at = pl.ds(mo(((xx // 2) * 2 + cc) * 64, 64), 64)
        total = jnp.zeros((64, 1), F32)
        for g in range(5):
            c0 = (xx % 2) * HALF + g * 512
            cs = pl.ds(mo(c0, 128), 512)
            v = X[at, cs].astype(F32)
            total = total + jnp.sum(v * v, axis=1, keepdims=True)
            v = dot((v * vec[1:2, cs]).astype(BF), p512[...]).astype(BF)
            for k in range(4):
                to = pl.ds(mo(k * 1280 + (xx % 2) * 640 + g * 128, 128), 128)
                xk[at, to] = v[:, k * 128 : (k + 1) * 128]
        ssq[xx % 2, at, :] = jnp.broadcast_to(total, (64, HEAD))

    def onward(i, s):
        fx_copy(0, i, s).start()
        fx_copy(1, i, s).start()
        fs_copy(0, i, s).start()

    def mid(s):
        for d in NEAR[1:]:
            wait_r(d, s)
        m = rs[s, 0].astype(F32)
        for i in range(1, YS):
            m = m + rs[s, i].astype(F32)
        cols = pl.ds(mo(xl * HALF + 640 * (y % 4), 128), 640)
        m = hid[pl.ds(mo(32 * (y // 4) + 16 * s, 16), 16), cols].astype(F32) + m * vec[2:3, cols]
        X[pl.ds(mo(src * 64 + 32 * (y // 4) + 16 * s, 16), 16), cols] = m.astype(BF)
        for n in range(4):
            fy_copy(n, s).start()
        onward(0, s)

    def from_y(i, s):
        yy = (y + i) % YS
        b0 = blk(x, core, yy, s)
        rcopy(b0, b0, fys.at[s, yy], fyr.at[s, yy], {"tp": xl * YS + yy}).wait_recv()
        if i in (2, 6):
            fy_copy(4 if i == 6 else 5, s).start()
            if i == (6 if s == 0 else 2):
                fy_copy(6, s).start()
        onward(i, s)

    def from_x(i, s):
        fx_in(0, i, s).wait_recv()
        fx_in(1, i, s).wait_recv()
        fq_copy(i, s).start()
        fs_copy(1, i, s).start()
        fs_copy(2, i, s).start()

    def from_sib(j):
        for s in (0, 1):
            for i in NEAR:
                fs_in(j, i, s).wait_recv()
        gained(froms[j], 1 - core)

    mid(0)
    hop(1, 2)
    mid(1)
    for i in NEAR[1:]:
        from_y(i, 0)
    from_x(0, 0)
    hop(0, 3)
    unpack(2)
    unpack(6)
    for i in NEAR[1:]:
        from_y(i, 1)
        from_x(i, 0)
    gained(x, core)
    for i in NEAR:
        from_x(i, 1)
    hop(1, 3)
    gained(xm, core)
    gained(xp, core)
    for s in (0, 1):
        for i in NEAR:
            fq_in(i, s).wait_recv()
            fs_copy(3, i, s).start()
    gained(xo, core)
    unpack(3)
    unpack(5)
    unpack_sib(1)
    unpack_sib(7)
    unpack_sib(2)
    unpack_sib(6)
    for j in (0, 1, 2):
        from_sib(j)
    hop(0, 4)
    hop(1, 4)
    unpack(4)
    unpack_sib(3)
    unpack_sib(5)
    from_sib(3)
    gsc[...] = jnp.zeros((8, 1024), F32)
    gsc[0:1, :800] = gscale[...][None, :]
    gsc[1:2, :800] = uscale[...][None, :]
    shifted = gsc[...]
    mine = shifted
    for s in range(1, 4):
        mine = jnp.where(src == s, pltpu.roll(shifted, 1024 - HID * s, 1), mine)
    both = dot(xk[...], wg[...])
    rms = lax.rsqrt((ssq[0, :, 0:1] + ssq[1, :, 0:1]) * (1.0 / D) + EPS)
    gate = both[:, :PAD] * rms * mine[0:1, :PAD]
    up = pltpu.roll(both, 512 - HID, 1)[:, :PAD] * rms * mine[1:2, :PAD]
    used = lax.broadcasted_iota(jnp.int32, (1, PAD), 1) < HID
    act = jnp.where(used, gate / (1.0 + jnp.exp(-gate)) * up, 0.0).astype(BF)
    act = dot(act, p256[...]).astype(BF)
    xk[:, :PAD] = act

    def act_rows(h, cc):
        return pl.ds(mo((h * 2 + cc) * 64, 64), 64)

    def ac_copy(h):
        return rcopy(xk.at[act_rows(h, 1 - core), 0:PAD], actr.at[h], acs.at[h], acr.at[h], SIB)

    for h in (0, 1):
        ac_copy(h).start()
    unpack_sib(4)
    own_act = jnp.concatenate([xk[act_rows(0, core), 0:PAD], xk[act_rows(1, core), 0:PAD]], axis=0)

    def first(n, _):
        half_down[:, pl.ds(mo(n * 640, 128), 640)] = dot(own_act, wd[0, :, pl.ds(mo(xl * HALF + n * 640, 128), 640)])
        return 0

    lax.fori_loop(0, 4, first, 0)
    for h in (0, 1):
        ac_copy(h).wait_recv()
    sib_act = jnp.concatenate([actr[0], actr[1]], axis=0)

    def second(n, _):
        at = pl.ds(mo(xl * HALF + n * 640, 128), 640)
        pd[:, at] = (half_down[:, pl.ds(mo(n * 640, 128), 640)] + dot(sib_act, wd[1, :, at])).astype(BF)
        return 0

    def other(n, _):
        at = pl.ds(mo((1 - xl) * HALF + n * 640, 128), 640)
        pd[:, at] = (dot(own_act, wd[0, :, at]) + dot(sib_act, wd[1, :, at])).astype(BF)
        return 0

    sides = (PLUS, MINUS)
    nexts = (xp, xm)

    def slab(xx, q, w):
        rows = pl.ds(mo((xx // 2) * 64 + q * 16, 16), 16)
        return rows, pl.ds(mo((xx % 2) * HALF + w * 1280, 128), 1280)

    def pre_copy(q, w):
        a, b = slab(xo, q, w)
        return rcopy(pd.at[a, b], pre.at[q, w], xps.at[q, w], xpr.at[q, w], sides[w])

    def plain_copy(q, w):
        a, b = slab(nexts[w], q, 1 - w)
        return rcopy(pd.at[a, b], rplain.at[q, w], xas.at[q, w], xar.at[q, w], sides[w])

    def merge_copy(q, w):
        return rcopy(smerge.at[q, w], rmerge.at[q, w], xms.at[q, w], xmr.at[q, w], sides[w])

    def pre_start(q):
        for w in (0, 1):
            pre_copy(q, w).start()

    def plain_start(q):
        for w in (0, 1):
            plain_copy(q, w).start()

    def merge(q):
        for w in (0, 1):
            pre_copy(q, w).wait_recv()
            a, b = slab(nexts[w], q, w)
            smerge[q, w] = (pd[a, b].astype(F32) + pre[q, w].astype(F32)).astype(BF)
            merge_copy(q, w).start()

    def window(yy):
        return pl.ds(mo(320 * yy - 64 * (yy % 2), 128), 384)

    def y_copy(d, q):
        to = (y + d) % YS
        at = pl.ds(q * 16, 16)
        return rcopy(u.at[at, window(to)], yr.at[y, at, :], yss.at[q, to], ysr.at[q, y], {"tp": xl * YS + to})

    def y_in(d, q):
        frm = (y + d) % YS
        at = pl.ds(q * 16, 16)
        return rcopy(u.at[at, window(frm)], yr.at[frm, at, :], yss.at[q, frm], ysr.at[q, frm], {"tp": xl * YS + frm})

    def finish(q):
        at = slice(q * 16, q * 16 + 16)
        for w in (0, 1):
            plain_copy(q, w).wait_recv()
        for w in (0, 1):
            merge_copy(q, w).wait_recv()
            a, b = slab(x, q, w)
            v = pd[a, b].astype(F32) + rplain[q, 1 - w].astype(F32) + rmerge[q, w].astype(F32)
            u[at, w * 1280 : w * 1280 + 1280] = v.astype(BF)
        for d in NEAR[:0:-1]:
            y_copy(d, q).start()
        yr[y, at, :] = u[at, window(y)]

    lax.fori_loop(0, 4, second, 0)
    pre_start(0)
    pre_start(1)
    lax.fori_loop(0, 4, other, 0)
    plain_start(0)
    merge(0)
    pre_start(2)
    plain_start(1)
    merge(1)
    pre_start(3)
    plain_start(2)
    finish(0)
    merge(2)
    plain_start(3)
    finish(1)
    merge(3)
    finish(2)
    finish(3)
    for d in (1, 2, 3):
        w1_gu(d).wait_send()
        w1_dn(d).wait_send()
    wo_copy.wait_send()
    wo_share.wait_send()
    for h in (0, 1):
        for step in (1, 2, 3, 4):
            for way in (0, 1):
                for c in ring(h, step, way):
                    c.wait_send()
    for slot in range(ZS):
        to_sib(slot).wait_send()

    def sent_tp(d, _):
        b_copy(d).wait_send()
        h_copy(d).wait_send()
        return 0

    lax.fori_loop(1, 16, sent_tp, 0)
    for d in NEAR[1:]:
        for s in (0, 1):
            r_copy(d, s).wait_send()
    for s in (0, 1):
        for n in range(7):
            fy_copy(n, s).wait_send()
        for i in range(YS):
            fx_copy(0, i, s).wait_send()
            fx_copy(1, i, s).wait_send()
            fq_copy(i, s).wait_send()
            for j in range(4):
                fs_copy(j, i, s).wait_send()
    for w in (0, 1):
        ac_copy(w).wait_send()
        for q in range(4):
            pre_copy(q, w).wait_send()
            plain_copy(q, w).wait_send()
            merge_copy(q, w).wait_send()
    for q in range(4):
        for d in NEAR[1:]:
            y_in(d, q).wait_recv()
    last = yr[0].astype(F32)
    for i in range(1, YS):
        last = last + yr[i].astype(F32)
    at = pl.ds(mo(xl * HALF + 320 * y - 64 * (y % 2), 128), 384)
    last = X[pl.ds(mo(src * 64, 64), 64), at].astype(F32) + last * vec[3:4, at]
    last = jnp.where(odd_y, pltpu.roll(last, 320, 1), last)
    out[...] = last[:, :320].astype(BF)

    for q in range(4):
        for d in NEAR[1:]:
            y_copy(d, q).wait_send()


def local(
    hidden_in, attn_gain, w_qkv, qkv_scale, q_gain, k_gain, key_cache, value_cache, lengths, w_out, out_scale,
    mlp_gain, w_gate, w_up, gate_scale, up_scale, w_down, down_scale,
):
    V, S = pltpu.VMEM, pltpu.SemaphoreType.DMA
    I32 = jnp.int32
    scratch = [
        V((ROWS, D), BF), V((D,), F32), V((320,), F32), V((HEAD,), F32), V((HEAD,), F32), V((D,), F32), V((D,), F32),
        V((40, 800), I32), V((40, 800), I32), V((800,), F32), V((800,), F32), V((160, HID), I32), V((D,), F32),
        V((320, 1280), I32), V((4, 128, 512), BF), V((4, 128, 512), BF), V((64, HALF), I32), V((512, 512), BF),
        V((HEAD, HEAD), BF), V((PAD, PAD), BF), V((4, ROWS, 256), BF), V((2 * ROWS, HALF), F32),
        V((8, D), F32), V((8, 1024), F32),
        V((ROWS, 384), F32), V((4, 40, 384), I32), V((4, 56, 256), I32),
        V((16, 4, 384), F32), V((16, 4, 384), F32), V((160, HEAD), F32), V((32, HEAD), F32),
        V((YS, 16, HEAD), BF), V((256, HEAD), BF), V((64, HALF), I32), V((512, HALF), BF), V((ROWS, HALF), BF),
        V((2, YS, 16, 640), BF), V((ALL, D), BF), V((ALL, D), BF), V((2, ALL, HEAD), F32),
        V((ZS, 160, 384), I32), V((4, 56, 256), I32), V((ZS, 2, 56, 384), I32), V((ZS, 2, 56, 384), I32),
        V((D, 512), BF), V((2, 256, D), BF), V((2, ROWS, PAD), BF), V((2 * ROWS, D), BF),
        V((4, 2, 16, 1280), BF), V((4, 2, 16, 1280), BF), V((4, 2, 16, 1280), BF), V((4, 2, 16, 1280), BF),
        V((ROWS, HALF), BF), V((YS, ROWS, 384), BF),
        S((18,)), S((2, 4)), S((2, 4)), S((2,)), S((2,)), S((2, 2, 4, 2)), S((2, 2, 4, 2)), S((8,)), S((8,)),
        S((16,)), S((16,)), S((16,)), S((16,)),
        S((2, 8)), S((2, 8)), S((2, 8)), S((2, 8)), S((2, 2, 8)), S((2, 2, 8)), S((2, 8)), S((2, 8)), S((2, 4, 8)), S((2, 4, 8)),
        S((2,)), S((2,)), S((4, 2)), S((4, 2)), S((4, 2)), S((4, 2)), S((4, 2)), S((4, 2)), S((4, 8)), S((4, 8)),
    ]
    vmem = pl.BlockSpec(memory_space=pltpu.VMEM)
    far = pl.BlockSpec(memory_space=pl.ANY)
    specs = [far] * 18
    specs[8] = pl.BlockSpec(memory_space=pltpu.SMEM)
    return pl.pallas_call(
        kernel,
        out_shape=jax.ShapeDtypeStruct((ROWS, 320), BF),
        in_specs=specs,
        out_specs=vmem,
        scratch_shapes=scratch,
        compiler_params=pltpu.CompilerParams(
            collective_id=0, has_side_effects=True, vmem_limit_bytes=60 * 1024 * 1024
        ),
        name="layer",
    )(
        hidden_in, attn_gain, w_qkv.T, qkv_scale, q_gain, k_gain, key_cache, value_cache, lengths, w_out, out_scale,
        mlp_gain, w_gate, w_up, gate_scale, up_scale, w_down.T, down_scale,
    )


def solution(mesh):
    return jax.shard_map(
        local,
        mesh=mesh,
        in_specs=(
            P(("grp", "src"), None),
            P(),
            P(None, "tp"),
            P("tp"),
            P(),
            P(),
            P(("grp", "src"), "tp", None, None),
            P(("grp", "src"), "tp", None, None),
            P(("grp", "src"), "tp"),
            P("tp", None),
            P(),
            P(),
            P(("grp", "src"), "tp"),
            P(("grp", "src"), "tp"),
            P("tp"),
            P("tp"),
            P("tp", ("grp", "src")),
            P(),
        ),
        out_specs=P(("grp", "src"), "tp"),
        check_vma=False,
    )
```

```python
import math

import jax
import jax.numpy as jnp
from jax import lax
from jax.experimental import pallas as pl
from jax.experimental.pallas import tpu as pltpu
from jax.sharding import PartitionSpec as P

D = 5120
HALF = 2560
HEADS = 32
KV = 4
HEAD = 128
ROWS = 64
ALL = 256
YS = 8
ZS = 8
HID = 200
PAD = 256
EPS = 1e-06
ROPE = 1000000.0
MESH = pl.DeviceIdType.MESH
F32 = jnp.float32
BF = jnp.bfloat16
NEAR = (0, 1, 7, 2, 6, 3, 5, 4)


def mo(value, k):
    return pl.multiple_of(value, k)


def byte_of(words, k):
    return jnp.right_shift(jnp.left_shift(words, 24 - 8 * k), 24).astype(F32).astype(BF)


def one_hot(n, used, stride):
    row = lax.broadcasted_iota(jnp.int32, (n, n), 0)
    col = lax.broadcasted_iota(jnp.int32, (n, n), 1)
    shift = stride.bit_length() - 1
    k, r = jnp.right_shift(col, shift), jnp.bitwise_and(col, stride - 1)
    return jnp.where((row == 4 * r + k) & (r < used), 1.0, 0.0).astype(BF)


def dot(a, b):
    return jnp.dot(a, b, preferred_element_type=F32)


def kernel(
    hid_hbm, again_hbm, wq_hbm, qscale_hbm, qgain_hbm, kgain_hbm, kc_hbm, vc_hbm, lens, wout, oscale_hbm, mgain_hbm,
    wgate_hbm, wup_hbm, gscale_hbm, uscale_hbm, wdown_hbm, dscale_hbm,
    out,
    hid, again, qscale, qgain, kgain, oscale, mgain, wgate, wup, gscale, uscale, wdown, dscale,
    wq, kc, vc, woh, p512, p128, p256, picks, half_down, vec, gsc, stage, gu4, dn4, bsend, brecv, qs, vs, hsend, hrecv, wo_r, wo, pm, rs, X, xk, ssq,
    gub, dnp, dnb, dns, wg, wd, actr, pd, pre, smerge, rplain, rmerge, u, yr,
    ld, w1s, w1r, wos, wor, zs, zr, ns, nr, bs, br, hs, hr, rss, rsr, fys, fyr, fxs, fxr, fqs, fqr, fss, fsr,
    acs, acr, xps, xpr, xas, xar, xms, xmr, yss, ysr,
):
    z = lax.axis_index("grp")
    tp = lax.axis_index("tp")
    src = lax.axis_index("src")
    xl, y = tp // YS, tp % YS
    xh, core = src // 2, src % 2
    x = xh * 2 + xl

    def at_x(xx, cc):
        return {"tp": (xx % 2) * YS + y, "src": (xx // 2) * 2 + cc}

    xp, xm, xo = (x + 1) % 4, (x + 3) % 4, (x + 2) % 4
    PLUS, MINUS = at_x(xp, core), at_x(xm, core)
    SIB = {"src": xh * 2 + 1 - core}
    ZP, ZM = {"grp": (z + 1) % ZS}, {"grp": (z + ZS - 1) % ZS}

    def rcopy(a, b, s, r, to):
        return pltpu.make_async_remote_copy(
            src_ref=a, dst_ref=b, send_sem=s, recv_sem=r, device_id=to, device_id_type=MESH
        )

    load_wq = [
        pltpu.make_async_copy(wq_hbm.at[:, pl.ds(i * 640, 640)], wq.at[:, pl.ds(i * 640, 640)], ld.at[i]) for i in (0, 1)
    ]
    load_kc = pltpu.make_async_copy(kc_hbm.at[0], kc, ld.at[2])
    load_vc = pltpu.make_async_copy(vc_hbm.at[0], vc, ld.at[3])
    load_wo = pltpu.make_async_copy(wout.at[:, pl.ds(mo(xl * HALF, 128), HALF)], woh, ld.at[4])
    pairs = (
        (hid_hbm, hid), (again_hbm, again), (wgate_hbm, wgate), (wup_hbm, wup), (wdown_hbm, wdown), (mgain_hbm, mgain),
        (oscale_hbm, oscale), (dscale_hbm, dscale), (qscale_hbm, qscale), (qgain_hbm, qgain), (kgain_hbm, kgain),
        (gscale_hbm, gscale), (uscale_hbm, uscale),
    )
    loads = [pltpu.make_async_copy(a, b, ld.at[5 + i]) for i, (a, b) in enumerate(pairs)]
    for c in loads[2:5] + loads[:2] + loads[5:] + load_wq:
        c.start()
    load_kc.start()
    load_vc.start()
    load_wo.start()

    barrier = pltpu.get_barrier_semaphore()

    def greet_tp(d, _):
        pl.semaphore_signal(barrier, inc=1, device_id={"tp": (tp + d) % 16}, device_id_type=MESH)
        return 0

    def greet_src(d, _):
        pl.semaphore_signal(barrier, inc=1, device_id={"src": (src + d) % 4}, device_id_type=MESH)
        return 0

    lax.fori_loop(1, 16, greet_tp, 0)
    lax.fori_loop(1, 4, greet_src, 0)
    across = {"tp": (1 - xl) * YS + y, "src": (1 - xh) * 2 + core}
    for to in (across, ZP, ZM):
        pl.semaphore_signal(barrier, inc=1, device_id=to, device_id_type=MESH)

    for c in loads:
        c.wait()
    turned = jnp.transpose(wdown[...])
    for s in range(4):
        piece = jnp.concatenate([wgate[:, HID * s : HID * s + HID], wup[:, HID * s : HID * s + HID]], axis=1)
        gu4[s] = piece[:, :384]
        dn4[s] = jnp.zeros((56, 256), jnp.int32)
        dn4[s, 0:50, 0:160] = turned[50 * s : 50 * s + 50, :]
        dn4[s, 0:40, 160:176] = piece[:, 384:400]
    gub[0, pl.ds(mo(src * 40, 8), 40), :] = gu4[src]
    dnp[src] = dn4[src]
    p512[...] = one_hot(512, 128, 128)
    vec[0:1, :] = again[...][None, :]
    vec[1:2, :] = mgain[...][None, :]
    vec[2:3, :] = oscale[...][None, :]
    vec[3:4, :] = dscale[...][None, :]

    total = jnp.zeros((ROWS, 1), F32)
    for g in range(10):
        v = hid[:, g * 512 : (g + 1) * 512].astype(F32)
        total = total + jnp.sum(v * v, axis=1, keepdims=True)
    rms = lax.rsqrt(total * (1.0 / D) + EPS)

    for g in range(10):
        at = slice(g * 512, g * 512 + 512)
        v = (hid[:, at].astype(F32) * rms * vec[0:1, at]).astype(BF)
        xk[:ROWS, at] = dot(v, p512[...]).astype(BF)
    pl.semaphore_wait(barrier, 21)

    def w1_gu(d):
        s2 = (src + d) % 4
        return rcopy(
            gu4.at[s2], gub.at[0, pl.ds(mo(src * 40, 8), 40), :], w1s.at[0, d], w1r.at[0, src], {"src": s2}
        )

    def w1_dn(d):
        s2 = (src + d) % 4
        return rcopy(dn4.at[s2], dnp.at[src], w1s.at[1, d], w1r.at[1, src], {"src": s2})

    for d in (1, 2, 3):
        w1_gu(d).start()
        w1_dn(d).start()

    acc = jnp.zeros((ROWS, 320), F32)
    for c in load_wq:
        c.wait()
    for g in range(10):
        w = wq[:, g * 128 : g * 128 + 128]
        for k in (0, 2):
            acc = acc + lax.dot_general(
                xk[:ROWS, g * 512 + k * 128 : g * 512 + k * 128 + 256],
                jnp.concatenate([byte_of(w, k), byte_of(w, k + 1)], axis=1),
                (((1,), (1,)), ((), ())),
                preferred_element_type=F32,
            )
    qkv = (acc * qscale[...][None, :]).astype(BF).astype(F32)
    stage[...] = jnp.zeros((ROWS, 384), F32)
    stage[:, :320] = qkv
    odd_y = (y % 2) == 1
    placed = stage[...]
    placed = jnp.where(odd_y, pltpu.roll(placed, 64, 1), placed)
    for t in range(16):
        bsend[t] = placed[4 * t : 4 * t + 4, :]

    def b_copy(d):
        to = (tp + d) % 16
        return rcopy(bsend.at[to], brecv.at[tp], bs.at[to], br.at[tp], {"tp": to})

    def start_b(d, _):
        b_copy(d).start()
        return 0

    def wait_b(d, _):
        frm = (tp + d) % 16
        rcopy(bsend.at[frm], brecv.at[frm], bs.at[frm], br.at[frm], {"tp": frm}).wait_recv()
        return 0

    lax.fori_loop(1, 16, start_b, 0)
    wo_side = (x + 1 + 2 * core) % 4
    wo_rows = pl.ds(mo(core * 32, 32), 32)
    wo_copy = rcopy(
        wout.at[wo_rows, pl.ds(mo((1 - xl) * HALF, 128), HALF)], wo_r.at[wo_rows, :], wos.at[0], wor.at[0],
        at_x(wo_side, core),
    )
    wo_share = rcopy(wo_r.at[wo_rows, :], wo_r.at[wo_rows, :], wos.at[1], wor.at[1], SIB)
    wo_copy.start()
    brecv[pl.ds(tp, 1)] = bsend[pl.ds(tp, 1)]

    def w1_in(d):
        s2 = (src + d) % 4
        rcopy(gu4.at[s2], gub.at[0, pl.ds(mo(s2 * 40, 8), 40), :], w1s.at[0, d], w1r.at[0, s2], {"src": s2}).wait_recv()
        rcopy(dn4.at[s2], dnp.at[s2], w1s.at[1, d], w1r.at[1, s2], {"src": s2}).wait_recv()

    def assemble(h):
        one, two = dnp[2 * h], dnp[2 * h + 1]
        dnb[0, h] = jnp.concatenate(
            [one[:, :160], two[:, :160], one[:, 160:192], two[:, 160:192]], axis=1
        )

    def ring(h, step, way):
        a = step - 1 if way == 0 else (9 - step) % 8
        b = step if way == 0 else 8 - step
        to = ZP if way == 0 else ZM
        if step == 4:
            n, off, d_at = (40, 0, slice(0, 32)) if way == 0 else (40, 40, slice(32, 56))
        else:
            n, off, d_at = 80, 0, slice(0, 56)
        at = pl.ds(mo(h * 80 + off, 8), n)
        one = rcopy(gub.at[a, at, :], gub.at[b, at, :], zs.at[h, way, step - 1, 0], zr.at[h, way, step - 1, 0], to)
        two = rcopy(
            dnb.at[a, h, d_at, :], dnb.at[b, h, d_at, :], zs.at[h, way, step - 1, 1], zr.at[h, way, step - 1, 1], to
        )
        return one, two

    def ring_start(h, step):
        for way in (0, 1):
            for c in ring(h, step, way):
                c.start()

    def ring_wait(h, step):
        for way in (0, 1):
            for c in ring(h, step, way):
                c.wait_recv()

    def to_sib(slot):
        return rcopy(dnb.at[slot], dns.at[slot], ns.at[slot], nr.at[slot], SIB)

    def hop(stream, step):
        h = xh if stream == 0 else 1 - xh
        ring_wait(h, step)
        if step < 4:
            ring_start(h, step + 1)
        if stream == 1:
            to_sib(step).start()
            if step < 4:
                to_sib(8 - step).start()

    def unpack_down(ref, slot, which):
        zz = (z + ZS - slot) % ZS
        w = jnp.concatenate([ref[slot, 0, :, :320], ref[slot, 1, :, :320]], axis=1)
        for k in range(4):
            wd[which, k * 64 : k * 64 + 56, pl.ds(mo(zz * 640, 128), 640)] = byte_of(w, k)

    lane40 = lax.broadcasted_iota(jnp.int32, (40, 128), 1)

    def unpack(slot):
        zz = (z + ZS - slot) % ZS

        def rows(i, _):
            w = gub[slot, pl.ds(mo(i * 32, 32), 32), :]
            for k in range(4):
                wg[pl.ds(mo(k * 1280 + zz * 160 + i * 32, 32), 32), 0:384] = byte_of(w, k)
            return 0

        lax.fori_loop(0, 5, rows, 0)
        tails = []
        for s in range(4):
            t = dnb[slot, s // 2, 0:40, 256:384]
            t = pltpu.roll(t, 64 - 32 * (s % 2), 1)
            tails.append(jnp.where(lane40 < 16, t, 0))
        tails = jnp.concatenate(tails, axis=0)
        for k in range(4):
            wg[pl.ds(mo(k * 1280 + zz * 160, 32), 160), 384:512] = byte_of(tails, k)
        unpack_down(dnb, slot, 0)

    def unpack_sib(slot):
        to_sib(slot).wait_recv()
        unpack_down(dns, slot, 1)

    rcopy(
        gu4.at[0], gub.at[0, pl.ds(mo((src + 1 - 2 * core) * 40, 8), 40), :], w1s.at[0, 1],
        w1r.at[0, src + 1 - 2 * core], SIB,
    ).wait_recv()
    rcopy(dn4.at[0], dnp.at[src + 1 - 2 * core], w1s.at[1, 1], w1r.at[1, src + 1 - 2 * core], SIB).wait_recv()
    assemble(xh)
    ring_start(xh, 1)
    wd[...] = jnp.zeros(wd.shape, BF)

    def unpack_wo(ref, base):
        def cols(i, _):
            at = pl.ds(mo(i * 640, 128), 640)
            for hl in range(2):
                w = ref[hl * 32 : hl * 32 + 32, at]
                for k in range(4):
                    wo[pl.ds(mo(base + hl * 128 + k * 32, 32), 32), at] = byte_of(w, k)
            return 0

        lax.fori_loop(0, 4, cols, 0)

    load_wo.wait()
    unpack_wo(woh, xl * 256)
    far = (1 - xh) * 2
    for s2 in (far, far + 1):
        rcopy(gu4.at[0], gub.at[0, pl.ds(mo(s2 * 40, 8), 40), :], w1s.at[0, 2], w1r.at[0, s2], {"src": s2}).wait_recv()
        rcopy(dn4.at[0], dnp.at[s2], w1s.at[1, 2], w1r.at[1, s2], {"src": s2}).wait_recv()
    assemble(1 - xh)
    ring_start(1 - xh, 1)
    to_sib(0).start()
    load_kc.wait()
    load_vc.wait()
    half = lax.broadcasted_iota(jnp.int32, (8, HEAD), 1)
    pair = jnp.bitwise_and(lax.broadcasted_iota(jnp.int32, (8, HEAD), 0), 3)
    length = jnp.full((8, HEAD), lens[0, 0], jnp.int32)
    for b in range(1, 4):
        length = jnp.where(pair == b, lens[0, b], length)
    freq = jnp.exp(jnp.bitwise_and(half, 63).astype(F32) * (-math.log(ROPE) / 64))
    angle = length.astype(F32) * freq
    ctab = jnp.cos(angle)
    stab = jnp.sin(angle)
    stab = jnp.where(half < 64, -stab, stab)

    p128[...] = one_hot(128, 32, 32)
    p256[...] = one_hot(PAD, HID // 4, 64)
    t = lax.broadcasted_iota(jnp.int32, (ROWS, 256), 0)
    c = lax.broadcasted_iota(jnp.int32, (ROWS, 256), 1)
    for hl in range(4):
        want = jnp.right_shift(t, 2) * 16 + hl * 4 + jnp.bitwise_and(t, 3)
        picks[hl] = jnp.where(c == want, 1.0, 0.0).astype(BF)
    lax.fori_loop(1, 16, wait_b, 0)
    lane = lax.broadcasted_iota(jnp.int32, (4, HEAD), 1)
    for p in range(8):
        even, odd = brecv[2 * p], brecv[2 * p + 1]
        pieces = (
            even[:, 0:128],
            even[:, 128:256],
            jnp.where(lane < 64, even[:, 256:384], odd[:, 0:128]),
            odd[:, 128:256],
            odd[:, 256:384],
        )
        for j, piece in enumerate(pieces):
            h = 5 * p + j
            if h < HEADS:
                qs[4 * h : 4 * h + 4, :] = piece
            elif h < HEADS + KV:
                at = 128 + 8 * (h - HEADS)
                qs[at : at + 4, :] = piece
                qs[at + 4 : at + 8, :] = piece
            else:
                at = 8 * (h - HEADS - KV)
                vs[at : at + 4, :] = piece
                vs[at + 4 : at + 8, :] = piece
    v = qs[...]
    v = v * lax.rsqrt(jnp.mean(v * v, axis=1, keepdims=True) + EPS)
    row = lax.broadcasted_iota(jnp.int32, (160, HEAD), 0)
    v = v * jnp.where(row < 128, qgain[...][None, :], kgain[...][None, :])
    turned = pltpu.roll(v, 64, 1)
    v = v.reshape(20, 8, HEAD) * ctab[None] + turned.reshape(20, 8, HEAD) * stab[None]
    v = v.reshape(160, HEAD).astype(BF)
    scale = 1.0 / math.sqrt(HEAD)
    seq = jnp.bitwise_and(lax.broadcasted_iota(jnp.int32, (32, HEAD), 0), 3)
    live = jnp.where(half < length, 1.0, 0.0)
    live = jnp.broadcast_to(live[None], (4, 8, HEAD)).reshape(32, HEAD) > 0.5
    heads = []
    for g in range(KV):
        q = v[32 * g : 32 * g + 32]
        newk = v[128 + 8 * g : 136 + 8 * g].astype(F32)
        own = jnp.sum((q.astype(F32).reshape(4, 8, HEAD) * newk[None]).reshape(32, HEAD), axis=1, keepdims=True)
        own = own * scale
        s = jnp.zeros((32, HEAD), F32)
        for b in range(4):
            sb = lax.dot_general(
                q, kc[b, :, g * 128 : (g + 1) * 128], (((1,), (1,)), ((), ())), preferred_element_type=F32
            )
            s = jnp.where(seq == b, sb, s)
        s = jnp.where(live, s * scale, -jnp.inf)
        top = jnp.maximum(jnp.max(s, axis=1, keepdims=True), own)
        e = jnp.exp(s - top)
        own_e = jnp.exp(own - top)
        den = jnp.sum(e, axis=1, keepdims=True) + own_e
        newv = vs[8 * g : 8 * g + 8, :]
        low = own_e.astype(BF).astype(F32)
        num = (low.reshape(4, 8, 1) * newv[None]).reshape(32, HEAD)
        for b in range(4):
            eb = jnp.where(seq == b, e, 0.0).astype(BF)
            num = num + dot(eb, vc[b, :, g * 128 : (g + 1) * 128])
        heads.append(num / den)
    for yy in range(YS):
        g, at = yy // 4, 8 * (yy % 4)
        hsend[yy] = jnp.concatenate([heads[g][at : at + 8], heads[g + 2][at : at + 8]], axis=0).astype(BF)

    def h_slot(t):
        return hrecv.at[pl.ds(mo(t * 16, 16), 16), :]

    def h_copy(d):
        to = (tp + d) % 16
        return rcopy(hsend.at[to % YS], h_slot(tp), hs.at[to], hr.at[tp], {"tp": to})

    def start_h(d, _):
        h_copy(d).start()
        return 0

    def wait_h(d, _):
        frm = (tp + d) % 16
        rcopy(hsend.at[frm % YS], h_slot(frm), hs.at[frm], hr.at[frm], {"tp": frm}).wait_recv()
        return 0

    lax.fori_loop(1, 16, start_h, 0)
    hrecv[pl.ds(mo(tp * 16, 16), 16), :] = hsend[y]

    hop(0, 1)
    wo_copy.wait_recv()
    wo_share.start()
    unpack(0)
    wo_share.wait_recv()
    unpack_wo(wo_r, (1 - xl) * 256)

    lax.fori_loop(1, 16, wait_h, 0)
    got = hrecv[...]
    zcat = [dot(dot(picks[hl], got).astype(BF), p128[...]).astype(BF) for hl in range(4)]
    zcat = jnp.concatenate(zcat, axis=1)

    def part(yy, s):
        return pl.ds(mo(32 * (yy // 4) + 16 * s, 16), 16), pl.ds(mo(640 * (yy % 4), 128), 640)

    for cb in range(4):
        pm[:, cb * 640 : cb * 640 + 640] = dot(zcat, wo[:, cb * 640 : cb * 640 + 640]).astype(BF)

    def r_copy(d, s):
        to = (y + d) % YS
        a, b = part(to, s)
        return rcopy(pm.at[a, b], rs.at[s, y], rss.at[s, to], rsr.at[s, y], {"tp": xl * YS + to})

    def wait_r(d, s):
        frm = (y + d) % YS
        a, b = part(frm, s)
        rcopy(pm.at[a, b], rs.at[s, frm], rss.at[s, frm], rsr.at[s, frm], {"tp": xl * YS + frm}).wait_recv()

    for s in (0, 1):
        for d in NEAR[:0:-1]:
            r_copy(d, s).start()
        a, b = part(y, s)
        rs[s, y] = pm[a, b]
    unpack_sib(0)
    hop(1, 1)

    def blk(xx, cc, yy, s):
        r0 = ((xx // 2) * 2 + cc) * 64 + 32 * (yy // 4) + 16 * s
        c0 = (xx % 2) * HALF + 640 * (yy % 4)
        return X.at[pl.ds(mo(r0, 16), 16), pl.ds(mo(c0, 128), 640)]

    def fy_copy(d, s):
        to = (y + d) % YS
        b0 = blk(x, core, y, s)
        return rcopy(b0, b0, fys.at[s, to], fyr.at[s, y], {"tp": xl * YS + to})

    def fx_copy(way, i, s):
        b0 = blk(x, core, (y + i) % YS, s)
        return rcopy(b0, b0, fxs.at[s, way, i], fxr.at[s, way, i], PLUS if way == 0 else MINUS)

    def fx_in(way, i, s):
        b0 = blk(xm if way == 0 else xp, core, (y + i) % YS, s)
        return rcopy(b0, b0, fxs.at[s, way, i], fxr.at[s, way, i], MINUS if way == 0 else PLUS)

    def fq_copy(i, s):
        way = i % 2
        b0 = blk(xm if way == 0 else xp, core, (y + i) % YS, s)
        return rcopy(b0, b0, fqs.at[s, i], fqr.at[s, i], PLUS if way == 0 else MINUS)

    def fq_in(i, s):
        b0 = blk(xo, core, (y + i) % YS, s)
        return rcopy(b0, b0, fqs.at[s, i], fqr.at[s, i], MINUS if i % 2 == 0 else PLUS)

    froms = (x, xm, xp, xo)

    def fs_copy(j, i, s):
        b0 = blk(froms[j], core, (y + i) % YS, s)
        return rcopy(b0, b0, fss.at[s, j, i], fsr.at[s, j, i], SIB)

    def fs_in(j, i, s):
        b0 = blk(froms[j], 1 - core, (y + i) % YS, s)
        return rcopy(b0, b0, fss.at[s, j, i], fsr.at[s, j, i], SIB)

    def gained(*slabs):
        side = slabs[0][0] % 2
        rows = [pl.ds(mo(((xx // 2) * 2 + cc) * 64, 64), 64) for xx, cc in slabs]
        total = jnp.zeros((64 * len(rows), 1), F32)
        for g in range(5):
            cs = pl.ds(mo(side * HALF + g * 512, 128), 512)
            v = jnp.concatenate([X[at, cs] for at in rows], axis=0).astype(F32)
            total = total + jnp.sum(v * v, axis=1, keepdims=True)
            v = dot((v * vec[1:2, cs]).astype(BF), p512[...]).astype(BF)
            for k in range(4):
                to = pl.ds(mo(k * 1280 + side * 640 + g * 128, 128), 128)
                for n, at in enumerate(rows):
                    xk[at, to] = v[n * 64 : n * 64 + 64, k * 128 : (k + 1) * 128]
        for n, at in enumerate(rows):
            ssq[side, at, :] = jnp.broadcast_to(total[n * 64 : n * 64 + 64], (64, HEAD))

    def onward(i, s):
        fx_copy(0, i, s).start()
        fx_copy(1, i, s).start()
        fs_copy(0, i, s).start()

    def mid(s):
        for d in NEAR[1:]:
            wait_r(d, s)
        m = rs[s, 0].astype(F32)
        for i in range(1, YS):
            m = m + rs[s, i].astype(F32)
        cols = pl.ds(mo(xl * HALF + 640 * (y % 4), 128), 640)
        m = hid[pl.ds(mo(32 * (y // 4) + 16 * s, 16), 16), cols].astype(F32) + m * vec[2:3, cols]
        X[pl.ds(mo(src * 64 + 32 * (y // 4) + 16 * s, 16), 16), cols] = m.astype(BF)
        for d in NEAR[1:]:
            fy_copy(d, s).start()
        onward(0, s)

    def from_y(i, s):
        yy = (y + i) % YS
        b0 = blk(x, core, yy, s)
        rcopy(b0, b0, fys.at[s, yy], fyr.at[s, yy], {"tp": xl * YS + yy}).wait_recv()
        onward(i, s)

    def from_x(i, s):
        fx_in(0, i, s).wait_recv()
        fx_in(1, i, s).wait_recv()
        fq_copy(i, s).start()
        fs_copy(1, i, s).start()
        fs_copy(2, i, s).start()

    def from_sib(j):
        for s in (0, 1):
            for i in NEAR:
                fs_in(j, i, s).wait_recv()

    mid(0)
    hop(0, 2)
    unpack(1)
    mid(1)
    hop(1, 2)

    def from_q(i, s):
        fq_in(i, s).wait_recv()
        fs_copy(3, i, s).start()

    idle = {1: (unpack, 7), 2: (unpack, 2), 3: (unpack, 6), 4: (unpack_sib, 1), 5: (unpack_sib, 7)}
    for n in range(1, 8):
        from_y(NEAR[n], 0)
        if n in idle:
            idle[n][0](idle[n][1])
    from_x(0, 0)
    hop(0, 3)
    for i in NEAR[1:]:
        from_y(i, 1)
        from_x(i, 0)
    hop(1, 3)
    for n in range(8):
        from_x(NEAR[n], 1)
        if n == 1:
            unpack_sib(2)
            unpack_sib(6)
        if n == 3:
            unpack(3)
        if n == 5:
            unpack(5)
    for i in NEAR:
        from_q(i, 0)
    gained((xm, core), (xp, core))
    for n in range(8):
        from_q(NEAR[n], 1)
        if n == 1:
            from_sib(0)
            gained((x, core), (x, 1 - core))
        if n == 4:
            unpack_sib(3)
            unpack_sib(5)
    from_sib(1)
    from_sib(2)
    gained((xm, 1 - core), (xp, 1 - core))
    hop(0, 4)
    hop(1, 4)
    unpack(4)
    from_sib(3)
    gained((xo, core), (xo, 1 - core))
    gsc[...] = jnp.zeros((8, 1024), F32)
    gsc[0:1, :800] = gscale[...][None, :]
    gsc[1:2, :800] = uscale[...][None, :]
    shifted = gsc[...]
    mine = shifted
    for s in range(1, 4):
        mine = jnp.where(src == s, pltpu.roll(shifted, 1024 - HID * s, 1), mine)
    both = dot(xk[...], wg[...])
    rms = lax.rsqrt((ssq[0, :, 0:1] + ssq[1, :, 0:1]) * (1.0 / D) + EPS)
    gate = both[:, :PAD] * rms * mine[0:1, :PAD]
    up = pltpu.roll(both, 512 - HID, 1)[:, :PAD] * rms * mine[1:2, :PAD]
    used = lax.broadcasted_iota(jnp.int32, (1, PAD), 1) < HID
    act = jnp.where(used, gate / (1.0 + jnp.exp(-gate)) * up, 0.0).astype(BF)
    act = dot(act, p256[...]).astype(BF)
    xk[:, :PAD] = act

    def act_rows(h, cc):
        return pl.ds(mo((h * 2 + cc) * 64, 64), 64)

    def ac_copy(h):
        return rcopy(xk.at[act_rows(h, 1 - core), 0:PAD], actr.at[h], acs.at[h], acr.at[h], SIB)

    for h in (0, 1):
        ac_copy(h).start()
    unpack_sib(4)
    own_act = jnp.concatenate([xk[act_rows(0, core), 0:PAD], xk[act_rows(1, core), 0:PAD]], axis=0)

    def first(n, _):
        half_down[:, pl.ds(mo(n * 640, 128), 640)] = dot(own_act, wd[0, :, pl.ds(mo(xl * HALF + n * 640, 128), 640)])
        return 0

    lax.fori_loop(0, 4, first, 0)
    for h in (0, 1):
        ac_copy(h).wait_recv()
    sib_act = jnp.concatenate([actr[0], actr[1]], axis=0)

    def second(n, _):
        at = pl.ds(mo(xl * HALF + n * 640, 128), 640)
        pd[:, at] = (half_down[:, pl.ds(mo(n * 640, 128), 640)] + dot(sib_act, wd[1, :, at])).astype(BF)
        return 0

    def other(n, _):
        at = pl.ds(mo((1 - xl) * HALF + n * 640, 128), 640)
        pd[:, at] = (dot(own_act, wd[0, :, at]) + dot(sib_act, wd[1, :, at])).astype(BF)
        return 0

    sides = (PLUS, MINUS)
    nexts = (xp, xm)

    def slab(xx, q, w):
        rows = pl.ds(mo((xx // 2) * 64 + q * 16, 16), 16)
        return rows, pl.ds(mo((xx % 2) * HALF + w * 1280, 128), 1280)

    def pre_copy(q, w):
        a, b = slab(xo, q, w)
        return rcopy(pd.at[a, b], pre.at[q, w], xps.at[q, w], xpr.at[q, w], sides[w])

    def plain_copy(q, w):
        a, b = slab(nexts[w], q, 1 - w)
        return rcopy(pd.at[a, b], rplain.at[q, w], xas.at[q, w], xar.at[q, w], sides[w])

    def merge_copy(q, w):
        return rcopy(smerge.at[q, w], rmerge.at[q, w], xms.at[q, w], xmr.at[q, w], sides[w])

    def pre_start(q):
        for w in (0, 1):
            pre_copy(q, w).start()

    def plain_start(q):
        for w in (0, 1):
            plain_copy(q, w).start()

    def merge(q):
        for w in (0, 1):
            pre_copy(q, w).wait_recv()
            a, b = slab(nexts[w], q, w)
            smerge[q, w] = (pd[a, b].astype(F32) + pre[q, w].astype(F32)).astype(BF)
            merge_copy(q, w).start()

    def window(yy):
        return pl.ds(mo(320 * yy - 64 * (yy % 2), 128), 384)

    def y_copy(d, q):
        to = (y + d) % YS
        at = pl.ds(q * 16, 16)
        return rcopy(u.at[at, window(to)], yr.at[y, at, :], yss.at[q, to], ysr.at[q, y], {"tp": xl * YS + to})

    def y_in(d, q):
        frm = (y + d) % YS
        at = pl.ds(q * 16, 16)
        return rcopy(u.at[at, window(frm)], yr.at[frm, at, :], yss.at[q, frm], ysr.at[q, frm], {"tp": xl * YS + frm})

    def finish(q):
        at = slice(q * 16, q * 16 + 16)
        for w in (0, 1):
            plain_copy(q, w).wait_recv()
        for w in (0, 1):
            merge_copy(q, w).wait_recv()
            a, b = slab(x, q, w)
            v = pd[a, b].astype(F32) + rplain[q, 1 - w].astype(F32) + rmerge[q, w].astype(F32)
            u[at, w * 1280 : w * 1280 + 1280] = v.astype(BF)
        for d in NEAR[:0:-1]:
            y_copy(d, q).start()
        yr[y, at, :] = u[at, window(y)]

    lax.fori_loop(0, 4, second, 0)
    pre_start(0)
    pre_start(1)
    lax.fori_loop(0, 4, other, 0)
    plain_start(0)
    merge(0)
    pre_start(2)
    plain_start(1)
    merge(1)
    pre_start(3)
    plain_start(2)
    finish(0)
    merge(2)
    plain_start(3)
    finish(1)
    merge(3)
    finish(2)
    finish(3)
    for d in (1, 2, 3):
        w1_gu(d).wait_send()
        w1_dn(d).wait_send()
    wo_copy.wait_send()
    wo_share.wait_send()
    for h in (0, 1):
        for step in (1, 2, 3, 4):
            for way in (0, 1):
                for c in ring(h, step, way):
                    c.wait_send()
    for slot in range(ZS):
        to_sib(slot).wait_send()

    def sent_tp(d, _):
        b_copy(d).wait_send()
        h_copy(d).wait_send()
        return 0

    lax.fori_loop(1, 16, sent_tp, 0)
    for d in NEAR[1:]:
        for s in (0, 1):
            r_copy(d, s).wait_send()
    for s in (0, 1):
        for d in NEAR[1:]:
            fy_copy(d, s).wait_send()
        for i in range(YS):
            fx_copy(0, i, s).wait_send()
            fx_copy(1, i, s).wait_send()
            fq_copy(i, s).wait_send()
            for j in range(4):
                fs_copy(j, i, s).wait_send()
    for w in (0, 1):
        ac_copy(w).wait_send()
        for q in range(4):
            pre_copy(q, w).wait_send()
            plain_copy(q, w).wait_send()
            merge_copy(q, w).wait_send()
    for q in range(4):
        for d in NEAR[1:]:
            y_in(d, q).wait_recv()
    last = yr[0].astype(F32)
    for i in range(1, YS):
        last = last + yr[i].astype(F32)
    at = pl.ds(mo(xl * HALF + 320 * y - 64 * (y % 2), 128), 384)
    last = X[pl.ds(mo(src * 64, 64), 64), at].astype(F32) + last * vec[3:4, at]
    last = jnp.where(odd_y, pltpu.roll(last, 320, 1), last)
    out[...] = last[:, :320].astype(BF)

    for q in range(4):
        for d in NEAR[1:]:
            y_copy(d, q).wait_send()


def local(
    hidden_in, attn_gain, w_qkv, qkv_scale, q_gain, k_gain, key_cache, value_cache, lengths, w_out, out_scale,
    mlp_gain, w_gate, w_up, gate_scale, up_scale, w_down, down_scale,
):
    V, S = pltpu.VMEM, pltpu.SemaphoreType.DMA
    I32 = jnp.int32
    scratch = [
        V((ROWS, D), BF), V((D,), F32), V((320,), F32), V((HEAD,), F32), V((HEAD,), F32), V((D,), F32), V((D,), F32),
        V((40, 800), I32), V((40, 800), I32), V((800,), F32), V((800,), F32), V((160, HID), I32), V((D,), F32),
        V((320, 1280), I32), V((4, 128, 512), BF), V((4, 128, 512), BF), V((64, HALF), I32), V((512, 512), BF),
        V((HEAD, HEAD), BF), V((PAD, PAD), BF), V((4, ROWS, 256), BF), V((2 * ROWS, HALF), F32),
        V((8, D), F32), V((8, 1024), F32),
        V((ROWS, 384), F32), V((4, 40, 384), I32), V((4, 56, 256), I32),
        V((16, 4, 384), F32), V((16, 4, 384), F32), V((160, HEAD), F32), V((32, HEAD), F32),
        V((YS, 16, HEAD), BF), V((256, HEAD), BF), V((64, HALF), I32), V((512, HALF), BF), V((ROWS, HALF), BF),
        V((2, YS, 16, 640), BF), V((ALL, D), BF), V((ALL, D), BF), V((2, ALL, HEAD), F32),
        V((ZS, 160, 384), I32), V((4, 56, 256), I32), V((ZS, 2, 56, 384), I32), V((ZS, 2, 56, 384), I32),
        V((D, 512), BF), V((2, 256, D), BF), V((2, ROWS, PAD), BF), V((2 * ROWS, D), BF),
        V((4, 2, 16, 1280), BF), V((4, 2, 16, 1280), BF), V((4, 2, 16, 1280), BF), V((4, 2, 16, 1280), BF),
        V((ROWS, HALF), BF), V((YS, ROWS, 384), BF),
        S((18,)), S((2, 4)), S((2, 4)), S((2,)), S((2,)), S((2, 2, 4, 2)), S((2, 2, 4, 2)), S((8,)), S((8,)),
        S((16,)), S((16,)), S((16,)), S((16,)),
        S((2, 8)), S((2, 8)), S((2, 8)), S((2, 8)), S((2, 2, 8)), S((2, 2, 8)), S((2, 8)), S((2, 8)), S((2, 4, 8)), S((2, 4, 8)),
        S((2,)), S((2,)), S((4, 2)), S((4, 2)), S((4, 2)), S((4, 2)), S((4, 2)), S((4, 2)), S((4, 8)), S((4, 8)),
    ]
    vmem = pl.BlockSpec(memory_space=pltpu.VMEM)
    far = pl.BlockSpec(memory_space=pl.ANY)
    specs = [far] * 18
    specs[8] = pl.BlockSpec(memory_space=pltpu.SMEM)
    return pl.pallas_call(
        kernel,
        out_shape=jax.ShapeDtypeStruct((ROWS, 320), BF),
        in_specs=specs,
        out_specs=vmem,
        scratch_shapes=scratch,
        compiler_params=pltpu.CompilerParams(
            collective_id=0, has_side_effects=True, vmem_limit_bytes=60 * 1024 * 1024
        ),
        name="layer",
    )(
        hidden_in, attn_gain, w_qkv.T, qkv_scale, q_gain, k_gain, key_cache, value_cache, lengths, w_out, out_scale,
        mlp_gain, w_gate, w_up, gate_scale, up_scale, w_down.T, down_scale,
    )


def solution(mesh):
    return jax.shard_map(
        local,
        mesh=mesh,
        in_specs=(
            P(("grp", "src"), None),
            P(),
            P(None, "tp"),
            P("tp"),
            P(),
            P(),
            P(("grp", "src"), "tp", None, None),
            P(("grp", "src"), "tp", None, None),
            P(("grp", "src"), "tp"),
            P("tp", None),
            P(),
            P(),
            P(("grp", "src"), "tp"),
            P(("grp", "src"), "tp"),
            P("tp"),
            P("tp"),
            P("tp", ("grp", "src")),
            P(),
        ),
        out_specs=P(("grp", "src"), "tp"),
        check_vma=False,
    )
```

```python
import math

import jax
import jax.numpy as jnp
from jax import lax
from jax.experimental import pallas as pl
from jax.experimental.pallas import tpu as pltpu
from jax.sharding import PartitionSpec as P

D = 5120
HALF = 2560
HEADS = 32
KV = 4
HEAD = 128
ROWS = 64
ALL = 256
YS = 8
ZS = 8
HID = 200
PAD = 256
EPS = 1e-06
ROPE = 1000000.0
MESH = pl.DeviceIdType.MESH
F32 = jnp.float32
BF = jnp.bfloat16
NEAR = (0, 1, 7, 2, 6, 3, 5, 4)


def mo(value, k):
    return pl.multiple_of(value, k)


def byte_of(words, k):
    return jnp.right_shift(jnp.left_shift(words, 24 - 8 * k), 24).astype(F32).astype(BF)


def one_hot(n, used, stride):
    row = lax.broadcasted_iota(jnp.int32, (n, n), 0)
    col = lax.broadcasted_iota(jnp.int32, (n, n), 1)
    shift = stride.bit_length() - 1
    k, r = jnp.right_shift(col, shift), jnp.bitwise_and(col, stride - 1)
    return jnp.where((row == 4 * r + k) & (r < used), 1.0, 0.0).astype(BF)


def dot(a, b):
    return jnp.dot(a, b, preferred_element_type=F32)


def kernel(
    hid_hbm, again_hbm, wq_hbm, qscale_hbm, qgain_hbm, kgain_hbm, kc_hbm, vc_hbm, lens, wout, oscale_hbm, mgain_hbm,
    wgate_hbm, wup_hbm, gscale_hbm, uscale_hbm, wdown_hbm, dscale_hbm,
    out,
    hid, again, qscale, qgain, kgain, oscale, mgain, wgate, wup, gscale, uscale, wdown, dscale,
    wq, kc, vc, woh, p512, p128, p256, picks, half_down, vec, gsc, stage, gu4, dn4, bsend, brecv, qs, vs, hsend, hrecv, wo_r, wo, pm, rs, X, xk, ssq,
    gub, dnp, dnb, dns, wg, wd, actr, pd, pre, smerge, rplain, rmerge, u, yr,
    ld, w1s, w1r, wos, wor, zs, zr, ns, nr, bs, br, hs, hr, rss, rsr, fys, fyr, fxs, fxr, fqs, fqr, fss, fsr,
    acs, acr, xps, xpr, xas, xar, xms, xmr, yss, ysr,
):
    z = lax.axis_index("grp")
    tp = lax.axis_index("tp")
    src = lax.axis_index("src")
    xl, y = tp // YS, tp % YS
    xh, core = src // 2, src % 2
    x = xh * 2 + xl

    def at_x(xx, cc):
        return {"tp": (xx % 2) * YS + y, "src": (xx // 2) * 2 + cc}

    xp, xm, xo = (x + 1) % 4, (x + 3) % 4, (x + 2) % 4
    PLUS, MINUS = at_x(xp, core), at_x(xm, core)
    SIB = {"src": xh * 2 + 1 - core}
    ZP, ZM = {"grp": (z + 1) % ZS}, {"grp": (z + ZS - 1) % ZS}

    def rcopy(a, b, s, r, to):
        return pltpu.make_async_remote_copy(
            src_ref=a, dst_ref=b, send_sem=s, recv_sem=r, device_id=to, device_id_type=MESH
        )

    load_wq = [
        pltpu.make_async_copy(wq_hbm.at[:, pl.ds(i * 640, 640)], wq.at[:, pl.ds(i * 640, 640)], ld.at[i]) for i in (0, 1)
    ]
    load_kc = pltpu.make_async_copy(kc_hbm.at[0], kc, ld.at[2])
    load_vc = pltpu.make_async_copy(vc_hbm.at[0], vc, ld.at[3])
    load_wo = pltpu.make_async_copy(wout.at[:, pl.ds(mo(xl * HALF, 128), HALF)], woh, ld.at[4])
    pairs = (
        (hid_hbm, hid), (again_hbm, again), (wgate_hbm, wgate), (wup_hbm, wup), (wdown_hbm, wdown), (mgain_hbm, mgain),
        (oscale_hbm, oscale), (dscale_hbm, dscale), (qscale_hbm, qscale), (qgain_hbm, qgain), (kgain_hbm, kgain),
        (gscale_hbm, gscale), (uscale_hbm, uscale),
    )
    loads = [pltpu.make_async_copy(a, b, ld.at[5 + i]) for i, (a, b) in enumerate(pairs)]
    for c in loads[2:5] + loads[:2] + loads[5:] + load_wq:
        c.start()
    load_kc.start()
    load_vc.start()
    load_wo.start()

    barrier = pltpu.get_barrier_semaphore()

    def greet_tp(d, _):
        pl.semaphore_signal(barrier, inc=1, device_id={"tp": (tp + d) % 16}, device_id_type=MESH)
        return 0

    def greet_src(d, _):
        pl.semaphore_signal(barrier, inc=1, device_id={"src": (src + d) % 4}, device_id_type=MESH)
        return 0

    lax.fori_loop(1, 16, greet_tp, 0)
    lax.fori_loop(1, 4, greet_src, 0)
    across = {"tp": (1 - xl) * YS + y, "src": (1 - xh) * 2 + core}
    for to in (across, ZP, ZM):
        pl.semaphore_signal(barrier, inc=1, device_id=to, device_id_type=MESH)

    p512[...] = one_hot(512, 128, 128)
    for c in loads:
        c.wait()
    turned = jnp.transpose(wdown[...])
    for s in range(4):
        piece = jnp.concatenate([wgate[:, HID * s : HID * s + HID], wup[:, HID * s : HID * s + HID]], axis=1)
        gu4[s] = piece[:, :384]
        dn4[s] = jnp.zeros((56, 256), jnp.int32)
        dn4[s, 0:50, 0:160] = turned[50 * s : 50 * s + 50, :]
        dn4[s, 0:40, 160:176] = piece[:, 384:400]
    gub[0, pl.ds(mo(src * 40, 8), 40), :] = gu4[src]
    dnp[src] = dn4[src]
    vec[0:1, :] = again[...][None, :]
    vec[1:2, :] = mgain[...][None, :]
    vec[2:3, :] = oscale[...][None, :]
    vec[3:4, :] = dscale[...][None, :]

    total = jnp.zeros((ROWS, 1), F32)
    for g in range(10):
        v = hid[:, g * 512 : (g + 1) * 512].astype(F32)
        total = total + jnp.sum(v * v, axis=1, keepdims=True)
    rms = lax.rsqrt(total * (1.0 / D) + EPS)

    for g in range(10):
        at = slice(g * 512, g * 512 + 512)
        v = (hid[:, at].astype(F32) * rms * vec[0:1, at]).astype(BF)
        xk[:ROWS, at] = dot(v, p512[...]).astype(BF)
    pl.semaphore_wait(barrier, 21)

    def w1_gu(d):
        s2 = (src + d) % 4
        return rcopy(
            gu4.at[s2], gub.at[0, pl.ds(mo(src * 40, 8), 40), :], w1s.at[0, d], w1r.at[0, src], {"src": s2}
        )

    def w1_dn(d):
        s2 = (src + d) % 4
        return rcopy(dn4.at[s2], dnp.at[src], w1s.at[1, d], w1r.at[1, src], {"src": s2})

    for d in (1, 2, 3):
        w1_gu(d).start()
        w1_dn(d).start()

    acc = jnp.zeros((ROWS, 320), F32)
    for c in load_wq:
        c.wait()
    for g in range(10):
        w = wq[:, g * 128 : g * 128 + 128]
        for k in (0, 2):
            acc = acc + lax.dot_general(
                xk[:ROWS, g * 512 + k * 128 : g * 512 + k * 128 + 256],
                jnp.concatenate([byte_of(w, k), byte_of(w, k + 1)], axis=1),
                (((1,), (1,)), ((), ())),
                preferred_element_type=F32,
            )
    qkv = (acc * qscale[...][None, :]).astype(BF).astype(F32)
    stage[...] = jnp.zeros((ROWS, 384), F32)
    stage[:, :320] = qkv
    odd_y = (y % 2) == 1
    placed = stage[...]
    placed = jnp.where(odd_y, pltpu.roll(placed, 64, 1), placed)
    for t in range(16):
        bsend[t] = placed[4 * t : 4 * t + 4, :]

    def b_copy(d):
        to = (tp + d) % 16
        return rcopy(bsend.at[to], brecv.at[tp], bs.at[to], br.at[tp], {"tp": to})

    def start_b(d, _):
        b_copy(d).start()
        return 0

    def wait_b(d, _):
        frm = (tp + d) % 16
        rcopy(bsend.at[frm], brecv.at[frm], bs.at[frm], br.at[frm], {"tp": frm}).wait_recv()
        return 0

    lax.fori_loop(1, 16, start_b, 0)
    wo_side = (x + 1 + 2 * core) % 4
    wo_rows = pl.ds(mo(core * 32, 32), 32)
    wo_copy = rcopy(
        wout.at[wo_rows, pl.ds(mo((1 - xl) * HALF, 128), HALF)], wo_r.at[wo_rows, :], wos.at[0], wor.at[0],
        at_x(wo_side, core),
    )
    wo_share = rcopy(wo_r.at[wo_rows, :], wo_r.at[wo_rows, :], wos.at[1], wor.at[1], SIB)
    wo_copy.start()
    brecv[pl.ds(tp, 1)] = bsend[pl.ds(tp, 1)]

    def w1_in(d):
        s2 = (src + d) % 4
        rcopy(gu4.at[s2], gub.at[0, pl.ds(mo(s2 * 40, 8), 40), :], w1s.at[0, d], w1r.at[0, s2], {"src": s2}).wait_recv()
        rcopy(dn4.at[s2], dnp.at[s2], w1s.at[1, d], w1r.at[1, s2], {"src": s2}).wait_recv()

    def assemble(h):
        one, two = dnp[2 * h], dnp[2 * h + 1]
        dnb[0, h] = jnp.concatenate(
            [one[:, :160], two[:, :160], one[:, 160:192], two[:, 160:192]], axis=1
        )

    def ring(h, step, way):
        a = step - 1 if way == 0 else (9 - step) % 8
        b = step if way == 0 else 8 - step
        to = ZP if way == 0 else ZM
        if step == 4:
            n, off, d_at = (40, 0, slice(0, 32)) if way == 0 else (40, 40, slice(32, 56))
        else:
            n, off, d_at = 80, 0, slice(0, 56)
        at = pl.ds(mo(h * 80 + off, 8), n)
        one = rcopy(gub.at[a, at, :], gub.at[b, at, :], zs.at[h, way, step - 1, 0], zr.at[h, way, step - 1, 0], to)
        two = rcopy(
            dnb.at[a, h, d_at, :], dnb.at[b, h, d_at, :], zs.at[h, way, step - 1, 1], zr.at[h, way, step - 1, 1], to
        )
        return one, two

    def ring_start(h, step):
        for way in (0, 1):
            for c in ring(h, step, way):
                c.start()

    def ring_wait(h, step):
        for way in (0, 1):
            for c in ring(h, step, way):
                c.wait_recv()

    def to_sib(slot):
        return rcopy(dnb.at[slot], dns.at[slot], ns.at[slot], nr.at[slot], SIB)

    def hop(stream, step):
        h = xh if stream == 0 else 1 - xh
        ring_wait(h, step)
        if step < 4:
            ring_start(h, step + 1)
        if stream == 1:
            to_sib(step).start()
            if step < 4:
                to_sib(8 - step).start()

    def unpack_down(ref, slot, which):
        zz = (z + ZS - slot) % ZS
        w = jnp.concatenate([ref[slot, 0, :, :320], ref[slot, 1, :, :320]], axis=1)
        for k in range(4):
            wd[which, k * 64 : k * 64 + 56, pl.ds(mo(zz * 640, 128), 640)] = byte_of(w, k)

    lane40 = lax.broadcasted_iota(jnp.int32, (40, 128), 1)

    def unpack(slot):
        zz = (z + ZS - slot) % ZS

        def rows(i, _):
            w = gub[slot, pl.ds(mo(i * 32, 32), 32), :]
            for k in range(4):
                wg[pl.ds(mo(k * 1280 + zz * 160 + i * 32, 32), 32), 0:384] = byte_of(w, k)
            return 0

        lax.fori_loop(0, 5, rows, 0)
        tails = []
        for s in range(4):
            t = dnb[slot, s // 2, 0:40, 256:384]
            t = pltpu.roll(t, 64 - 32 * (s % 2), 1)
            tails.append(jnp.where(lane40 < 16, t, 0))
        tails = jnp.concatenate(tails, axis=0)
        for k in range(4):
            wg[pl.ds(mo(k * 1280 + zz * 160, 32), 160), 384:512] = byte_of(tails, k)
        unpack_down(dnb, slot, 0)

    def unpack_sib(slot):
        to_sib(slot).wait_recv()
        unpack_down(dns, slot, 1)

    rcopy(
        gu4.at[0], gub.at[0, pl.ds(mo((src + 1 - 2 * core) * 40, 8), 40), :], w1s.at[0, 1],
        w1r.at[0, src + 1 - 2 * core], SIB,
    ).wait_recv()
    rcopy(dn4.at[0], dnp.at[src + 1 - 2 * core], w1s.at[1, 1], w1r.at[1, src + 1 - 2 * core], SIB).wait_recv()
    assemble(xh)
    ring_start(xh, 1)
    wd[...] = jnp.zeros(wd.shape, BF)

    def unpack_wo(ref, base):
        def cols(i, _):
            at = pl.ds(mo(i * 640, 128), 640)
            for hl in range(2):
                w = ref[hl * 32 : hl * 32 + 32, at]
                for k in range(4):
                    wo[pl.ds(mo(base + hl * 128 + k * 32, 32), 32), at] = byte_of(w, k)
            return 0

        lax.fori_loop(0, 4, cols, 0)

    load_wo.wait()
    unpack_wo(woh, xl * 256)
    far = (1 - xh) * 2
    for s2 in (far, far + 1):
        rcopy(gu4.at[0], gub.at[0, pl.ds(mo(s2 * 40, 8), 40), :], w1s.at[0, 2], w1r.at[0, s2], {"src": s2}).wait_recv()
        rcopy(dn4.at[0], dnp.at[s2], w1s.at[1, 2], w1r.at[1, s2], {"src": s2}).wait_recv()
    assemble(1 - xh)
    ring_start(1 - xh, 1)
    to_sib(0).start()
    load_kc.wait()
    load_vc.wait()
    half = lax.broadcasted_iota(jnp.int32, (8, HEAD), 1)
    pair = jnp.bitwise_and(lax.broadcasted_iota(jnp.int32, (8, HEAD), 0), 3)
    length = jnp.full((8, HEAD), lens[0, 0], jnp.int32)
    for b in range(1, 4):
        length = jnp.where(pair == b, lens[0, b], length)
    freq = jnp.exp(jnp.bitwise_and(half, 63).astype(F32) * (-math.log(ROPE) / 64))
    angle = length.astype(F32) * freq
    ctab = jnp.cos(angle)
    stab = jnp.sin(angle)
    stab = jnp.where(half < 64, -stab, stab)

    p128[...] = one_hot(128, 32, 32)
    p256[...] = one_hot(PAD, HID // 4, 64)
    t = lax.broadcasted_iota(jnp.int32, (ROWS, 256), 0)
    c = lax.broadcasted_iota(jnp.int32, (ROWS, 256), 1)
    for hl in range(4):
        want = jnp.right_shift(t, 2) * 16 + hl * 4 + jnp.bitwise_and(t, 3)
        picks[hl] = jnp.where(c == want, 1.0, 0.0).astype(BF)
    lax.fori_loop(1, 16, wait_b, 0)
    lane = lax.broadcasted_iota(jnp.int32, (4, HEAD), 1)
    for p in range(8):
        even, odd = brecv[2 * p], brecv[2 * p + 1]
        pieces = (
            even[:, 0:128],
            even[:, 128:256],
            jnp.where(lane < 64, even[:, 256:384], odd[:, 0:128]),
            odd[:, 128:256],
            odd[:, 256:384],
        )
        for j, piece in enumerate(pieces):
            h = 5 * p + j
            if h < HEADS:
                qs[4 * h : 4 * h + 4, :] = piece
            elif h < HEADS + KV:
                at = 128 + 8 * (h - HEADS)
                qs[at : at + 4, :] = piece
                qs[at + 4 : at + 8, :] = piece
            else:
                at = 8 * (h - HEADS - KV)
                vs[at : at + 4, :] = piece
                vs[at + 4 : at + 8, :] = piece
    v = qs[...]
    v = v * lax.rsqrt(jnp.mean(v * v, axis=1, keepdims=True) + EPS)
    row = lax.broadcasted_iota(jnp.int32, (160, HEAD), 0)
    v = v * jnp.where(row < 128, qgain[...][None, :], kgain[...][None, :])
    turned = pltpu.roll(v, 64, 1)
    v = v.reshape(20, 8, HEAD) * ctab[None] + turned.reshape(20, 8, HEAD) * stab[None]
    v = v.reshape(160, HEAD).astype(BF)
    scale = 1.0 / math.sqrt(HEAD)
    seq = jnp.bitwise_and(lax.broadcasted_iota(jnp.int32, (32, HEAD), 0), 3)
    live = jnp.where(half < length, 1.0, 0.0)
    live = jnp.broadcast_to(live[None], (4, 8, HEAD)).reshape(32, HEAD) > 0.5
    heads = []
    for g in range(KV):
        q = v[32 * g : 32 * g + 32]
        newk = v[128 + 8 * g : 136 + 8 * g].astype(F32)
        own = jnp.sum((q.astype(F32).reshape(4, 8, HEAD) * newk[None]).reshape(32, HEAD), axis=1, keepdims=True)
        own = own * scale
        s = jnp.zeros((32, HEAD), F32)
        for b in range(4):
            sb = lax.dot_general(
                q, kc[b, :, g * 128 : (g + 1) * 128], (((1,), (1,)), ((), ())), preferred_element_type=F32
            )
            s = jnp.where(seq == b, sb, s)
        s = jnp.where(live, s * scale, -jnp.inf)
        top = jnp.maximum(jnp.max(s, axis=1, keepdims=True), own)
        e = jnp.exp(s - top)
        own_e = jnp.exp(own - top)
        den = jnp.sum(e, axis=1, keepdims=True) + own_e
        newv = vs[8 * g : 8 * g + 8, :]
        low = own_e.astype(BF).astype(F32)
        num = (low.reshape(4, 8, 1) * newv[None]).reshape(32, HEAD)
        for b in range(4):
            eb = jnp.where(seq == b, e, 0.0).astype(BF)
            num = num + dot(eb, vc[b, :, g * 128 : (g + 1) * 128])
        heads.append(num / den)
    for yy in range(YS):
        g, at = yy // 4, 8 * (yy % 4)
        hsend[yy] = jnp.concatenate([heads[g][at : at + 8], heads[g + 2][at : at + 8]], axis=0).astype(BF)

    def h_slot(t):
        return hrecv.at[pl.ds(mo(t * 16, 16), 16), :]

    def h_copy(d):
        to = (tp + d) % 16
        return rcopy(hsend.at[to % YS], h_slot(tp), hs.at[to], hr.at[tp], {"tp": to})

    def start_h(d, _):
        h_copy(d).start()
        return 0

    def wait_h(d, _):
        frm = (tp + d) % 16
        rcopy(hsend.at[frm % YS], h_slot(frm), hs.at[frm], hr.at[frm], {"tp": frm}).wait_recv()
        return 0

    lax.fori_loop(1, 16, start_h, 0)
    hrecv[pl.ds(mo(tp * 16, 16), 16), :] = hsend[y]

    hop(0, 1)
    wo_copy.wait_recv()
    wo_share.start()
    unpack(0)
    wo_share.wait_recv()
    unpack_wo(wo_r, (1 - xl) * 256)

    hop(1, 1)
    lax.fori_loop(1, 16, wait_h, 0)
    got = hrecv[...]
    zcat = [dot(dot(picks[hl], got).astype(BF), p128[...]).astype(BF) for hl in range(4)]
    zcat = jnp.concatenate(zcat, axis=1)

    def part(yy, s):
        return pl.ds(mo(32 * (yy // 4) + 16 * s, 16), 16), pl.ds(mo(640 * (yy % 4), 128), 640)

    for cb in range(4):
        pm[:, cb * 640 : cb * 640 + 640] = dot(zcat, wo[:, cb * 640 : cb * 640 + 640]).astype(BF)

    def r_copy(d, s):
        to = (y + d) % YS
        a, b = part(to, s)
        return rcopy(pm.at[a, b], rs.at[s, y], rss.at[s, to], rsr.at[s, y], {"tp": xl * YS + to})

    def wait_r(d, s):
        frm = (y + d) % YS
        a, b = part(frm, s)
        rcopy(pm.at[a, b], rs.at[s, frm], rss.at[s, frm], rsr.at[s, frm], {"tp": xl * YS + frm}).wait_recv()

    for s in (0, 1):
        for d in NEAR[:0:-1]:
            r_copy(d, s).start()
        a, b = part(y, s)
        rs[s, y] = pm[a, b]
    unpack_sib(0)
    hop(0, 2)

    def blk(xx, cc, yy, s):
        r0 = ((xx // 2) * 2 + cc) * 64 + 32 * (yy // 4) + 16 * s
        c0 = (xx % 2) * HALF + 640 * (yy % 4)
        return X.at[pl.ds(mo(r0, 16), 16), pl.ds(mo(c0, 128), 640)]

    def fy_copy(d, s):
        to = (y + d) % YS
        b0 = blk(x, core, y, s)
        return rcopy(b0, b0, fys.at[s, to], fyr.at[s, y], {"tp": xl * YS + to})

    def fx_copy(way, i, s):
        b0 = blk(x, core, (y + i) % YS, s)
        return rcopy(b0, b0, fxs.at[s, way, i], fxr.at[s, way, i], PLUS if way == 0 else MINUS)

    def fx_in(way, i, s):
        b0 = blk(xm if way == 0 else xp, core, (y + i) % YS, s)
        return rcopy(b0, b0, fxs.at[s, way, i], fxr.at[s, way, i], MINUS if way == 0 else PLUS)

    def fq_copy(i, s):
        if s == 1 and i in (5, 4):
            b0 = blk(x, core, (y + i) % YS, s)
            return rcopy(b0, b0, fqs.at[s, i], fqr.at[s, i], at_x(xo, core))
        way = i % 2
        b0 = blk(xm if way == 0 else xp, core, (y + i) % YS, s)
        return rcopy(b0, b0, fqs.at[s, i], fqr.at[s, i], PLUS if way == 0 else MINUS)

    def fq_in(i, s):
        b0 = blk(xo, core, (y + i) % YS, s)
        return rcopy(b0, b0, fqs.at[s, i], fqr.at[s, i], MINUS if i % 2 == 0 else PLUS)

    froms = (x, xm, xp, xo)

    def fs_copy(j, i, s):
        b0 = blk(froms[j], core, (y + i) % YS, s)
        return rcopy(b0, b0, fss.at[s, j, i], fsr.at[s, j, i], SIB)

    def fs_in(j, i, s):
        b0 = blk(froms[j], 1 - core, (y + i) % YS, s)
        return rcopy(b0, b0, fss.at[s, j, i], fsr.at[s, j, i], SIB)

    def gained(*slabs):
        side = slabs[0][0] % 2
        rows = [pl.ds(mo(((xx // 2) * 2 + cc) * 64, 64), 64) for xx, cc in slabs]
        total = jnp.zeros((64 * len(rows), 1), F32)
        for g in range(5):
            cs = pl.ds(mo(side * HALF + g * 512, 128), 512)
            v = jnp.concatenate([X[at, cs] for at in rows], axis=0).astype(F32)
            total = total + jnp.sum(v * v, axis=1, keepdims=True)
            v = dot((v * vec[1:2, cs]).astype(BF), p512[...]).astype(BF)
            for k in range(4):
                to = pl.ds(mo(k * 1280 + side * 640 + g * 128, 128), 128)
                for n, at in enumerate(rows):
                    xk[at, to] = v[n * 64 : n * 64 + 64, k * 128 : (k + 1) * 128]
        for n, at in enumerate(rows):
            ssq[side, at, :] = jnp.broadcast_to(total[n * 64 : n * 64 + 64], (64, HEAD))

    def onward(i, s):
        fx_copy(0, i, s).start()
        fx_copy(1, i, s).start()
        if s == 1 and i in (5, 4):
            fq_copy(i, s).start()
        fs_copy(0, i, s).start()

    def mid(s):
        for d in NEAR[1:]:
            wait_r(d, s)
        m = rs[s, 0].astype(F32)
        for i in range(1, YS):
            m = m + rs[s, i].astype(F32)
        cols = pl.ds(mo(xl * HALF + 640 * (y % 4), 128), 640)
        m = hid[pl.ds(mo(32 * (y // 4) + 16 * s, 16), 16), cols].astype(F32) + m * vec[2:3, cols]
        X[pl.ds(mo(src * 64 + 32 * (y // 4) + 16 * s, 16), 16), cols] = m.astype(BF)
        for d in NEAR[1:]:
            fy_copy(d, s).start()
        onward(0, s)

    def from_y(i, s):
        yy = (y + i) % YS
        b0 = blk(x, core, yy, s)
        rcopy(b0, b0, fys.at[s, yy], fyr.at[s, yy], {"tp": xl * YS + yy}).wait_recv()
        onward(i, s)

    def from_x(i, s):
        fx_in(0, i, s).wait_recv()
        fx_in(1, i, s).wait_recv()
        if not (s == 1 and i in (5, 4)):
            fq_copy(i, s).start()
        fs_copy(1, i, s).start()
        fs_copy(2, i, s).start()

    def from_sib(j):
        for s in (0, 1):
            for i in NEAR:
                fs_in(j, i, s).wait_recv()

    mid(0)
    unpack(1)
    mid(1)
    hop(1, 2)

    def from_q(i, s):
        fq_in(i, s).wait_recv()
        fs_copy(3, i, s).start()

    idle = {1: (unpack, 7), 2: (unpack, 2), 3: (unpack, 6), 4: (unpack_sib, 1), 5: (unpack_sib, 7)}
    for n in range(1, 8):
        from_y(NEAR[n], 0)
        if n in idle:
            idle[n][0](idle[n][1])
    from_x(0, 0)
    for n in range(1, 8):
        from_y(NEAR[n], 1)
        from_x(NEAR[n], 0)
        if n == 3:
            hop(0, 3)
    hop(1, 3)
    for n in range(8):
        from_x(NEAR[n], 1)
        if n == 1:
            unpack_sib(2)
            unpack_sib(6)
        if n == 3:
            unpack(3)
        if n == 5:
            unpack(5)
    for i in NEAR:
        from_q(i, 0)
    gained((xm, core), (xp, core))
    for n in range(8):
        from_q(NEAR[n], 1)
        if n == 1:
            from_sib(0)
            gained((x, core), (x, 1 - core))
        if n == 4:
            unpack_sib(3)
            unpack_sib(5)
    from_sib(1)
    from_sib(2)
    gained((xm, 1 - core), (xp, 1 - core))
    hop(0, 4)
    hop(1, 4)
    unpack(4)
    from_sib(3)
    gained((xo, core), (xo, 1 - core))
    gsc[...] = jnp.zeros((8, 1024), F32)
    gsc[0:1, :800] = gscale[...][None, :]
    gsc[1:2, :800] = uscale[...][None, :]
    shifted = gsc[...]
    mine = shifted
    for s in range(1, 4):
        mine = jnp.where(src == s, pltpu.roll(shifted, 1024 - HID * s, 1), mine)
    both = dot(xk[...], wg[...])
    rms = lax.rsqrt((ssq[0, :, 0:1] + ssq[1, :, 0:1]) * (1.0 / D) + EPS)
    gate = both[:, :PAD] * rms * mine[0:1, :PAD]
    up = pltpu.roll(both, 512 - HID, 1)[:, :PAD] * rms * mine[1:2, :PAD]
    used = lax.broadcasted_iota(jnp.int32, (1, PAD), 1) < HID
    act = jnp.where(used, gate / (1.0 + jnp.exp(-gate)) * up, 0.0).astype(BF)
    act = dot(act, p256[...]).astype(BF)
    xk[:, :PAD] = act

    def act_rows(h, cc):
        return pl.ds(mo((h * 2 + cc) * 64, 64), 64)

    def ac_copy(h):
        return rcopy(xk.at[act_rows(h, 1 - core), 0:PAD], actr.at[h], acs.at[h], acr.at[h], SIB)

    for h in (0, 1):
        ac_copy(h).start()
    unpack_sib(4)
    own_act = jnp.concatenate([xk[act_rows(0, core), 0:PAD], xk[act_rows(1, core), 0:PAD]], axis=0)

    def first(n, _):
        half_down[:, pl.ds(mo(n * 640, 128), 640)] = dot(own_act, wd[0, :, pl.ds(mo(xl * HALF + n * 640, 128), 640)])
        return 0

    lax.fori_loop(0, 4, first, 0)
    for h in (0, 1):
        ac_copy(h).wait_recv()
    sib_act = jnp.concatenate([actr[0], actr[1]], axis=0)

    def second(n, _):
        at = pl.ds(mo(xl * HALF + n * 640, 128), 640)
        pd[:, at] = (half_down[:, pl.ds(mo(n * 640, 128), 640)] + dot(sib_act, wd[1, :, at])).astype(BF)
        return 0

    def other(n, _):
        at = pl.ds(mo((1 - xl) * HALF + n * 640, 128), 640)
        pd[:, at] = (dot(own_act, wd[0, :, at]) + dot(sib_act, wd[1, :, at])).astype(BF)
        return 0

    sides = (PLUS, MINUS)
    nexts = (xp, xm)

    def slab(xx, q, w):
        rows = pl.ds(mo((xx // 2) * 64 + q * 16, 16), 16)
        return rows, pl.ds(mo((xx % 2) * HALF + w * 1280, 128), 1280)

    def pre_copy(q, w):
        a, b = slab(xo, q, w)
        return rcopy(pd.at[a, b], pre.at[q, w], xps.at[q, w], xpr.at[q, w], sides[w])

    def plain_copy(q, w):
        a, b = slab(nexts[w], q, 1 - w)
        return rcopy(pd.at[a, b], rplain.at[q, w], xas.at[q, w], xar.at[q, w], sides[w])

    def merge_copy(q, w):
        return rcopy(smerge.at[q, w], rmerge.at[q, w], xms.at[q, w], xmr.at[q, w], sides[w])

    def pre_start(q):
        for w in (0, 1):
            pre_copy(q, w).start()

    def plain_start(q):
        for w in (0, 1):
            plain_copy(q, w).start()

    def merge(q):
        for w in (0, 1):
            pre_copy(q, w).wait_recv()
            a, b = slab(nexts[w], q, w)
            smerge[q, w] = (pd[a, b].astype(F32) + pre[q, w].astype(F32)).astype(BF)
            merge_copy(q, w).start()

    def window(yy):
        return pl.ds(mo(320 * yy - 64 * (yy % 2), 128), 384)

    def y_copy(d, q):
        to = (y + d) % YS
        at = pl.ds(q * 16, 16)
        return rcopy(u.at[at, window(to)], yr.at[y, at, :], yss.at[q, to], ysr.at[q, y], {"tp": xl * YS + to})

    def y_in(d, q):
        frm = (y + d) % YS
        at = pl.ds(q * 16, 16)
        return rcopy(u.at[at, window(frm)], yr.at[frm, at, :], yss.at[q, frm], ysr.at[q, frm], {"tp": xl * YS + frm})

    def finish(q):
        at = slice(q * 16, q * 16 + 16)
        for w in (0, 1):
            plain_copy(q, w).wait_recv()
        for w in (0, 1):
            merge_copy(q, w).wait_recv()
            a, b = slab(x, q, w)
            v = pd[a, b].astype(F32) + rplain[q, 1 - w].astype(F32) + rmerge[q, w].astype(F32)
            u[at, w * 1280 : w * 1280 + 1280] = v.astype(BF)
        for d in NEAR[:0:-1]:
            y_copy(d, q).start()
        yr[y, at, :] = u[at, window(y)]

    lax.fori_loop(0, 4, second, 0)
    pre_start(0)
    pre_start(1)
    lax.fori_loop(0, 4, other, 0)
    plain_start(0)
    merge(0)
    pre_start(2)
    plain_start(1)
    merge(1)
    pre_start(3)
    plain_start(2)
    finish(0)
    merge(2)
    plain_start(3)
    finish(1)
    merge(3)
    finish(2)
    finish(3)
    for d in (1, 2, 3):
        w1_gu(d).wait_send()
        w1_dn(d).wait_send()
    wo_copy.wait_send()
    wo_share.wait_send()
    for h in (0, 1):
        for step in (1, 2, 3, 4):
            for way in (0, 1):
                for c in ring(h, step, way):
                    c.wait_send()
    for slot in range(ZS):
        to_sib(slot).wait_send()

    def sent_tp(d, _):
        b_copy(d).wait_send()
        h_copy(d).wait_send()
        return 0

    lax.fori_loop(1, 16, sent_tp, 0)
    for d in NEAR[1:]:
        for s in (0, 1):
            r_copy(d, s).wait_send()
    for s in (0, 1):
        for d in NEAR[1:]:
            fy_copy(d, s).wait_send()
        for i in range(YS):
            fx_copy(0, i, s).wait_send()
            fx_copy(1, i, s).wait_send()
            fq_copy(i, s).wait_send()
            for j in range(4):
                fs_copy(j, i, s).wait_send()
    for w in (0, 1):
        ac_copy(w).wait_send()
        for q in range(4):
            pre_copy(q, w).wait_send()
            plain_copy(q, w).wait_send()
            merge_copy(q, w).wait_send()
    for q in range(4):
        for d in NEAR[1:]:
            y_in(d, q).wait_recv()
    last = yr[0].astype(F32)
    for i in range(1, YS):
        last = last + yr[i].astype(F32)
    at = pl.ds(mo(xl * HALF + 320 * y - 64 * (y % 2), 128), 384)
    last = X[pl.ds(mo(src * 64, 64), 64), at].astype(F32) + last * vec[3:4, at]
    last = jnp.where(odd_y, pltpu.roll(last, 320, 1), last)
    out[...] = last[:, :320].astype(BF)

    for q in range(4):
        for d in NEAR[1:]:
            y_copy(d, q).wait_send()


def local(
    hidden_in, attn_gain, w_qkv, qkv_scale, q_gain, k_gain, key_cache, value_cache, lengths, w_out, out_scale,
    mlp_gain, w_gate, w_up, gate_scale, up_scale, w_down, down_scale,
):
    V, S = pltpu.VMEM, pltpu.SemaphoreType.DMA
    I32 = jnp.int32
    scratch = [
        V((ROWS, D), BF), V((D,), F32), V((320,), F32), V((HEAD,), F32), V((HEAD,), F32), V((D,), F32), V((D,), F32),
        V((40, 800), I32), V((40, 800), I32), V((800,), F32), V((800,), F32), V((160, HID), I32), V((D,), F32),
        V((320, 1280), I32), V((4, 128, 512), BF), V((4, 128, 512), BF), V((64, HALF), I32), V((512, 512), BF),
        V((HEAD, HEAD), BF), V((PAD, PAD), BF), V((4, ROWS, 256), BF), V((2 * ROWS, HALF), F32),
        V((8, D), F32), V((8, 1024), F32),
        V((ROWS, 384), F32), V((4, 40, 384), I32), V((4, 56, 256), I32),
        V((16, 4, 384), F32), V((16, 4, 384), F32), V((160, HEAD), F32), V((32, HEAD), F32),
        V((YS, 16, HEAD), BF), V((256, HEAD), BF), V((64, HALF), I32), V((512, HALF), BF), V((ROWS, HALF), BF),
        V((2, YS, 16, 640), BF), V((ALL, D), BF), V((ALL, D), BF), V((2, ALL, HEAD), F32),
        V((ZS, 160, 384), I32), V((4, 56, 256), I32), V((ZS, 2, 56, 384), I32), V((ZS, 2, 56, 384), I32),
        V((D, 512), BF), V((2, 256, D), BF), V((2, ROWS, PAD), BF), V((2 * ROWS, D), BF),
        V((4, 2, 16, 1280), BF), V((4, 2, 16, 1280), BF), V((4, 2, 16, 1280), BF), V((4, 2, 16, 1280), BF),
        V((ROWS, HALF), BF), V((YS, ROWS, 384), BF),
        S((18,)), S((2, 4)), S((2, 4)), S((2,)), S((2,)), S((2, 2, 4, 2)), S((2, 2, 4, 2)), S((8,)), S((8,)),
        S((16,)), S((16,)), S((16,)), S((16,)),
        S((2, 8)), S((2, 8)), S((2, 8)), S((2, 8)), S((2, 2, 8)), S((2, 2, 8)), S((2, 8)), S((2, 8)), S((2, 4, 8)), S((2, 4, 8)),
        S((2,)), S((2,)), S((4, 2)), S((4, 2)), S((4, 2)), S((4, 2)), S((4, 2)), S((4, 2)), S((4, 8)), S((4, 8)),
    ]
    vmem = pl.BlockSpec(memory_space=pltpu.VMEM)
    far = pl.BlockSpec(memory_space=pl.ANY)
    specs = [far] * 18
    specs[8] = pl.BlockSpec(memory_space=pltpu.SMEM)
    return pl.pallas_call(
        kernel,
        out_shape=jax.ShapeDtypeStruct((ROWS, 320), BF),
        in_specs=specs,
        out_specs=vmem,
        scratch_shapes=scratch,
        compiler_params=pltpu.CompilerParams(
            collective_id=0, has_side_effects=True, vmem_limit_bytes=60 * 1024 * 1024
        ),
        name="layer",
    )(
        hidden_in, attn_gain, w_qkv.T, qkv_scale, q_gain, k_gain, key_cache, value_cache, lengths, w_out, out_scale,
        mlp_gain, w_gate, w_up, gate_scale, up_scale, w_down.T, down_scale,
    )


def solution(mesh):
    return jax.shard_map(
        local,
        mesh=mesh,
        in_specs=(
            P(("grp", "src"), None),
            P(),
            P(None, "tp"),
            P("tp"),
            P(),
            P(),
            P(("grp", "src"), "tp", None, None),
            P(("grp", "src"), "tp", None, None),
            P(("grp", "src"), "tp"),
            P("tp", None),
            P(),
            P(),
            P(("grp", "src"), "tp"),
            P(("grp", "src"), "tp"),
            P("tp"),
            P("tp"),
            P("tp", ("grp", "src")),
            P(),
        ),
        out_specs=P(("grp", "src"), "tp"),
        check_vma=False,
    )
```

```python
import math

import jax
import jax.numpy as jnp
from jax import lax
from jax.experimental import pallas as pl
from jax.experimental.pallas import tpu as pltpu
from jax.sharding import PartitionSpec as P

D = 5120
HALF = 2560
HEADS = 32
KV = 4
HEAD = 128
ROWS = 64
ALL = 256
YS = 8
ZS = 8
HID = 200
PAD = 256
EPS = 1e-06
ROPE = 1000000.0
MESH = pl.DeviceIdType.MESH
F32 = jnp.float32
BF = jnp.bfloat16
NEAR = (0, 1, 7, 2, 6, 3, 5, 4)


def mo(value, k):
    return pl.multiple_of(value, k)


def byte_of(words, k):
    return jnp.right_shift(jnp.left_shift(words, 24 - 8 * k), 24).astype(F32).astype(BF)


def one_hot(n, used, stride):
    row = lax.broadcasted_iota(jnp.int32, (n, n), 0)
    col = lax.broadcasted_iota(jnp.int32, (n, n), 1)
    shift = stride.bit_length() - 1
    k, r = jnp.right_shift(col, shift), jnp.bitwise_and(col, stride - 1)
    return jnp.where((row == 4 * r + k) & (r < used), 1.0, 0.0).astype(BF)


def dot(a, b):
    return jnp.dot(a, b, preferred_element_type=F32)


def kernel(
    hid_hbm, again_hbm, wq_hbm, qscale_hbm, qgain_hbm, kgain_hbm, kc_hbm, vc_hbm, lens, wout, oscale_hbm, mgain_hbm,
    wgate_hbm, wup_hbm, gscale_hbm, uscale_hbm, wdown_hbm, dscale_hbm,
    out,
    hid, again, qscale, qgain, kgain, oscale, mgain, wgate, wup, gscale, uscale, wdown, dscale,
    wq, kc, vc, woh, p512, p128, p256, picks, half_down, vec, gsc, stage, gu4, dn4, bsend, brecv, qs, vs, hsend, hrecv, wo_r, wo, pm, rs, X, xk, ssq,
    gub, dnp, dnb, dns, wg, wd, actr, pd, pre, smerge, rplain, rmerge, u, yr,
    ld, w1s, w1r, wos, wor, zs, zr, ns, nr, bs, br, hs, hr, rss, rsr, fys, fyr, fxs, fxr, fqs, fqr, fss, fsr,
    acs, acr, xps, xpr, xas, xar, xms, xmr, yss, ysr,
):
    z = lax.axis_index("grp")
    tp = lax.axis_index("tp")
    src = lax.axis_index("src")
    xl, y = tp // YS, tp % YS
    xh, core = src // 2, src % 2
    x = xh * 2 + xl

    def at_x(xx, cc):
        return {"tp": (xx % 2) * YS + y, "src": (xx // 2) * 2 + cc}

    xp, xm, xo = (x + 1) % 4, (x + 3) % 4, (x + 2) % 4
    PLUS, MINUS = at_x(xp, core), at_x(xm, core)
    SIB = {"src": xh * 2 + 1 - core}
    ZP, ZM = {"grp": (z + 1) % ZS}, {"grp": (z + ZS - 1) % ZS}

    def rcopy(a, b, s, r, to):
        return pltpu.make_async_remote_copy(
            src_ref=a, dst_ref=b, send_sem=s, recv_sem=r, device_id=to, device_id_type=MESH
        )

    load_wq = [
        pltpu.make_async_copy(wq_hbm.at[:, pl.ds(i * 640, 640)], wq.at[:, pl.ds(i * 640, 640)], ld.at[i]) for i in (0, 1)
    ]
    load_kc = pltpu.make_async_copy(kc_hbm.at[0], kc, ld.at[2])
    load_vc = pltpu.make_async_copy(vc_hbm.at[0], vc, ld.at[3])
    load_wo = pltpu.make_async_copy(wout.at[:, pl.ds(mo(xl * HALF, 128), HALF)], woh, ld.at[4])
    pairs = (
        (hid_hbm, hid), (again_hbm, again), (wgate_hbm, wgate), (wup_hbm, wup), (wdown_hbm, wdown), (mgain_hbm, mgain),
        (oscale_hbm, oscale), (dscale_hbm, dscale), (qscale_hbm, qscale), (qgain_hbm, qgain), (kgain_hbm, kgain),
        (gscale_hbm, gscale), (uscale_hbm, uscale),
    )
    loads = [pltpu.make_async_copy(a, b, ld.at[5 + i]) for i, (a, b) in enumerate(pairs)]
    for c in loads[2:5] + loads[:2] + loads[5:] + load_wq:
        c.start()
    load_kc.start()
    load_vc.start()
    load_wo.start()

    barrier = pltpu.get_barrier_semaphore()

    def greet_tp(d, _):
        pl.semaphore_signal(barrier, inc=1, device_id={"tp": (tp + d) % 16}, device_id_type=MESH)
        return 0

    def greet_src(d, _):
        pl.semaphore_signal(barrier, inc=1, device_id={"src": (src + d) % 4}, device_id_type=MESH)
        return 0

    lax.fori_loop(1, 16, greet_tp, 0)
    lax.fori_loop(1, 4, greet_src, 0)
    across = {"tp": (1 - xl) * YS + y, "src": (1 - xh) * 2 + core}
    for to in (across, ZP, ZM):
        pl.semaphore_signal(barrier, inc=1, device_id=to, device_id_type=MESH)

    p512[...] = one_hot(512, 128, 128)
    for c in loads:
        c.wait()
    turned = jnp.transpose(wdown[...])
    for s in range(4):
        piece = jnp.concatenate([wgate[:, HID * s : HID * s + HID], wup[:, HID * s : HID * s + HID]], axis=1)
        gu4[s] = piece[:, :384]
        dn4[s] = jnp.zeros((56, 256), jnp.int32)
        dn4[s, 0:50, 0:160] = turned[50 * s : 50 * s + 50, :]
        dn4[s, 0:40, 160:176] = piece[:, 384:400]
    gub[0, pl.ds(mo(src * 40, 8), 40), :] = gu4[src]
    dnp[src] = dn4[src]
    vec[0:1, :] = again[...][None, :]
    vec[1:2, :] = mgain[...][None, :]
    vec[2:3, :] = oscale[...][None, :]
    vec[3:4, :] = dscale[...][None, :]

    total = jnp.zeros((ROWS, 1), F32)
    for g in range(10):
        v = hid[:, g * 512 : (g + 1) * 512].astype(F32)
        total = total + jnp.sum(v * v, axis=1, keepdims=True)
    rms = lax.rsqrt(total * (1.0 / D) + EPS)

    for g in range(10):
        at = slice(g * 512, g * 512 + 512)
        v = (hid[:, at].astype(F32) * rms * vec[0:1, at]).astype(BF)
        xk[:ROWS, at] = dot(v, p512[...]).astype(BF)
    pl.semaphore_wait(barrier, 21)

    def w1_gu(d):
        s2 = (src + d) % 4
        return rcopy(
            gu4.at[s2], gub.at[0, pl.ds(mo(src * 40, 8), 40), :], w1s.at[0, d], w1r.at[0, src], {"src": s2}
        )

    def w1_dn(d):
        s2 = (src + d) % 4
        return rcopy(dn4.at[s2], dnp.at[src], w1s.at[1, d], w1r.at[1, src], {"src": s2})

    for d in (1, 2, 3):
        w1_gu(d).start()
        w1_dn(d).start()

    acc = jnp.zeros((ROWS, 320), F32)
    for c in load_wq:
        c.wait()
    for g in range(10):
        w = wq[:, g * 128 : g * 128 + 128]
        for k in (0, 2):
            acc = acc + lax.dot_general(
                xk[:ROWS, g * 512 + k * 128 : g * 512 + k * 128 + 256],
                jnp.concatenate([byte_of(w, k), byte_of(w, k + 1)], axis=1),
                (((1,), (1,)), ((), ())),
                preferred_element_type=F32,
            )
    qkv = (acc * qscale[...][None, :]).astype(BF).astype(F32)
    stage[...] = jnp.zeros((ROWS, 384), F32)
    stage[:, :320] = qkv
    odd_y = (y % 2) == 1
    placed = stage[...]
    placed = jnp.where(odd_y, pltpu.roll(placed, 64, 1), placed)
    for t in range(16):
        bsend[t] = placed[4 * t : 4 * t + 4, :]

    def b_copy(d):
        to = (tp + d) % 16
        return rcopy(bsend.at[to], brecv.at[tp], bs.at[to], br.at[tp], {"tp": to})

    def start_b(d, _):
        b_copy(d).start()
        return 0

    def wait_b(d, _):
        frm = (tp + d) % 16
        rcopy(bsend.at[frm], brecv.at[frm], bs.at[frm], br.at[frm], {"tp": frm}).wait_recv()
        return 0

    lax.fori_loop(1, 16, start_b, 0)
    wo_side = (x + 1 + 2 * core) % 4
    wo_rows = pl.ds(mo(core * 32, 32), 32)
    wo_copy = rcopy(
        wout.at[wo_rows, pl.ds(mo((1 - xl) * HALF, 128), HALF)], wo_r.at[wo_rows, :], wos.at[0], wor.at[0],
        at_x(wo_side, core),
    )
    wo_share = rcopy(wo_r.at[wo_rows, :], wo_r.at[wo_rows, :], wos.at[1], wor.at[1], SIB)
    wo_copy.start()
    brecv[pl.ds(tp, 1)] = bsend[pl.ds(tp, 1)]

    def w1_in(d):
        s2 = (src + d) % 4
        rcopy(gu4.at[s2], gub.at[0, pl.ds(mo(s2 * 40, 8), 40), :], w1s.at[0, d], w1r.at[0, s2], {"src": s2}).wait_recv()
        rcopy(dn4.at[s2], dnp.at[s2], w1s.at[1, d], w1r.at[1, s2], {"src": s2}).wait_recv()

    def assemble(h):
        one, two = dnp[2 * h], dnp[2 * h + 1]
        dnb[0, h] = jnp.concatenate(
            [one[:, :160], two[:, :160], one[:, 160:192], two[:, 160:192]], axis=1
        )

    def ring(h, step, way):
        a = step - 1 if way == 0 else (9 - step) % 8
        b = step if way == 0 else 8 - step
        to = ZP if way == 0 else ZM
        if step == 4:
            n, off, d_at = (40, 0, slice(0, 32)) if way == 0 else (40, 40, slice(32, 56))
        else:
            n, off, d_at = 80, 0, slice(0, 56)
        at = pl.ds(mo(h * 80 + off, 8), n)
        one = rcopy(gub.at[a, at, :], gub.at[b, at, :], zs.at[h, way, step - 1, 0], zr.at[h, way, step - 1, 0], to)
        two = rcopy(
            dnb.at[a, h, d_at, :], dnb.at[b, h, d_at, :], zs.at[h, way, step - 1, 1], zr.at[h, way, step - 1, 1], to
        )
        return one, two

    def ring_start(h, step):
        for way in (0, 1):
            for c in ring(h, step, way):
                c.start()

    def ring_wait(h, step):
        for way in (0, 1):
            for c in ring(h, step, way):
                c.wait_recv()

    def to_sib(slot):
        return rcopy(dnb.at[slot], dns.at[slot], ns.at[slot], nr.at[slot], SIB)

    def hop(stream, step):
        h = xh if stream == 0 else 1 - xh
        ring_wait(h, step)
        if step < 4:
            ring_start(h, step + 1)
        if stream == 1:
            to_sib(step).start()
            if step < 4:
                to_sib(8 - step).start()

    def unpack_down(ref, slot, which):
        zz = (z + ZS - slot) % ZS
        w = jnp.concatenate([ref[slot, 0, :, :320], ref[slot, 1, :, :320]], axis=1)
        for k in range(4):
            wd[which, k * 64 : k * 64 + 56, pl.ds(mo(zz * 640, 128), 640)] = byte_of(w, k)

    lane40 = lax.broadcasted_iota(jnp.int32, (40, 128), 1)

    def unpack(slot):
        zz = (z + ZS - slot) % ZS

        def rows(i, _):
            w = gub[slot, pl.ds(mo(i * 32, 32), 32), :]
            for k in range(4):
                wg[pl.ds(mo(k * 1280 + zz * 160 + i * 32, 32), 32), 0:384] = byte_of(w, k)
            return 0

        lax.fori_loop(0, 5, rows, 0)
        tails = []
        for s in range(4):
            t = dnb[slot, s // 2, 0:40, 256:384]
            t = pltpu.roll(t, 64 - 32 * (s % 2), 1)
            tails.append(jnp.where(lane40 < 16, t, 0))
        tails = jnp.concatenate(tails, axis=0)
        for k in range(4):
            wg[pl.ds(mo(k * 1280 + zz * 160, 32), 160), 384:512] = byte_of(tails, k)
        unpack_down(dnb, slot, 0)

    def unpack_sib(slot):
        to_sib(slot).wait_recv()
        unpack_down(dns, slot, 1)

    rcopy(
        gu4.at[0], gub.at[0, pl.ds(mo((src + 1 - 2 * core) * 40, 8), 40), :], w1s.at[0, 1],
        w1r.at[0, src + 1 - 2 * core], SIB,
    ).wait_recv()
    rcopy(dn4.at[0], dnp.at[src + 1 - 2 * core], w1s.at[1, 1], w1r.at[1, src + 1 - 2 * core], SIB).wait_recv()
    assemble(xh)
    ring_start(xh, 1)
    wd[...] = jnp.zeros(wd.shape, BF)

    def unpack_wo(ref, base):
        def cols(i, _):
            at = pl.ds(mo(i * 640, 128), 640)
            for hl in range(2):
                w = ref[hl * 32 : hl * 32 + 32, at]
                for k in range(4):
                    wo[pl.ds(mo(base + hl * 128 + k * 32, 32), 32), at] = byte_of(w, k)
            return 0

        lax.fori_loop(0, 4, cols, 0)

    load_wo.wait()
    unpack_wo(woh, xl * 256)
    far = (1 - xh) * 2
    for s2 in (far, far + 1):
        rcopy(gu4.at[0], gub.at[0, pl.ds(mo(s2 * 40, 8), 40), :], w1s.at[0, 2], w1r.at[0, s2], {"src": s2}).wait_recv()
        rcopy(dn4.at[0], dnp.at[s2], w1s.at[1, 2], w1r.at[1, s2], {"src": s2}).wait_recv()
    assemble(1 - xh)
    ring_start(1 - xh, 1)
    to_sib(0).start()
    load_kc.wait()
    load_vc.wait()
    half = lax.broadcasted_iota(jnp.int32, (8, HEAD), 1)
    pair = jnp.bitwise_and(lax.broadcasted_iota(jnp.int32, (8, HEAD), 0), 3)
    length = jnp.full((8, HEAD), lens[0, 0], jnp.int32)
    for b in range(1, 4):
        length = jnp.where(pair == b, lens[0, b], length)
    freq = jnp.exp(jnp.bitwise_and(half, 63).astype(F32) * (-math.log(ROPE) / 64))
    angle = length.astype(F32) * freq
    ctab = jnp.cos(angle)
    stab = jnp.sin(angle)
    stab = jnp.where(half < 64, -stab, stab)

    p128[...] = one_hot(128, 32, 32)
    p256[...] = one_hot(PAD, HID // 4, 64)
    t = lax.broadcasted_iota(jnp.int32, (ROWS, 256), 0)
    c = lax.broadcasted_iota(jnp.int32, (ROWS, 256), 1)
    for hl in range(4):
        want = jnp.right_shift(t, 2) * 16 + hl * 4 + jnp.bitwise_and(t, 3)
        picks[hl] = jnp.where(c == want, 1.0, 0.0).astype(BF)
    lax.fori_loop(1, 16, wait_b, 0)
    lane = lax.broadcasted_iota(jnp.int32, (4, HEAD), 1)
    for p in range(8):
        even, odd = brecv[2 * p], brecv[2 * p + 1]
        pieces = (
            even[:, 0:128],
            even[:, 128:256],
            jnp.where(lane < 64, even[:, 256:384], odd[:, 0:128]),
            odd[:, 128:256],
            odd[:, 256:384],
        )
        for j, piece in enumerate(pieces):
            h = 5 * p + j
            if h < HEADS:
                qs[4 * h : 4 * h + 4, :] = piece
            elif h < HEADS + KV:
                at = 128 + 8 * (h - HEADS)
                qs[at : at + 4, :] = piece
                qs[at + 4 : at + 8, :] = piece
            else:
                at = 8 * (h - HEADS - KV)
                vs[at : at + 4, :] = piece
                vs[at + 4 : at + 8, :] = piece
    v = qs[...]
    v = v * lax.rsqrt(jnp.mean(v * v, axis=1, keepdims=True) + EPS)
    row = lax.broadcasted_iota(jnp.int32, (160, HEAD), 0)
    v = v * jnp.where(row < 128, qgain[...][None, :], kgain[...][None, :])
    turned = pltpu.roll(v, 64, 1)
    v = v.reshape(20, 8, HEAD) * ctab[None] + turned.reshape(20, 8, HEAD) * stab[None]
    v = v.reshape(160, HEAD).astype(BF)
    scale = 1.0 / math.sqrt(HEAD)
    seq = jnp.bitwise_and(lax.broadcasted_iota(jnp.int32, (32, HEAD), 0), 3)
    live = jnp.where(half < length, 1.0, 0.0)
    live = jnp.broadcast_to(live[None], (4, 8, HEAD)).reshape(32, HEAD) > 0.5
    heads = []
    for g in range(KV):
        q = v[32 * g : 32 * g + 32]
        newk = v[128 + 8 * g : 136 + 8 * g].astype(F32)
        own = jnp.sum((q.astype(F32).reshape(4, 8, HEAD) * newk[None]).reshape(32, HEAD), axis=1, keepdims=True)
        own = own * scale
        s = jnp.zeros((32, HEAD), F32)
        for b in range(4):
            sb = lax.dot_general(
                q, kc[b, :, g * 128 : (g + 1) * 128], (((1,), (1,)), ((), ())), preferred_element_type=F32
            )
            s = jnp.where(seq == b, sb, s)
        s = jnp.where(live, s * scale, -jnp.inf)
        top = jnp.maximum(jnp.max(s, axis=1, keepdims=True), own)
        e = jnp.exp(s - top)
        own_e = jnp.exp(own - top)
        den = jnp.sum(e, axis=1, keepdims=True) + own_e
        newv = vs[8 * g : 8 * g + 8, :]
        low = own_e.astype(BF).astype(F32)
        num = (low.reshape(4, 8, 1) * newv[None]).reshape(32, HEAD)
        for b in range(4):
            eb = jnp.where(seq == b, e, 0.0).astype(BF)
            num = num + dot(eb, vc[b, :, g * 128 : (g + 1) * 128])
        heads.append(num / den)
    for yy in range(YS):
        g, at = yy // 4, 8 * (yy % 4)
        hsend[yy] = jnp.concatenate([heads[g][at : at + 8], heads[g + 2][at : at + 8]], axis=0).astype(BF)

    def h_slot(t):
        return hrecv.at[pl.ds(mo(t * 16, 16), 16), :]

    def h_copy(d):
        to = (tp + d) % 16
        return rcopy(hsend.at[to % YS], h_slot(tp), hs.at[to], hr.at[tp], {"tp": to})

    def start_h(d, _):
        h_copy(d).start()
        return 0

    def wait_h(d, _):
        frm = (tp + d) % 16
        rcopy(hsend.at[frm % YS], h_slot(frm), hs.at[frm], hr.at[frm], {"tp": frm}).wait_recv()
        return 0

    lax.fori_loop(1, 16, start_h, 0)
    hrecv[pl.ds(mo(tp * 16, 16), 16), :] = hsend[y]

    hop(0, 1)
    wo_copy.wait_recv()
    wo_share.start()
    unpack(0)
    wo_share.wait_recv()
    unpack_wo(wo_r, (1 - xl) * 256)

    lax.fori_loop(1, 16, wait_h, 0)
    got = hrecv[...]
    zcat = [dot(dot(picks[hl], got).astype(BF), p128[...]).astype(BF) for hl in range(4)]
    zcat = jnp.concatenate(zcat, axis=1)

    def part(yy, s):
        return pl.ds(mo(32 * (yy // 4) + 16 * s, 16), 16), pl.ds(mo(640 * (yy % 4), 128), 640)

    for cb in range(4):
        pm[:, cb * 640 : cb * 640 + 640] = dot(zcat, wo[:, cb * 640 : cb * 640 + 640]).astype(BF)

    def r_copy(d, s):
        to = (y + d) % YS
        a, b = part(to, s)
        return rcopy(pm.at[a, b], rs.at[s, y], rss.at[s, to], rsr.at[s, y], {"tp": xl * YS + to})

    def wait_r(d, s):
        frm = (y + d) % YS
        a, b = part(frm, s)
        rcopy(pm.at[a, b], rs.at[s, frm], rss.at[s, frm], rsr.at[s, frm], {"tp": xl * YS + frm}).wait_recv()

    for s in (0, 1):
        for d in NEAR[:0:-1]:
            r_copy(d, s).start()
        a, b = part(y, s)
        rs[s, y] = pm[a, b]
    unpack_sib(0)
    hop(1, 1)

    def blk(xx, cc, yy, s):
        r0 = ((xx // 2) * 2 + cc) * 64 + 32 * (yy // 4) + 16 * s
        c0 = (xx % 2) * HALF + 640 * (yy % 4)
        return X.at[pl.ds(mo(r0, 16), 16), pl.ds(mo(c0, 128), 640)]

    def fy_copy(d, s):
        to = (y + d) % YS
        b0 = blk(x, core, y, s)
        return rcopy(b0, b0, fys.at[s, to], fyr.at[s, y], {"tp": xl * YS + to})

    def fx_copy(way, i, s):
        b0 = blk(x, core, (y + i) % YS, s)
        return rcopy(b0, b0, fxs.at[s, way, i], fxr.at[s, way, i], PLUS if way == 0 else MINUS)

    def fx_in(way, i, s):
        b0 = blk(xm if way == 0 else xp, core, (y + i) % YS, s)
        return rcopy(b0, b0, fxs.at[s, way, i], fxr.at[s, way, i], MINUS if way == 0 else PLUS)

    def fq_copy(i, s):
        if s == 1 and i in (5, 4):
            b0 = blk(x, core, (y + i) % YS, s)
            return rcopy(b0, b0, fqs.at[s, i], fqr.at[s, i], at_x(xo, core))
        way = i % 2
        b0 = blk(xm if way == 0 else xp, core, (y + i) % YS, s)
        return rcopy(b0, b0, fqs.at[s, i], fqr.at[s, i], PLUS if way == 0 else MINUS)

    def fq_in(i, s):
        b0 = blk(xo, core, (y + i) % YS, s)
        return rcopy(b0, b0, fqs.at[s, i], fqr.at[s, i], MINUS if i % 2 == 0 else PLUS)

    froms = (x, xm, xp, xo)

    def fs_copy(j, i, s):
        b0 = blk(froms[j], core, (y + i) % YS, s)
        return rcopy(b0, b0, fss.at[s, j, i], fsr.at[s, j, i], SIB)

    def fs_in(j, i, s):
        b0 = blk(froms[j], 1 - core, (y + i) % YS, s)
        return rcopy(b0, b0, fss.at[s, j, i], fsr.at[s, j, i], SIB)

    def gained(*slabs):
        side = slabs[0][0] % 2
        rows = [pl.ds(mo(((xx // 2) * 2 + cc) * 64, 64), 64) for xx, cc in slabs]
        total = jnp.zeros((64 * len(rows), 1), F32)
        for g in range(5):
            cs = pl.ds(mo(side * HALF + g * 512, 128), 512)
            v = jnp.concatenate([X[at, cs] for at in rows], axis=0).astype(F32)
            total = total + jnp.sum(v * v, axis=1, keepdims=True)
            v = dot((v * vec[1:2, cs]).astype(BF), p512[...]).astype(BF)
            for k in range(4):
                to = pl.ds(mo(k * 1280 + side * 640 + g * 128, 128), 128)
                for n, at in enumerate(rows):
                    xk[at, to] = v[n * 64 : n * 64 + 64, k * 128 : (k + 1) * 128]
        for n, at in enumerate(rows):
            ssq[side, at, :] = jnp.broadcast_to(total[n * 64 : n * 64 + 64], (64, HEAD))

    def onward(i, s):
        fx_copy(0, i, s).start()
        fx_copy(1, i, s).start()
        if s == 1 and i in (5, 4):
            fq_copy(i, s).start()
        fs_copy(0, i, s).start()

    def mid(s):
        for d in NEAR[1:]:
            wait_r(d, s)
        m = rs[s, 0].astype(F32)
        for i in range(1, YS):
            m = m + rs[s, i].astype(F32)
        cols = pl.ds(mo(xl * HALF + 640 * (y % 4), 128), 640)
        m = hid[pl.ds(mo(32 * (y // 4) + 16 * s, 16), 16), cols].astype(F32) + m * vec[2:3, cols]
        X[pl.ds(mo(src * 64 + 32 * (y // 4) + 16 * s, 16), 16), cols] = m.astype(BF)
        for d in NEAR[1:]:
            fy_copy(d, s).start()
        onward(0, s)

    def from_y(i, s):
        yy = (y + i) % YS
        b0 = blk(x, core, yy, s)
        rcopy(b0, b0, fys.at[s, yy], fyr.at[s, yy], {"tp": xl * YS + yy}).wait_recv()
        onward(i, s)

    def from_x(i, s):
        fx_in(0, i, s).wait_recv()
        fx_in(1, i, s).wait_recv()
        if not (s == 1 and i in (5, 4)):
            fq_copy(i, s).start()
        fs_copy(1, i, s).start()
        fs_copy(2, i, s).start()

    def from_sib(j):
        for s in (0, 1):
            for i in NEAR:
                fs_in(j, i, s).wait_recv()

    mid(0)
    hop(0, 2)
    unpack(1)
    mid(1)
    hop(1, 2)

    def from_q(i, s):
        fq_in(i, s).wait_recv()
        fs_copy(3, i, s).start()

    idle = {1: (unpack, 7), 2: (unpack, 2), 3: (unpack, 6), 4: (unpack_sib, 1), 5: (unpack_sib, 7)}
    for n in range(1, 8):
        from_y(NEAR[n], 0)
        if n in idle:
            idle[n][0](idle[n][1])
    from_x(0, 0)
    hop(0, 3)
    for i in NEAR[1:]:
        from_y(i, 1)
        from_x(i, 0)
    hop(1, 3)
    for n in range(8):
        from_x(NEAR[n], 1)
        if n == 1:
            unpack_sib(2)
            unpack_sib(6)
        if n == 3:
            unpack(3)
        if n == 5:
            unpack(5)
    for i in NEAR:
        from_q(i, 0)
    gained((xm, core), (xp, core))
    for n in range(8):
        from_q(NEAR[n], 1)
        if n == 1:
            from_sib(0)
            gained((x, core), (x, 1 - core))
        if n == 4:
            unpack_sib(3)
            unpack_sib(5)
    from_sib(1)
    from_sib(2)
    gained((xm, 1 - core), (xp, 1 - core))
    hop(0, 4)
    hop(1, 4)
    unpack(4)
    from_sib(3)
    gained((xo, core), (xo, 1 - core))
    gsc[...] = jnp.zeros((8, 1024), F32)
    gsc[0:1, :800] = gscale[...][None, :]
    gsc[1:2, :800] = uscale[...][None, :]
    shifted = gsc[...]
    mine = shifted
    for s in range(1, 4):
        mine = jnp.where(src == s, pltpu.roll(shifted, 1024 - HID * s, 1), mine)
    both = dot(xk[...], wg[...])
    rms = lax.rsqrt((ssq[0, :, 0:1] + ssq[1, :, 0:1]) * (1.0 / D) + EPS)
    gate = both[:, :PAD] * rms * mine[0:1, :PAD]
    up = pltpu.roll(both, 512 - HID, 1)[:, :PAD] * rms * mine[1:2, :PAD]
    used = lax.broadcasted_iota(jnp.int32, (1, PAD), 1) < HID
    act = jnp.where(used, gate / (1.0 + jnp.exp(-gate)) * up, 0.0).astype(BF)
    act = dot(act, p256[...]).astype(BF)
    xk[:, :PAD] = act

    def act_rows(h, cc):
        return pl.ds(mo((h * 2 + cc) * 64, 64), 64)

    def ac_copy(h):
        return rcopy(xk.at[act_rows(h, 1 - core), 0:PAD], actr.at[h], acs.at[h], acr.at[h], SIB)

    for h in (0, 1):
        ac_copy(h).start()
    unpack_sib(4)
    own_act = jnp.concatenate([xk[act_rows(0, core), 0:PAD], xk[act_rows(1, core), 0:PAD]], axis=0)

    def first(n, _):
        half_down[:, pl.ds(mo(n * 640, 128), 640)] = dot(own_act, wd[0, :, pl.ds(mo(xl * HALF + n * 640, 128), 640)])
        return 0

    lax.fori_loop(0, 4, first, 0)
    for h in (0, 1):
        ac_copy(h).wait_recv()
    sib_act = jnp.concatenate([actr[0], actr[1]], axis=0)

    def second(n, _):
        at = pl.ds(mo(xl * HALF + n * 640, 128), 640)
        pd[:, at] = (half_down[:, pl.ds(mo(n * 640, 128), 640)] + dot(sib_act, wd[1, :, at])).astype(BF)
        return 0

    def other(n, _):
        at = pl.ds(mo((1 - xl) * HALF + n * 640, 128), 640)
        pd[:, at] = (dot(own_act, wd[0, :, at]) + dot(sib_act, wd[1, :, at])).astype(BF)
        return 0

    sides = (PLUS, MINUS)
    nexts = (xp, xm)

    def slab(xx, q, w):
        rows = pl.ds(mo((xx // 2) * 64 + q * 16, 16), 16)
        return rows, pl.ds(mo((xx % 2) * HALF + w * 1280, 128), 1280)

    def pre_copy(q, w):
        a, b = slab(xo, q, w)
        return rcopy(pd.at[a, b], pre.at[q, w], xps.at[q, w], xpr.at[q, w], sides[w])

    def plain_copy(q, w):
        a, b = slab(nexts[w], q, 1 - w)
        return rcopy(pd.at[a, b], rplain.at[q, w], xas.at[q, w], xar.at[q, w], sides[w])

    def merge_copy(q, w):
        return rcopy(smerge.at[q, w], rmerge.at[q, w], xms.at[q, w], xmr.at[q, w], sides[w])

    def pre_start(q):
        for w in (0, 1):
            pre_copy(q, w).start()

    def plain_start(q):
        for w in (0, 1):
            plain_copy(q, w).start()

    def merge(q):
        for w in (0, 1):
            pre_copy(q, w).wait_recv()
            a, b = slab(nexts[w], q, w)
            smerge[q, w] = (pd[a, b].astype(F32) + pre[q, w].astype(F32)).astype(BF)
            merge_copy(q, w).start()

    def window(yy):
        return pl.ds(mo(320 * yy - 64 * (yy % 2), 128), 384)

    def y_copy(d, q):
        to = (y + d) % YS
        at = pl.ds(q * 16, 16)
        return rcopy(u.at[at, window(to)], yr.at[y, at, :], yss.at[q, to], ysr.at[q, y], {"tp": xl * YS + to})

    def y_in(d, q):
        frm = (y + d) % YS
        at = pl.ds(q * 16, 16)
        return rcopy(u.at[at, window(frm)], yr.at[frm, at, :], yss.at[q, frm], ysr.at[q, frm], {"tp": xl * YS + frm})

    def finish(q):
        at = slice(q * 16, q * 16 + 16)
        for w in (0, 1):
            plain_copy(q, w).wait_recv()
        for w in (0, 1):
            merge_copy(q, w).wait_recv()
            a, b = slab(x, q, w)
            v = pd[a, b].astype(F32) + rplain[q, 1 - w].astype(F32) + rmerge[q, w].astype(F32)
            u[at, w * 1280 : w * 1280 + 1280] = v.astype(BF)
        for d in NEAR[:0:-1]:
            y_copy(d, q).start()
        yr[y, at, :] = u[at, window(y)]

    lax.fori_loop(0, 4, second, 0)
    pre_start(0)
    pre_start(1)
    lax.fori_loop(0, 4, other, 0)
    plain_start(0)
    merge(0)
    pre_start(2)
    plain_start(1)
    merge(1)
    pre_start(3)
    plain_start(2)
    finish(0)
    merge(2)
    plain_start(3)
    finish(1)
    merge(3)
    finish(2)
    finish(3)
    for d in (1, 2, 3):
        w1_gu(d).wait_send()
        w1_dn(d).wait_send()
    wo_copy.wait_send()
    wo_share.wait_send()
    for h in (0, 1):
        for step in (1, 2, 3, 4):
            for way in (0, 1):
                for c in ring(h, step, way):
                    c.wait_send()
    for slot in range(ZS):
        to_sib(slot).wait_send()

    def sent_tp(d, _):
        b_copy(d).wait_send()
        h_copy(d).wait_send()
        return 0

    lax.fori_loop(1, 16, sent_tp, 0)
    for d in NEAR[1:]:
        for s in (0, 1):
            r_copy(d, s).wait_send()
    for s in (0, 1):
        for d in NEAR[1:]:
            fy_copy(d, s).wait_send()
        for i in range(YS):
            fx_copy(0, i, s).wait_send()
            fx_copy(1, i, s).wait_send()
            fq_copy(i, s).wait_send()
            for j in range(4):
                fs_copy(j, i, s).wait_send()
    for w in (0, 1):
        ac_copy(w).wait_send()
        for q in range(4):
            pre_copy(q, w).wait_send()
            plain_copy(q, w).wait_send()
            merge_copy(q, w).wait_send()
    for q in range(4):
        for d in NEAR[1:]:
            y_in(d, q).wait_recv()
    last = yr[0].astype(F32)
    for i in range(1, YS):
        last = last + yr[i].astype(F32)
    at = pl.ds(mo(xl * HALF + 320 * y - 64 * (y % 2), 128), 384)
    last = X[pl.ds(mo(src * 64, 64), 64), at].astype(F32) + last * vec[3:4, at]
    last = jnp.where(odd_y, pltpu.roll(last, 320, 1), last)
    out[...] = last[:, :320].astype(BF)

    for q in range(4):
        for d in NEAR[1:]:
            y_copy(d, q).wait_send()


def local(
    hidden_in, attn_gain, w_qkv, qkv_scale, q_gain, k_gain, key_cache, value_cache, lengths, w_out, out_scale,
    mlp_gain, w_gate, w_up, gate_scale, up_scale, w_down, down_scale,
):
    V, S = pltpu.VMEM, pltpu.SemaphoreType.DMA
    I32 = jnp.int32
    scratch = [
        V((ROWS, D), BF), V((D,), F32), V((320,), F32), V((HEAD,), F32), V((HEAD,), F32), V((D,), F32), V((D,), F32),
        V((40, 800), I32), V((40, 800), I32), V((800,), F32), V((800,), F32), V((160, HID), I32), V((D,), F32),
        V((320, 1280), I32), V((4, 128, 512), BF), V((4, 128, 512), BF), V((64, HALF), I32), V((512, 512), BF),
        V((HEAD, HEAD), BF), V((PAD, PAD), BF), V((4, ROWS, 256), BF), V((2 * ROWS, HALF), F32),
        V((8, D), F32), V((8, 1024), F32),
        V((ROWS, 384), F32), V((4, 40, 384), I32), V((4, 56, 256), I32),
        V((16, 4, 384), F32), V((16, 4, 384), F32), V((160, HEAD), F32), V((32, HEAD), F32),
        V((YS, 16, HEAD), BF), V((256, HEAD), BF), V((64, HALF), I32), V((512, HALF), BF), V((ROWS, HALF), BF),
        V((2, YS, 16, 640), BF), V((ALL, D), BF), V((ALL, D), BF), V((2, ALL, HEAD), F32),
        V((ZS, 160, 384), I32), V((4, 56, 256), I32), V((ZS, 2, 56, 384), I32), V((ZS, 2, 56, 384), I32),
        V((D, 512), BF), V((2, 256, D), BF), V((2, ROWS, PAD), BF), V((2 * ROWS, D), BF),
        V((4, 2, 16, 1280), BF), V((4, 2, 16, 1280), BF), V((4, 2, 16, 1280), BF), V((4, 2, 16, 1280), BF),
        V((ROWS, HALF), BF), V((YS, ROWS, 384), BF),
        S((18,)), S((2, 4)), S((2, 4)), S((2,)), S((2,)), S((2, 2, 4, 2)), S((2, 2, 4, 2)), S((8,)), S((8,)),
        S((16,)), S((16,)), S((16,)), S((16,)),
        S((2, 8)), S((2, 8)), S((2, 8)), S((2, 8)), S((2, 2, 8)), S((2, 2, 8)), S((2, 8)), S((2, 8)), S((2, 4, 8)), S((2, 4, 8)),
        S((2,)), S((2,)), S((4, 2)), S((4, 2)), S((4, 2)), S((4, 2)), S((4, 2)), S((4, 2)), S((4, 8)), S((4, 8)),
    ]
    vmem = pl.BlockSpec(memory_space=pltpu.VMEM)
    far = pl.BlockSpec(memory_space=pl.ANY)
    specs = [far] * 18
    specs[8] = pl.BlockSpec(memory_space=pltpu.SMEM)
    return pl.pallas_call(
        kernel,
        out_shape=jax.ShapeDtypeStruct((ROWS, 320), BF),
        in_specs=specs,
        out_specs=vmem,
        scratch_shapes=scratch,
        compiler_params=pltpu.CompilerParams(
            collective_id=0, has_side_effects=True, vmem_limit_bytes=60 * 1024 * 1024
        ),
        name="layer",
    )(
        hidden_in, attn_gain, w_qkv.T, qkv_scale, q_gain, k_gain, key_cache, value_cache, lengths, w_out, out_scale,
        mlp_gain, w_gate, w_up, gate_scale, up_scale, w_down.T, down_scale,
    )


def solution(mesh):
    return jax.shard_map(
        local,
        mesh=mesh,
        in_specs=(
            P(("grp", "src"), None),
            P(),
            P(None, "tp"),
            P("tp"),
            P(),
            P(),
            P(("grp", "src"), "tp", None, None),
            P(("grp", "src"), "tp", None, None),
            P(("grp", "src"), "tp"),
            P("tp", None),
            P(),
            P(),
            P(("grp", "src"), "tp"),
            P(("grp", "src"), "tp"),
            P("tp"),
            P("tp"),
            P("tp", ("grp", "src")),
            P(),
        ),
        out_specs=P(("grp", "src"), "tp"),
        check_vma=False,
    )
```
